32 devices in a mesh: tile: 8 (over z, x), dir: 4 (over y, core).
Axes of the slice: x: 2, y: 2, z: 4, core: 2. Of those that a mesh axis runs over, the one named last changes fastest.
Arguments:
- layers: bfloat16 [4, 1024, 2048], P('dir', 'tile'), may hold values from -6 to 6
- offsets: int32 [4, 4, 2], replicated, may hold values from 0 to 8191, as said below
- subap_valid: int32 [8, 16], P('tile'), may hold values from 0 to 1, as said below
- defocus: float32 [3], replicated, may hold values from -0.08 to 0.08
- weights: float32 [3], replicated, may hold values from 0.25 to 1
Outputs:
- spots: bfloat16 [4, 8, 128, 2048], P('dir', 'tile')
The draws below stay inside these ranges and needn't reach their ends.
Inputs may be any that keep to these rules, and one draw needn't show every extreme that they name: offsets[d, l, 0] < 1024 and offsets[d, l, 1] < 8192; both bounds minus one are taken by some pair in every draw. `subap_valid`: the part of an annulus of lit subapertures that falls in the strip, with a few dead ones.
All inputs are finite; a program needn't handle non-finite values.
Results may differ from the reference program's by a relative error of at most 0.0055.
Values may be sent and summed in bfloat16 or wider, within the bound.
A program may use at most 64 MiB of HBM per device.

```python
import math
import jax
import jax.numpy as jnp
from jax import lax

SUBPIX = 128
SPOT = 128
SUBX = 16
SLICES = 3
REACH = 2
QUANT = 4
OVER = 2
ROWS = 8
PCOLS = 2048
DIRS = 4
LAYERS = 4


def draw_offsets(key, part):
    keys = jax.random.split(jax.random.fold_in(key, 11), 3)
    row_bound = REACH * SUBPIX * QUANT
    col_bound = PCOLS * QUANT
    row_values = jax.random.randint(keys[0], (DIRS * LAYERS,), 0, row_bound, dtype=jnp.int32)
    col_values = jax.random.randint(keys[1], (DIRS * LAYERS,), 0, col_bound, dtype=jnp.int32)
    chosen = jax.random.permutation(keys[2], DIRS * LAYERS)
    row_values = row_values.at[chosen[0]].set(row_bound - 1).at[chosen[1]].set(0)
    col_values = col_values.at[chosen[2]].set(col_bound - 1)
    return jnp.stack([row_values, col_values], 1).reshape(DIRS, LAYERS, 2).astype(jnp.int32)


def draw_subap_valid(key, part):
    keys = jax.random.split(jax.random.fold_in(key, 23), 5)
    centre_row = jax.random.randint(keys[0], (), -4, 5, dtype=jnp.int32)
    outer_share = jax.random.randint(keys[2], (), 30, 71, dtype=jnp.int32)
    inner_most = (2 * SUBX - 1) * (2 * SUBX - 1) // 2 + 1
    inner = jax.random.randint(keys[3], (), 1, inner_most + 1, dtype=jnp.int32)
    row_twice = 2 * jnp.arange(ROWS, dtype=jnp.int32)[:, None] - (ROWS - 1) - centre_row
    col_twice = 2 * jnp.arange(SUBX, dtype=jnp.int32)[None, :] + 1
    radius = row_twice * row_twice + col_twice * col_twice
    outer = (ROWS + 4) * (ROWS + 4) + 4 * SUBX * SUBX * outer_share // 100
    alive = jax.random.randint(keys[4], (ROWS, SUBX), 0, 32, dtype=jnp.int32) != 0
    lit = (radius <= outer) & (radius >= inner) & alive
    return jnp.where(lit, 1, 0).astype(jnp.int32)


def level_of(own_key, dims, pieces, least, largest):
    def one(dim, blocks):
        heights = jax.random.uniform(jax.random.fold_in(jax.random.fold_in(own_key, 6), dim), (blocks,), jnp.float32, least / len(pieces), largest / len(pieces))
        return jnp.repeat(jnp.exp(heights), dims[dim] // blocks).reshape((-1,) + (1,) * (len(dims) - dim - 1))

    level = one(*pieces[0])
    for cut in pieces[1:]:
        level = level * one(*cut)
    return level


def noise(rng, extent, width, limit, shards=(), kind=jnp.bfloat16):
    array = width * jax.random.normal(rng, extent, jnp.float32)
    if shards:
        array = array * level_of(rng, extent, shards, -0.22, 0.18)
    return jnp.clip(array, -limit, limit).astype(kind)


def setup_inputs(seed: int = 0) -> dict:
    arg_keys = jax.random.split(jax.random.key(seed), 6)
    layers = noise(arg_keys[0], (LAYERS, ROWS * SUBPIX, PCOLS), 1.0, 6.0, ((0, 4), (1, 8)))
    offsets = draw_offsets(jax.random.fold_in(arg_keys[5], 71), 0)
    subap_valid = draw_subap_valid(jax.random.fold_in(arg_keys[5], 71), 0)
    defocus = jnp.clip(jax.random.uniform(arg_keys[3], (SLICES,), jnp.float32, -0.08, 0.08), -0.08, 0.08)
    weights = jnp.clip(jnp.exp(jax.random.uniform(arg_keys[4], (SLICES,), jnp.float32, math.log(0.25), math.log(1.0))), 0.25, 1.0)
    return dict(layers=layers, offsets=offsets, subap_valid=subap_valid, defocus=defocus, weights=weights)


def tables():
    frequency = jnp.arange(SPOT, dtype=jnp.float32) - SPOT // 2
    position = jnp.arange(SUBPIX, dtype=jnp.float32) - (SUBPIX - 1) / 2.0
    phase_angle = -2.0 * math.pi / (OVER * SUBPIX) * frequency[:, None] * position[None, :]
    factor = 1.0 / math.sqrt(SUBPIX)
    real_part = jnp.cos(phase_angle) * factor
    imag_part = jnp.sin(phase_angle) * factor
    left_table = jnp.concatenate([jnp.concatenate([real_part, -imag_part], 1), jnp.concatenate([imag_part, real_part], 1)], 0).astype(jnp.bfloat16)
    right_table = jnp.concatenate([jnp.concatenate([real_part.T, imag_part.T], 1), jnp.concatenate([-imag_part.T, real_part.T], 1)], 0).astype(jnp.bfloat16)
    return (left_table, right_table)

def interpolate(window, offset_pair):
    col_steps = offset_pair[1] // QUANT
    col_frac = (offset_pair[1] % QUANT).astype(jnp.float32) / QUANT
    row_frac = (offset_pair[0] % QUANT).astype(jnp.float32) / QUANT
    col_first = jnp.roll(window, -col_steps, axis=1)
    col_second = jnp.roll(window, -(col_steps + 1), axis=1)
    across = (1.0 - col_frac) * col_first + col_frac * col_second
    return ((1.0 - row_frac) * across[:-1] + row_frac * across[1:]).astype(jnp.bfloat16)

def spots_row(pupil_phase, first_row, total_rows, defocus, weights, valid_row):
    left_table, right_table = tables()
    row_position = ((first_row + jnp.arange(SUBPIX, dtype=jnp.int32)).astype(jnp.float32) - (total_rows - 1) / 2.0) / SUBPIX
    col_position = (jnp.arange(PCOLS, dtype=jnp.float32) - (PCOLS - 1) / 2.0) / SUBPIX
    radius = row_position[:, None] ** 2 + col_position[None, :] ** 2
    spot_sum = jnp.zeros((SPOT * SUBX, SPOT), jnp.float32)
    for altitude in range(SLICES):
        phase_angle = pupil_phase + defocus[altitude] * radius
        pupil_field = jnp.concatenate([jnp.cos(phase_angle), jnp.sin(phase_angle)], 0).astype(jnp.bfloat16)
        focal_plane = jnp.dot(left_table, pupil_field, preferred_element_type=jnp.float32).astype(jnp.bfloat16)
        blocks = jnp.concatenate([focal_plane[:SPOT].reshape(SPOT * SUBX, SUBPIX), focal_plane[SPOT:].reshape(SPOT * SUBX, SUBPIX)], 1)
        spot_field = jnp.dot(blocks, right_table, preferred_element_type=jnp.float32)
        spot_sum = spot_sum + weights[altitude] * (spot_field[:, :SPOT] ** 2 + spot_field[:, SPOT:] ** 2)
    scaled = spot_sum / jnp.sum(weights)
    masked = scaled.reshape(SPOT, SUBX, SPOT) * valid_row.astype(jnp.float32)[None, :, None]
    return masked.reshape(SPOT, SUBX * SPOT).astype(jnp.bfloat16)

def reference(layers, offsets, subap_valid, defocus, weights):
    total_rows = ROWS * SUBPIX

    def one_direction(direction):
        offset_pairs = offsets[direction]

        def one_row(row_index):
            pupil_phase = jnp.zeros((SUBPIX, PCOLS), jnp.float32)
            for layer_index in range(LAYERS):
                offset_pair = offset_pairs[layer_index]
                start_row = row_index * SUBPIX + offset_pair[0] // QUANT
                rows_index = ((start_row + jnp.arange(SUBPIX + 1, dtype=jnp.int32)) % total_rows).astype(jnp.int32)
                window = jnp.take(layers[layer_index], rows_index, axis=0).astype(jnp.float32)
                pupil_phase = pupil_phase + interpolate(window, offset_pair).astype(jnp.float32)
            return spots_row(pupil_phase, row_index * SUBPIX, total_rows, defocus, weights, subap_valid[row_index])
        return lax.map(one_row, jnp.arange(ROWS, dtype=jnp.int32))
    return lax.map(one_direction, jnp.arange(DIRS, dtype=jnp.int32))
```

```python
import functools
import math

import jax
import jax.numpy as jnp
import numpy as np
from jax import lax
from jax.experimental import pallas as pl
from jax.experimental.pallas import tpu as pltpu
from jax.sharding import PartitionSpec as P

OVER = 2
QUANT = 4
REACH = 2
LANES = 128
CHUNKS = 8
MESH = pl.DeviceIdType.MESH
HALF_PI_HI = 1.5703125
HALF_PI_LO = math.pi / 2 - 1.5703125


def base_tables(n):
    frequency = np.arange(n, dtype=np.float64) - n // 2
    position = np.arange(n, dtype=np.float64) - (n - 1) / 2.0
    angle = -2.0 * math.pi / (OVER * n) * frequency[:, None] * position[None, :]
    factor = 1.0 / math.sqrt(n)
    return (np.cos(angle) * factor).astype(np.float32), (np.sin(angle) * factor).astype(np.float32)


def cos_sin(angle):
    turns = jnp.round(angle * (2.0 / math.pi))
    rest = (angle - turns * HALF_PI_HI) - turns * HALF_PI_LO
    quadrant = turns.astype(jnp.int32)
    square = rest * rest
    sin = rest + rest * square * (-1.0 / 6 + square * (1.0 / 120 - square * (1.0 / 5040)))
    cos = 1.0 + square * (-0.5 + square * (1.0 / 24 - square * (1.0 / 720 - square * (1.0 / 40320))))
    swap = (quadrant & 1) == 1
    cos_value = jnp.where(swap, sin, cos)
    sin_value = jnp.where(swap, cos, sin)
    cos_value = jnp.where(((quadrant + 1) & 2) == 2, -cos_value, cos_value)
    sin_value = jnp.where((quadrant & 2) == 2, -sin_value, sin_value)
    return cos_value, sin_value


def kernel(
    tiles, n, blocks, slices,
    x_ref, off_ref, valid_ref, defocus_ref, weights_ref, fr_ref, fi_ref, right_ref,
    out_ref,
    ext, shifted, mix, slide, send_buf, recv_buf, local, left, col_cos, col_sin,
    z_send, z_recv, s_send, s_recv, o_send, o_recv, p_send, p_recv, y_send, y_recv,
):
    tile = lax.axis_index("tile")
    own = lax.axis_index("dir")
    core = lax.rem(own, 2)
    chip = lax.div(own, 2)
    other_core = chip * 2 + (1 - core)
    other_chip = (1 - chip) * 2 + core
    odd = lax.rem(tile, 2)
    mate = tile + 1 - 2 * odd
    below = lax.rem(tile + tiles - 2, tiles)
    above = lax.rem(tile + 2, tiles)

    barrier = pltpu.get_barrier_semaphore()
    for device in ((tile, other_core), (tile, other_chip), (mate, own), (below, own), (above, own)):
        pl.semaphore_signal(barrier, inc=1, device_id=device, device_id_type=MESH)
    pl.semaphore_wait(barrier, 5)

    rows = n // CHUNKS
    pairs = blocks // 2

    def copy(source, target, send, recv, device):
        return pltpu.make_async_remote_copy(
            src_ref=source, dst_ref=target, send_sem=send, recv_sem=recv,
            device_id=device, device_id_type=MESH,
        )

    def z_copy(k):
        return copy(
            x_ref.at[0, pl.ds(k * rows, rows)], ext.at[core, 2, pl.ds(k * rows, rows)],
            z_send.at[k], z_recv.at[k], (below, own),
        )

    def first_copy(k):
        return copy(
            x_ref.at[0, pl.ds(k * rows, rows)], ext.at[core, 1, pl.ds(k * rows, rows)],
            s_send.at[k], s_recv.at[k], (mate, own),
        )

    def relay_copy(k):
        return copy(
            ext.at[core, 2, pl.ds(k * rows, rows)], ext.at[core, 1, pl.ds(k * rows, rows)],
            s_send.at[k], s_recv.at[k], (mate, own),
        )

    def share_copy(which, k):
        part = ext.at[core, which, pl.ds(k * rows, rows)]
        return copy(part, part, p_send.at[which - 1, k], p_recv.at[which - 1, k], (tile, other_core))

    own_copy = copy(x_ref.at[0], ext.at[core, 0], o_send, o_recv, (tile, other_core))

    for k in range(CHUNKS):
        z_copy(k).start()

        @pl.when(odd == 1)
        def _():
            first_copy(k).start()

    own_copy.start()
    ext[core, 0] = x_ref[0]

    first_row = (tile * n).astype(jnp.float32)
    row_at = lax.broadcasted_iota(jnp.int32, (8, n), 1).astype(jnp.float32)
    p = (first_row + row_at - (tiles * n - 1) / 2.0) / n
    col_at = lax.broadcasted_iota(jnp.int32, (8, blocks * n), 1).astype(jnp.float32)
    q = (col_at - (blocks * n - 1) / 2.0) / n
    for a in range(slices):
        row_cos, row_sin = cos_sin(defocus_ref[a] * (p * p))
        row_cos, row_sin = row_cos[0:1], row_sin[0:1]
        real = fr_ref[...] * row_cos - fi_ref[...] * row_sin
        imag = fr_ref[...] * row_sin + fi_ref[...] * row_cos
        left[2 * a * n : (2 * a + 1) * n, 0:n] = real.astype(jnp.bfloat16)
        left[2 * a * n : (2 * a + 1) * n, n : 2 * n] = (-imag).astype(jnp.bfloat16)
        left[(2 * a + 1) * n : (2 * a + 2) * n, 0:n] = imag.astype(jnp.bfloat16)
        left[(2 * a + 1) * n : (2 * a + 2) * n, n : 2 * n] = real.astype(jnp.bfloat16)
        c, s = cos_sin(defocus_ref[a] * (q * q))
        for j in range(pairs):
            col_cos[j, a] = c[:, j * 2 * n : (j + 1) * 2 * n]
            col_sin[j, a] = s[:, j * 2 * n : (j + 1) * 2 * n]

    def steps_of(direction, slot):
        return off_ref[direction, 0, chip * 2 + slot], off_ref[direction, 1, chip * 2 + slot]

    def taps(shape, shift, fraction, along, across):
        gap = lax.broadcasted_iota(jnp.int32, shape, along) - lax.broadcasted_iota(
            jnp.int32, shape, across
        ) - shift
        return jnp.where(gap == 0, 1.0 - fraction, jnp.where(gap == 1, fraction, 0.0)).astype(
            jnp.bfloat16
        )

    for index, direction in enumerate((other_chip, own)):
        for slot in range(2):
            row_steps, col_steps = steps_of(direction, slot)
            fy = (row_steps & (QUANT - 1)).astype(jnp.float32) * (1.0 / QUANT)
            fx = (col_steps & (QUANT - 1)).astype(jnp.float32) * (1.0 / QUANT)
            down = lax.shift_right_logical(row_steps, 2) & (n - 1)
            over = lax.shift_right_logical(col_steps, 2) & (n - 1)
            mix[index, slot] = taps((n, 2 * n), down, fy, 1, 0)
            tap = taps((3 * n, 2 * n), over, fx, 0, 1)
            for half in range(2):
                first = (slot * 2 + half) * 3 * n
                slide[index, first : first + 3 * n, :] = tap

    for k in range(CHUNKS):
        z_copy(k).wait_recv()
        share_copy(2, k).start()

        @pl.when(odd == 0)
        def _():
            relay_copy(k).start()

        first_copy(k).wait_recv()
        share_copy(1, k).start()
    own_copy.wait_recv()
    for k in range(CHUNKS):
        share_copy(2, k).wait_recv()
        share_copy(1, k).wait_recv()

    def interpolated(index, direction, store, after):
        plans = []
        for slot in range(2):
            row_steps, col_steps = steps_of(direction, slot)
            top = lax.shift_right_logical(row_steps, n.bit_length() + 1)
            plans.append((top, lax.shift_right_logical(col_steps, n.bit_length() + 1)))

        def rows_step(j, carry):
            span = pl.ds(pl.multiple_of(j * 2 * n, 2 * n), 2 * n)
            for slot in range(2):
                top = plans[slot][0]
                window = jnp.concatenate([ext[slot, top, :, span], ext[slot, top + 1, :, span]], 0)
                mixed = jnp.dot(mix[index, slot], window, preferred_element_type=jnp.float32)
                high = mixed.astype(jnp.bfloat16)
                low = (mixed - high.astype(jnp.float32)).astype(jnp.bfloat16)
                for b in range(2):
                    shifted[slot, 0, 2 * j + b] = high[:, b * n : (b + 1) * n]
                    shifted[slot, 1, 2 * j + b] = low[:, b * n : (b + 1) * n]
            return carry

        lax.fori_loop(0, pairs, rows_step, 0, unroll=4)

        def cols_step(j, carry):
            parts = []
            for slot in range(2):
                begin = plans[slot][1] + 2 * j
                for half in range(2):
                    for b in range(3):
                        parts.append(shifted[slot, half, (begin + b) & (blocks - 1)])
            total = jnp.dot(
                jnp.concatenate(parts, 1), slide[index], preferred_element_type=jnp.float32
            )
            store(j, [total[:, :n], total[:, n:]])
            after(j)
            return carry

        lax.fori_loop(0, pairs, cols_step, 0, unroll=2)

    def y_copy(j):
        return copy(send_buf.at[j], recv_buf.at[j], y_send.at[j], y_recv.at[j], (tile, other_chip))

    def store_send(j, total):
        for b in range(2):
            send_buf[j, b] = total[b].astype(jnp.bfloat16)

    def send_previous(j):
        @pl.when(j > 0)
        def _():
            y_copy(j - 1).start()

    def store_local(j, total):
        for b in range(2):
            local[j, b] = total[b]

        @pl.when(j == 0)
        def _():
            y_copy(pairs - 1).start()

    interpolated(0, other_chip, store_send, send_previous)
    interpolated(1, own, store_local, lambda j: None)

    weight_sum = weights_ref[0]
    for a in range(1, slices):
        weight_sum = weight_sum + weights_ref[a]

    def final_step(j, carry):
        y_copy(j).wait_recv()
        fields = []
        for b in range(2):
            c, s = cos_sin(local[j, b] + recv_buf[j, b].astype(jnp.float32))
            fields.append(jnp.concatenate([c, s], 0).astype(jnp.bfloat16))
        field = jnp.concatenate(fields, 1)
        sums = [jnp.zeros((n, n), jnp.float32) for _ in range(2)]
        for a in range(slices):
            focal = jnp.dot(
                left[2 * a * n : (2 * a + 2) * n, :], field, preferred_element_type=jnp.float32
            )
            real, imag = focal[:n], focal[n:]
            c, s = col_cos[j, a][0:1], col_sin[j, a][0:1]
            new_real = (real * c - imag * s).astype(jnp.bfloat16)
            new_imag = (real * s + imag * c).astype(jnp.bfloat16)
            both = jnp.concatenate(
                [
                    jnp.concatenate([new_real[:, b * n : (b + 1) * n], new_imag[:, b * n : (b + 1) * n]], 1)
                    for b in range(2)
                ],
                0,
            )
            spot = jnp.dot(both, right_ref[...], preferred_element_type=jnp.float32)
            power = spot * spot
            for b in range(2):
                piece = power[b * n : (b + 1) * n]
                sums[b] = sums[b] + weights_ref[a] * (piece[:, :n] + piece[:, n:])
        for b in range(2):
            lit = valid_ref[0, 2 * j + b].astype(jnp.float32)
            out_ref[0, 0, :, pl.ds(pl.multiple_of((2 * j + b) * n, n), n)] = (
                sums[b] / weight_sum * lit
            ).astype(jnp.bfloat16)
        return carry

    lax.fori_loop(0, pairs, final_step, 0, unroll=2)

    for k in range(CHUNKS):
        z_copy(k).wait_send()
        first_copy(k).wait_send()
        share_copy(1, k).wait_send()
        share_copy(2, k).wait_send()
    own_copy.wait_send()
    for j in range(pairs):
        y_copy(j).wait_send()


def solution(mesh):
    tiles = mesh.shape["tile"]

    def shards(layers, offsets, subap_valid, defocus, weights):
        n, cols = layers.shape[1], layers.shape[2]
        blocks = cols // n
        slices = defocus.shape[0]
        pairs = blocks // 2
        fr, fi = base_tables(n)
        right = jnp.asarray(np.block([[fr.T, fi.T], [-fi.T, fr.T]])).astype(jnp.bfloat16)
        vmem = pl.BlockSpec(memory_space=pltpu.VMEM)
        smem = pl.BlockSpec(memory_space=pltpu.SMEM)
        dma = pltpu.SemaphoreType.DMA
        return pl.pallas_call(
            functools.partial(kernel, tiles, n, blocks, slices),
            out_shape=pltpu.VMEM((1, 1, n, cols), jnp.bfloat16),
            in_specs=[vmem, smem, smem, smem, smem, vmem, vmem, vmem],
            out_specs=vmem,
            scratch_shapes=[
                pltpu.VMEM((2, REACH + 1, n, cols), jnp.bfloat16),
                pltpu.VMEM((2, 2, blocks, n, n), jnp.bfloat16),
                pltpu.VMEM((2, 2, n, 2 * n), jnp.bfloat16),
                pltpu.VMEM((2, 12 * n, 2 * n), jnp.bfloat16),
                pltpu.VMEM((pairs, 2, n, n), jnp.bfloat16),
                pltpu.VMEM((pairs, 2, n, n), jnp.bfloat16),
                pltpu.VMEM((pairs, 2, n, n), jnp.float32),
                pltpu.VMEM((2 * slices * n, 2 * n), jnp.bfloat16),
                pltpu.VMEM((pairs, slices, 8, 2 * n), jnp.float32),
                pltpu.VMEM((pairs, slices, 8, 2 * n), jnp.float32),
                dma((CHUNKS,)), dma((CHUNKS,)),
                dma((CHUNKS,)), dma((CHUNKS,)),
                dma, dma,
                dma((REACH, CHUNKS)), dma((REACH, CHUNKS)),
                dma((pairs,)), dma((pairs,)),
            ],
            compiler_params=pltpu.CompilerParams(collective_id=0, has_side_effects=True),
        )(layers, jnp.transpose(offsets, (0, 2, 1)), subap_valid, defocus, weights, jnp.asarray(fr), jnp.asarray(fi), right)

    placed = (P("dir", "tile", None), P(), P("tile", None), P(), P())
    return jax.shard_map(
        shards, mesh=mesh, in_specs=placed, out_specs=P("dir", "tile", None, None), check_vma=False
    )
```

```python
import functools
import math

import jax
import jax.numpy as jnp
import numpy as np
from jax import lax
from jax.experimental import pallas as pl
from jax.experimental.pallas import tpu as pltpu
from jax.sharding import PartitionSpec as P

OVER = 2
QUANT = 4
REACH = 2
GROUP = 4
MESH = pl.DeviceIdType.MESH
HALF_PI_HI = 1.5703125
HALF_PI_LO = math.pi / 2 - 1.5703125


def base_tables(n):
    frequency = np.arange(n, dtype=np.float64) - n // 2
    position = np.arange(n, dtype=np.float64) - (n - 1) / 2.0
    angle = -2.0 * math.pi / (OVER * n) * frequency[:, None] * position[None, :]
    factor = 1.0 / math.sqrt(n)
    return (np.cos(angle) * factor).astype(np.float32), (np.sin(angle) * factor).astype(np.float32)


def cos_sin(angle):
    turns = jnp.round(angle * (2.0 / math.pi))
    rest = (angle - turns * HALF_PI_HI) - turns * HALF_PI_LO
    quadrant = turns.astype(jnp.int32)
    square = rest * rest
    sin = rest + rest * square * (-1.0 / 6 + square * (1.0 / 120 - square * (1.0 / 5040)))
    cos = 1.0 + square * (-0.5 + square * (1.0 / 24 - square * (1.0 / 720 - square * (1.0 / 40320))))
    swap = (quadrant & 1) == 1
    cos_value = jnp.where(swap, sin, cos)
    sin_value = jnp.where(swap, cos, sin)
    cos_value = jnp.where(((quadrant + 1) & 2) == 2, -cos_value, cos_value)
    sin_value = jnp.where((quadrant & 2) == 2, -sin_value, sin_value)
    return cos_value, sin_value


def taps(shape, shift, fraction, along, across):
    gap = lax.broadcasted_iota(jnp.int32, shape, along) - lax.broadcasted_iota(
        jnp.int32, shape, across
    ) - shift
    return jnp.where(gap == 0, 1.0 - fraction, jnp.where(gap == 1, fraction, 0.0)).astype(
        jnp.bfloat16
    )


def kernel(
    tiles, n, blocks, slices,
    x_ref, off_ref, valid_ref, defocus_ref, weights_ref, fr_ref, fi_ref, right_ref,
    out_ref,
    own, twin, far, halo, mixed, moved, front_mix, front_slide, back_mix, back_slide,
    x_buf, x_in, tail, out_buf, in_buf, local, left, col_cos, col_sin, fr_tab, fi_tab, right_tab,
    load_sem, table_sem, z_send, z_recv, f_send, r_send, h_recv, y_send, y_recv, t_send, t_recv,
    x_send, x_recv, o_send, o_recv, ready,
):
    tile = lax.axis_index("tile")
    place = lax.axis_index("dir")
    core = lax.rem(place, 2)
    chip = lax.div(place, 2)
    partner = chip * 2 + (1 - core)
    front, back = chip * 2, chip * 2 + 1
    far_front, far_back = (1 - chip) * 2, (1 - chip) * 2 + 1
    odd = lax.rem(tile, 2)
    mate = tile + 1 - 2 * odd
    below = lax.rem(tile + tiles - 2, tiles)
    above = lax.rem(tile + 2, tiles)
    pairs = blocks // 2
    is_front, is_back = core == 0, core == 1

    barrier = pltpu.get_barrier_semaphore()

    def greet(device):
        pl.semaphore_signal(barrier, inc=1, device_id=device, device_id_type=MESH)

    first, last = tile < 2, tile >= tiles - 2

    @pl.when(jnp.logical_not(last))
    def _():
        greet((above, front + core))

        @pl.when(is_back)
        def _():
            greet((above, front))

    @pl.when(first)
    def _():
        greet((below, back))

        @pl.when(is_front)
        def _():
            greet((below, front))

    @pl.when(is_front)
    def _():
        greet((tile, far_back))

    @pl.when(is_back)
    def _():
        @pl.when(odd == 0)
        def _():
            greet((mate, front))

    greet((mate, front + core))
    greet((tile, far_front + core))
    greet((tile, partner))

    def load(k):
        return pltpu.make_async_copy(
            x_ref.at[0, :, pl.ds(k * n, n)], own.at[k], load_sem.at[k]
        )

    tables = [
        pltpu.make_async_copy(source, target, table_sem.at[i])
        for i, (source, target) in enumerate(
            ((fr_ref, fr_tab), (fi_ref, fi_tab), (right_ref, right_tab))
        )
    ]
    for k in range(blocks):
        load(k).start()
    for table in tables:
        table.start()

    def copy(source, target, send, recv, device):
        return pltpu.make_async_remote_copy(
            src_ref=source, dst_ref=target, send_sem=send, recv_sem=recv,
            device_id=device, device_id_type=MESH,
        )

    def z_copy(k, layer=core):
        return copy(own.at[k], halo.at[layer, 1, k], z_send.at[k], z_recv.at[layer, k], (below, back))

    def f_copy(k, layer=core):
        return copy(own.at[k], halo.at[layer, 0, k], f_send.at[k], h_recv.at[layer, k], (mate, back))

    def relay(k, layer):
        return copy(
            halo.at[layer, 1, k], halo.at[layer, 0, k], r_send.at[layer, k], h_recv.at[layer, k],
            (mate, back),
        )

    def far_copy(layer=core):
        return copy(own, far.at[layer], y_send, y_recv.at[layer], (tile, far_front))

    twin_copy = copy(own, twin, t_send, t_recv, (tile, partner))

    def x_copy(j):
        return copy(x_buf.at[j], x_in.at[j], x_send.at[j], x_recv.at[j], (mate, front))

    def down_copy(j):
        return copy(out_buf.at[j], in_buf.at[j], o_send.at[j], o_recv.at[j], (below, front))

    def across_copy(j):
        return copy(out_buf.at[j], in_buf.at[j], o_send.at[j], o_recv.at[j], (tile, far_back))

    downward = jnp.where(is_front, 2, 1)
    upward = jnp.where(is_front, 1, 2)
    pl.semaphore_wait(
        barrier,
        5 + jnp.where(is_front, odd, 0) - jnp.where(first, downward, 0) + jnp.where(last, upward, 0),
    )

    @pl.when(last)
    def _():
        def answer(device):
            pl.semaphore_signal(ready, inc=1, device_id=device, device_id_type=MESH)

        answer((above, front))

        @pl.when(is_back)
        def _():
            answer((above, back))

    for k in range(blocks):
        load(k).wait()

        @pl.when(jnp.logical_not(first))
        def _():
            z_copy(k).start()

        @pl.when(odd == 1)
        def _():
            f_copy(k).start()

    far_copy().start()
    twin_copy.start()
    for table in tables:
        table.wait()

    first_row = (tile * n).astype(jnp.float32)
    row_at = lax.broadcasted_iota(jnp.int32, (8, n), 1).astype(jnp.float32)
    p = (first_row + row_at - (tiles * n - 1) / 2.0) / n
    col_at = lax.broadcasted_iota(jnp.int32, (8, blocks * n), 1).astype(jnp.float32)
    q = (col_at - (blocks * n - 1) / 2.0) / n
    for a in range(slices):
        row_cos, row_sin = cos_sin(defocus_ref[a] * (p * p))
        row_cos, row_sin = row_cos[0:1], row_sin[0:1]
        real = fr_tab[...] * row_cos - fi_tab[...] * row_sin
        imag = fr_tab[...] * row_sin + fi_tab[...] * row_cos
        left[2 * a * n : (2 * a + 1) * n, 0:n] = real.astype(jnp.bfloat16)
        left[2 * a * n : (2 * a + 1) * n, n : 2 * n] = (-imag).astype(jnp.bfloat16)
        left[(2 * a + 1) * n : (2 * a + 2) * n, 0:n] = imag.astype(jnp.bfloat16)
        left[(2 * a + 1) * n : (2 * a + 2) * n, n : 2 * n] = real.astype(jnp.bfloat16)
        c, s = cos_sin(defocus_ref[a] * (q * q))
        for j in range(pairs):
            col_cos[j, a] = c[:, j * 2 * n : (j + 1) * 2 * n]
            col_sin[j, a] = s[:, j * 2 * n : (j + 1) * 2 * n]

    @pl.when(first)
    def _():
        pl.semaphore_wait(ready, downward)
        for k in range(blocks):
            z_copy(k).start()

    def plan_of(direction, layer):
        row_steps, col_steps = off_ref[direction, 0, layer], off_ref[direction, 1, layer]
        fy = (row_steps & (QUANT - 1)).astype(jnp.float32) * (1.0 / QUANT)
        fx = (col_steps & (QUANT - 1)).astype(jnp.float32) * (1.0 / QUANT)
        down = lax.shift_right_logical(row_steps, 2)
        over = lax.shift_right_logical(col_steps, 2) & (n - 1)
        begin = lax.shift_right_logical(col_steps, n.bit_length() + 1)
        return down, fy, over, fx, begin

    @pl.when(is_front)
    def _():
        plans = [
            plan_of(place, layer)
            for layer in (front, back, far_front, far_back)
        ]
        for slot, (down, fy, over, fx, _) in enumerate(plans):
            front_slide[slot] = taps((3 * n, 2 * n), over, fx, 0, 1)
            for reach in range(REACH + 1):
                front_mix[reach * n : (reach + 1) * n, slot * n : (slot + 1) * n] = taps(
                    (n, n), down - reach * n, fy, 1, 0
                )

        def shift(slot, block_of):
            begin = plans[slot][4]

            def step(g, carry):
                rows = []
                for j in range(GROUP):
                    at = begin + 2 * (g * GROUP + j)
                    rows.append(
                        jnp.concatenate([block_of((at + b) & (blocks - 1)) for b in range(3)], 1)
                    )
                total = jnp.dot(
                    jnp.concatenate(rows, 0), front_slide[slot], preferred_element_type=jnp.float32
                ).astype(jnp.bfloat16)
                for j in range(GROUP):
                    mixed[g * GROUP + j, slot * n : (slot + 1) * n, :] = total[j * n : (j + 1) * n]
                return carry

            lax.fori_loop(0, pairs // GROUP, step, 0)

        shift(0, lambda b: own[b])
        twin_copy.wait_recv()
        shift(1, lambda b: twin[b])
        for layer in range(2):
            far_copy(layer).wait_recv()
        for layer in range(2):
            shift(2 + layer, lambda b: far[layer, b])

        def give_step(j, carry):
            total = jnp.dot(front_mix[...], mixed[j], preferred_element_type=jnp.float32)
            local[j] = total[:n]
            x_buf[j] = total[n : 2 * n].astype(jnp.bfloat16)
            tail[j] = total[2 * n :]
            out_buf[j] = total[2 * n :].astype(jnp.bfloat16)

            @pl.when(j > 0)
            def _():
                x_copy(j - 1).start()

            @pl.when((j > 0) & (odd == 0))
            def _():
                down_copy(j - 1).start()

            return carry

        lax.fori_loop(0, pairs, give_step, 0, unroll=2)
        x_copy(pairs - 1).start()

        @pl.when(odd == 0)
        def _():
            down_copy(pairs - 1).start()

        @pl.when(odd == 1)
        def _():
            def pass_step(j, carry):
                x_copy(j).wait_recv()
                out_buf[j] = (tail[j] + x_in[j].astype(jnp.float32)).astype(jnp.bfloat16)

                @pl.when(j > 0)
                def _():
                    down_copy(j - 1).start()

                return carry

            lax.fori_loop(0, pairs, pass_step, 0)
            down_copy(pairs - 1).start()

    @pl.when(is_back)
    def _():
        plans = [
            [plan_of(direction, layer) for layer in (front, back)]
            for direction in (far_back, place)
        ]
        for index in range(2):
            for slot in range(2):
                down, fy, over, fx, _ = plans[index][slot]
                back_mix[slot, index * n : (index + 1) * n, :] = taps((n, 3 * n), down, fy, 1, 0)
                back_slide[index, slot * 3 * n : (slot + 1) * 3 * n, :] = taps(
                    (3 * n, 2 * n), over, fx, 0, 1
                )
        twin_copy.wait_recv()

        def rows_step(j, carry):
            for b in range(2):
                for layer in range(2):
                    z_copy(2 * j + b, layer).wait_recv()

                    @pl.when(odd == 0)
                    def _():
                        relay(2 * j + b, layer).start()

            for layer in range(2):
                nearest = twin if layer == 0 else own
                for b in range(2):
                    relay(2 * j + b, layer).wait_recv()
                window = jnp.concatenate(
                    [
                        jnp.concatenate(
                            [nearest[2 * j + b], halo[layer, 0, 2 * j + b], halo[layer, 1, 2 * j + b]], 0
                        )
                        for b in range(2)
                    ],
                    1,
                )
                total = jnp.dot(
                    back_mix[layer], window, preferred_element_type=jnp.float32
                ).astype(jnp.bfloat16)
                for index in range(2):
                    for b in range(2):
                        moved[layer, index, 2 * j + b] = total[
                            index * n : (index + 1) * n, b * n : (b + 1) * n
                        ]
            return carry

        lax.fori_loop(0, pairs, rows_step, 0)

        def cols(index, j):
            parts = []
            for layer in range(2):
                begin = plans[index][layer][4] + 2 * j
                for b in range(3):
                    parts.append(moved[layer, index, (begin + b) & (blocks - 1)])
            return jnp.dot(
                jnp.concatenate(parts, 1), back_slide[index], preferred_element_type=jnp.float32
            )

        def give_step(j, carry):
            out_buf[j] = cols(0, j).astype(jnp.bfloat16)

            @pl.when(j > 0)
            def _():
                across_copy(j - 1).start()

            return carry

        lax.fori_loop(0, pairs, give_step, 0, unroll=2)

        def keep_step(j, carry):
            local[j] = cols(1, j)

            @pl.when(j == 0)
            def _():
                across_copy(pairs - 1).start()

            return carry

        lax.fori_loop(0, pairs, keep_step, 0, unroll=2)

    weight_sum = weights_ref[0]
    for a in range(1, slices):
        weight_sum = weight_sum + weights_ref[a]

    def final_step(j, carry):
        across_copy(j).wait_recv()

        @pl.when(is_front & (odd == 0))
        def _():
            x_copy(j).wait_recv()
            local[j] = local[j] + x_in[j].astype(jnp.float32)

        c, s = cos_sin(local[j] + in_buf[j].astype(jnp.float32))
        field = jnp.concatenate([c, s], 0).astype(jnp.bfloat16)
        sums = [jnp.zeros((n, n), jnp.float32) for _ in range(2)]
        for a in range(slices):
            focal = jnp.dot(
                left[2 * a * n : (2 * a + 2) * n, :], field, preferred_element_type=jnp.float32
            )
            real, imag = focal[:n], focal[n:]
            c, s = col_cos[j, a][0:1], col_sin[j, a][0:1]
            new_real = (real * c - imag * s).astype(jnp.bfloat16)
            new_imag = (real * s + imag * c).astype(jnp.bfloat16)
            both = jnp.concatenate(
                [
                    jnp.concatenate([new_real[:, b * n : (b + 1) * n], new_imag[:, b * n : (b + 1) * n]], 1)
                    for b in range(2)
                ],
                0,
            )
            spot = jnp.dot(both, right_tab[...], preferred_element_type=jnp.float32)
            power = spot * spot
            for b in range(2):
                piece = power[b * n : (b + 1) * n]
                sums[b] = sums[b] + weights_ref[a] * (piece[:, :n] + piece[:, n:])
        for b in range(2):
            lit = valid_ref[0, 2 * j + b].astype(jnp.float32)
            out_ref[0, 0, :, pl.ds(pl.multiple_of((2 * j + b) * n, n), n)] = (
                sums[b] / weight_sum * lit
            ).astype(jnp.bfloat16)
        return carry

    lax.fori_loop(0, pairs, final_step, 0, unroll=2)

    for k in range(blocks):
        z_copy(k).wait_send()

    @pl.when(odd == 1)
    def _():
        for k in range(blocks):
            f_copy(k).wait_send()

    far_copy().wait_send()
    twin_copy.wait_send()
    for j in range(pairs):
        across_copy(j).wait_send()

    @pl.when(is_front)
    def _():
        for j in range(pairs):
            x_copy(j).wait_send()

    @pl.when(is_back & (odd == 0))
    def _():
        for k in range(blocks):
            for layer in range(2):
                relay(k, layer).wait_send()


def solution(mesh):
    tiles = mesh.shape["tile"]

    def shards(layers, offsets, subap_valid, defocus, weights):
        n, cols = layers.shape[1], layers.shape[2]
        blocks = cols // n
        slices = defocus.shape[0]
        pairs = blocks // 2
        fr, fi = base_tables(n)
        right = jnp.asarray(np.block([[fr.T, fi.T], [-fi.T, fr.T]])).astype(jnp.bfloat16)
        vmem = pl.BlockSpec(memory_space=pltpu.VMEM)
        smem = pl.BlockSpec(memory_space=pltpu.SMEM)
        hbm = pl.BlockSpec(memory_space=pl.ANY)
        dma = pltpu.SemaphoreType.DMA
        half, full = jnp.bfloat16, jnp.float32
        return pl.pallas_call(
            functools.partial(kernel, tiles, n, blocks, slices),
            out_shape=pltpu.VMEM((1, 1, n, cols), half),
            in_specs=[hbm, smem, smem, smem, smem, hbm, hbm, hbm],
            out_specs=vmem,
            scratch_shapes=[
                pltpu.VMEM((blocks, n, n), half),
                pltpu.VMEM((blocks, n, n), half),
                pltpu.VMEM((2, blocks, n, n), half),
                pltpu.VMEM((2, REACH, blocks, n, n), half),
                pltpu.VMEM((pairs, 4 * n, 2 * n), half),
                pltpu.VMEM((2, 2, blocks, n, n), half),
                pltpu.VMEM(((REACH + 1) * n, 4 * n), half),
                pltpu.VMEM((4, 3 * n, 2 * n), half),
                pltpu.VMEM((2, 2 * n, (REACH + 1) * n), half),
                pltpu.VMEM((2, 6 * n, 2 * n), half),
                pltpu.VMEM((pairs, n, 2 * n), half),
                pltpu.VMEM((pairs, n, 2 * n), half),
                pltpu.VMEM((pairs, n, 2 * n), full),
                pltpu.VMEM((pairs, n, 2 * n), half),
                pltpu.VMEM((pairs, n, 2 * n), half),
                pltpu.VMEM((pairs, n, 2 * n), full),
                pltpu.VMEM((2 * slices * n, 2 * n), half),
                pltpu.VMEM((pairs, slices, 8, 2 * n), full),
                pltpu.VMEM((pairs, slices, 8, 2 * n), full),
                pltpu.VMEM((n, n), full),
                pltpu.VMEM((n, n), full),
                pltpu.VMEM((2 * n, 2 * n), half),
                dma((blocks,)), dma((3,)),
                dma((blocks,)), dma((2, blocks)),
                dma((blocks,)), dma((2, blocks)), dma((2, blocks)),
                dma, dma((2,)),
                dma, dma,
                dma((pairs,)), dma((pairs,)),
                dma((pairs,)), dma((pairs,)),
                pltpu.SemaphoreType.REGULAR,
            ],
            compiler_params=pltpu.CompilerParams(collective_id=0, has_side_effects=True),
        )(layers, jnp.transpose(offsets, (0, 2, 1)), subap_valid, defocus, weights, jnp.asarray(fr), jnp.asarray(fi), right)

    placed = (P("dir", "tile", None), P(), P("tile", None), P(), P())
    return jax.shard_map(
        shards, mesh=mesh, in_specs=placed, out_specs=P("dir", "tile", None, None), check_vma=False
    )
```

```python
import functools
import math

import jax
import jax.numpy as jnp
import numpy as np
from jax import lax
from jax.experimental import pallas as pl
from jax.experimental.pallas import tpu as pltpu
from jax.sharding import PartitionSpec as P

OVER = 2
QUANT = 4
REACH = 2
GROUP = 4
AHEAD = 8
MESH = pl.DeviceIdType.MESH
SIN = (3.141582022082025, -5.167142794167084, 2.541899009948703, -0.5546361567315732)
COS = (0.999999953466345, -4.934792858633932, 4.058411913339297, -1.3318801559459539, 0.21969678799073292)


def base_tables(n):
    frequency = np.arange(n, dtype=np.float64) - n // 2
    position = np.arange(n, dtype=np.float64) - (n - 1) / 2.0
    angle = -2.0 * math.pi / (OVER * n) * frequency[:, None] * position[None, :]
    factor = 1.0 / math.sqrt(n)
    return (np.cos(angle) * factor).astype(np.float32), (np.sin(angle) * factor).astype(np.float32)


def cos_sin(angle):
    turns = angle * (1.0 / math.pi)
    whole = jnp.round(turns)
    rest = turns - whole
    sign = jnp.where((whole.astype(jnp.int32) & 1) == 0, 1.0, -1.0)
    square = rest * rest
    sin, cos = SIN[-1], COS[-1]
    for factor in SIN[-2::-1]:
        sin = factor + square * sin
    for factor in COS[-2::-1]:
        cos = factor + square * cos
    return cos * sign, sin * (rest * sign)


def taps(shape, shift, fraction, along, across):
    gap = lax.broadcasted_iota(jnp.int32, shape, along) - lax.broadcasted_iota(
        jnp.int32, shape, across
    ) - shift
    return jnp.where(gap == 0, 1.0 - fraction, jnp.where(gap == 1, fraction, 0.0)).astype(
        jnp.bfloat16
    )


def kernel(
    tiles, n, blocks, slices,
    x_ref, off_hbm, valid_hbm, defocus_hbm, weights_hbm, base_ref, right_ref,
    out_ref,
    off_ref, valid_ref, defocus_ref, weights_ref, own, twin, far, halo, mixed, moved, front_mix, front_slide, back_mix, back_slide,
    x_buf, x_in, tail, out_buf, in_buf, local, left, col_cos, col_sin, base_tab, right_tab,
    load_sem, table_sem, z_send, z_recv, f_send, r_send, h_recv, y_send, y_recv, t_send, t_recv,
    x_send, x_recv, o_send, o_recv, ready,
):
    tile = lax.axis_index("tile")
    place = lax.axis_index("dir")
    core = lax.rem(place, 2)
    chip = lax.div(place, 2)
    partner = chip * 2 + (1 - core)
    front, back = chip * 2, chip * 2 + 1
    far_front, far_back = (1 - chip) * 2, (1 - chip) * 2 + 1
    odd = lax.rem(tile, 2)
    mate = tile + 1 - 2 * odd
    below = lax.rem(tile + tiles - 2, tiles)
    above = lax.rem(tile + 2, tiles)
    pairs = blocks // 2
    is_front, is_back = core == 0, core == 1

    barrier = pltpu.get_barrier_semaphore()

    def greet(device):
        pl.semaphore_signal(barrier, inc=1, device_id=device, device_id_type=MESH)

    first, last = tile < 2, tile >= tiles - 2

    @pl.when(jnp.logical_not(last))
    def _():
        greet((above, front + core))

        @pl.when(is_back)
        def _():
            greet((above, front))

    @pl.when(first)
    def _():
        greet((below, back))

        @pl.when(is_front)
        def _():
            greet((below, front))

    @pl.when(is_front)
    def _():
        greet((tile, far_back))

    @pl.when(is_back)
    def _():
        @pl.when(odd == 0)
        def _():
            greet((mate, front))

    greet((mate, front + core))
    greet((tile, far_front + core))
    greet((tile, partner))

    for k in range(blocks):
        pltpu.make_async_copy(x_ref.at[0, :, pl.ds(k * n, n)], own.at[k], load_sem).start()
    tables = [
        pltpu.make_async_copy(source, target, table_sem.at[i])
        for i, (source, target) in enumerate(
            (
                (defocus_hbm, defocus_ref), (off_hbm, off_ref), (weights_hbm, weights_ref),
                (valid_hbm, valid_ref), (base_ref, base_tab), (right_ref, right_tab),
            )
        )
    ]
    for table in tables:
        table.start()

    def copy(source, target, send, recv, device):
        return pltpu.make_async_remote_copy(
            src_ref=source, dst_ref=target, send_sem=send, recv_sem=recv,
            device_id=device, device_id_type=MESH,
        )

    def pair_of(k):
        return pl.ds(2 * k, 2)

    def z_copy(k):
        return copy(
            own.at[pair_of(k)], halo.at[core, 1, pair_of(k)], z_send, z_recv.at[k], (below, back)
        )

    def f_copy(k):
        return copy(
            own.at[pair_of(k)], halo.at[core, 0, pair_of(k)], f_send, h_recv.at[k], (mate, back)
        )

    def relay(k):
        return copy(
            halo.at[:, 1, pair_of(k)], halo.at[:, 0, pair_of(k)], r_send, h_recv.at[k], (mate, back)
        )

    def z_both(k):
        part = halo.at[:, 1, pair_of(k)]
        return copy(part, part, r_send, z_recv.at[k], (mate, back))

    z_all = copy(own, halo.at[core, 1], z_send, z_recv.at[0], (below, back))
    f_all = copy(own, halo.at[core, 0], f_send, h_recv.at[0], (mate, back))
    r_all = copy(halo.at[:, 1], halo.at[:, 0], r_send, h_recv.at[0], (mate, back))
    far_copy = copy(own, far.at[core], y_send, y_recv, (tile, far_front))
    far_both = copy(far, far, y_send, y_recv, (tile, far_front))

    twin_copy = copy(own, twin, t_send, t_recv, (tile, partner))

    def x_copy(j):
        return copy(x_buf.at[j], x_in.at[j], x_send, x_recv.at[j], (mate, front))

    def down_copy(j):
        return copy(out_buf.at[j], in_buf.at[j], o_send, o_recv.at[j], (below, front))

    def pass_on(j):
        for b in range(2):
            k = 2 * j + b
            x_copy(k).wait_recv()
            out_buf[k] = (
                tail[j, :, b * n : (b + 1) * n] + x_in[k].astype(jnp.float32)
            ).astype(jnp.bfloat16)

            @pl.when(k > 0)
            def _():
                down_copy(k - 1).start()

    def across_copy(j):
        return copy(out_buf.at[j], in_buf.at[j], o_send, o_recv.at[j], (tile, far_back))

    x_all = copy(x_buf, x_in, x_send, x_recv.at[0], (mate, front))
    out_all = copy(out_buf, in_buf, o_send, o_recv.at[0], (tile, far_back))

    downward = jnp.where(is_front, 2, 1)
    upward = jnp.where(is_front, 1, 2)
    pl.semaphore_wait(
        barrier,
        5 + jnp.where(is_front, odd, 0) - jnp.where(first, downward, 0) + jnp.where(last, upward, 0),
    )

    @pl.when(last)
    def _():
        def answer(device):
            pl.semaphore_signal(ready, inc=1, device_id=device, device_id_type=MESH)

        answer((above, front))

        @pl.when(is_back)
        def _():
            answer((above, back))

    pltpu.make_async_copy(twin, own, load_sem).wait()
    for k in range(pairs):

        @pl.when(jnp.logical_not(first))
        def _():
            z_copy(k).start()

        @pl.when(odd == 1)
        def _():
            f_copy(k).start()

    far_copy.start()
    twin_copy.start()
    for table in tables:
        table.wait()

    first_row = (tile * n).astype(jnp.float32)
    row_at = lax.broadcasted_iota(jnp.int32, (8, n), 1).astype(jnp.float32)
    p = (first_row + row_at - (tiles * n - 1) / 2.0) / n
    col_at = lax.broadcasted_iota(jnp.int32, (8, blocks * n), 1).astype(jnp.float32)
    q = (col_at - (blocks * n - 1) / 2.0) / n
    for a in range(slices):
        row_cos, row_sin = cos_sin(defocus_ref[a] * (p * p))
        row_cos, row_sin = row_cos[0:1], row_sin[0:1]
        real = base_tab[0] * row_cos - base_tab[1] * row_sin
        imag = base_tab[0] * row_sin + base_tab[1] * row_cos
        left[2 * a * n : (2 * a + 1) * n, 0:n] = real.astype(jnp.bfloat16)
        left[2 * a * n : (2 * a + 1) * n, n : 2 * n] = (-imag).astype(jnp.bfloat16)
        left[(2 * a + 1) * n : (2 * a + 2) * n, 0:n] = imag.astype(jnp.bfloat16)
        left[(2 * a + 1) * n : (2 * a + 2) * n, n : 2 * n] = real.astype(jnp.bfloat16)
        c, s = cos_sin(defocus_ref[a] * (q * q))
        for j in range(pairs):
            col_cos[j, a] = c[:, j * 2 * n : (j + 1) * 2 * n]
            col_sin[j, a] = s[:, j * 2 * n : (j + 1) * 2 * n]

    @pl.when(first)
    def _():
        pl.semaphore_wait(ready, downward)
        for k in range(pairs):
            z_copy(k).start()

    def plan_of(direction, layer):
        row_steps, col_steps = off_ref[direction, 0, layer], off_ref[direction, 1, layer]
        fy = (row_steps & (QUANT - 1)).astype(jnp.float32) * (1.0 / QUANT)
        fx = (col_steps & (QUANT - 1)).astype(jnp.float32) * (1.0 / QUANT)
        down = lax.shift_right_logical(row_steps, 2)
        over = lax.shift_right_logical(col_steps, 2) & (n - 1)
        begin = lax.shift_right_logical(col_steps, n.bit_length() + 1)
        return down, fy, over, fx, begin

    @pl.when(is_front)
    def _():
        plans = [
            plan_of(place, layer)
            for layer in (front, back, far_front, far_back)
        ]
        for slot, (down, fy, over, fx, _) in enumerate(plans):
            front_slide[slot] = taps((3 * n, 2 * n), over, fx, 0, 1)
            for reach in range(REACH + 1):
                front_mix[reach * n : (reach + 1) * n, slot * n : (slot + 1) * n] = taps(
                    (n, n), down - reach * n, fy, 1, 0
                )

        def shift(slot, block_of):
            begin = plans[slot][4]

            def step(g, carry):
                rows = []
                for j in range(GROUP):
                    at = begin + 2 * (g * GROUP + j)
                    rows.append(
                        jnp.concatenate([block_of((at + b) & (blocks - 1)) for b in range(3)], 1)
                    )
                total = jnp.dot(
                    jnp.concatenate(rows, 0), front_slide[slot], preferred_element_type=jnp.float32
                ).astype(jnp.bfloat16)
                for j in range(GROUP):
                    mixed[g * GROUP + j, slot * n : (slot + 1) * n, :] = total[j * n : (j + 1) * n]
                return carry

            lax.fori_loop(0, pairs // GROUP, step, 0)

        shift(0, lambda b: own[b])
        twin_copy.wait_recv()
        shift(1, lambda b: twin[b])
        far_both.wait_recv()
        for layer in range(2):
            shift(2 + layer, lambda b: far[layer, b])

        def give_step(j, carry):
            total = jnp.dot(front_mix[...], mixed[j], preferred_element_type=jnp.float32)
            local[j] = total[:n]
            tail[j] = total[2 * n :]
            for b in range(2):
                part = slice(b * n, (b + 1) * n)
                x_buf[2 * j + b] = total[n : 2 * n, part].astype(jnp.bfloat16)
                out_buf[2 * j + b] = total[2 * n :, part].astype(jnp.bfloat16)

            @pl.when((j > 0) & (odd == 0))
            def _():
                for b in range(2):
                    down_copy(2 * j - 2 + b).start()

            @pl.when((j > 0) & (odd == 1))
            def _():
                for b in range(2):
                    x_copy(2 * j - 2 + b).start()

            return carry

        lax.fori_loop(0, pairs, give_step, 0, unroll=2)

        @pl.when(odd == 0)
        def _():
            for b in range(2):
                down_copy(blocks - 2 + b).start()
            for k in range(blocks):
                x_copy(k).start()

        @pl.when(odd == 1)
        def _():
            for b in range(2):
                x_copy(blocks - 2 + b).start()

            def step(j, carry):
                pass_on(j)
                return carry

            lax.fori_loop(0, AHEAD, step, 0)

    @pl.when(is_back)
    def _():
        plans = [
            [plan_of(direction, layer) for layer in (front, back)]
            for direction in (far_back, place)
        ]
        for index in range(2):
            for slot in range(2):
                down, fy, over, fx, _ = plans[index][slot]
                back_mix[slot, index * n : (index + 1) * n, :] = taps((n, 3 * n), down, fy, 1, 0)
                back_slide[index, slot * 3 * n : (slot + 1) * 3 * n, :] = taps(
                    (3 * n, 2 * n), over, fx, 0, 1
                )
        twin_copy.wait_recv()

        def rows_step(j, carry):
            z_both(j).wait_recv()

            @pl.when(odd == 0)
            def _():
                relay(j).start()

            relay(j).wait_recv()
            for layer in range(2):
                nearest = twin if layer == 0 else own
                window = jnp.concatenate(
                    [
                        jnp.concatenate(
                            [nearest[2 * j + b], halo[layer, 0, 2 * j + b], halo[layer, 1, 2 * j + b]], 0
                        )
                        for b in range(2)
                    ],
                    1,
                )
                total = jnp.dot(
                    back_mix[layer], window, preferred_element_type=jnp.float32
                ).astype(jnp.bfloat16)
                for index in range(2):
                    for b in range(2):
                        moved[layer, index, 2 * j + b] = total[
                            index * n : (index + 1) * n, b * n : (b + 1) * n
                        ]
            return carry

        lax.fori_loop(0, pairs, rows_step, 0)

        def cols(index, j):
            parts = []
            for layer in range(2):
                begin = plans[index][layer][4] + 2 * j
                for b in range(3):
                    parts.append(moved[layer, index, (begin + b) & (blocks - 1)])
            return jnp.dot(
                jnp.concatenate(parts, 1), back_slide[index], preferred_element_type=jnp.float32
            )

        def give_step(j, carry):
            total = cols(0, j).astype(jnp.bfloat16)
            for b in range(2):
                out_buf[2 * j + b] = total[:, b * n : (b + 1) * n]

            @pl.when(j > 0)
            def _():
                for b in range(2):
                    across_copy(2 * j - 2 + b).start()

            return carry

        lax.fori_loop(0, pairs, give_step, 0, unroll=2)

        def keep_step(j, carry):
            local[j] = cols(1, j)

            @pl.when(j == 0)
            def _():
                for b in range(2):
                    across_copy(blocks - 2 + b).start()

            return carry

        lax.fori_loop(0, pairs, keep_step, 0, unroll=2)

    weight_sum = weights_ref[0]
    for a in range(1, slices):
        weight_sum = weight_sum + weights_ref[a]
    share = 1.0 / jnp.full((8, n), weight_sum, jnp.float32)[0:1]

    def final_step(j, carry):
        @pl.when(is_front & (odd == 1) & (j < pairs - AHEAD))
        def _():
            pass_on(j + AHEAD)

        @pl.when(is_front & (odd == 1) & (j == pairs - AHEAD))
        def _():
            down_copy(blocks - 1).start()

        @pl.when(is_front & (odd == 0))
        def _():
            for b in range(2):
                x_copy(2 * j + b).wait_recv()
                part = slice(b * n, (b + 1) * n)
                local[j, :, part] = local[j, :, part] + x_in[2 * j + b].astype(jnp.float32)

        for b in range(2):
            across_copy(2 * j + b).wait_recv()
        arrived = jnp.concatenate([in_buf[2 * j + b].astype(jnp.float32) for b in range(2)], 1)
        c, s = cos_sin(local[j] + arrived)
        field = jnp.concatenate([c, s], 0).astype(jnp.bfloat16)
        sums = [jnp.zeros((n, n), jnp.float32) for _ in range(2)]
        for a in range(slices):
            focal = jnp.dot(
                left[2 * a * n : (2 * a + 2) * n, :], field, preferred_element_type=jnp.float32
            )
            real, imag = focal[:n], focal[n:]
            c, s = col_cos[j, a][0:1], col_sin[j, a][0:1]
            new_real = (real * c - imag * s).astype(jnp.bfloat16)
            new_imag = (real * s + imag * c).astype(jnp.bfloat16)
            both = jnp.concatenate(
                [
                    jnp.concatenate([new_real[:, b * n : (b + 1) * n], new_imag[:, b * n : (b + 1) * n]], 1)
                    for b in range(2)
                ],
                0,
            )
            spot = jnp.dot(both, right_tab[...], preferred_element_type=jnp.float32)
            power = spot * spot
            for b in range(2):
                piece = power[b * n : (b + 1) * n]
                sums[b] = sums[b] + weights_ref[a] * (piece[:, :n] + piece[:, n:])
        for b in range(2):
            lit = valid_ref[0, 2 * j + b].astype(jnp.float32)
            out_ref[0, 0, :, pl.ds(pl.multiple_of((2 * j + b) * n, n), n)] = (
                sums[b] * (share * lit)
            ).astype(jnp.bfloat16)
        return carry

    lax.fori_loop(0, pairs, final_step, 0, unroll=2)

    z_all.wait_send()
    far_copy.wait_send()
    twin_copy.wait_send()
    out_all.wait_send()

    @pl.when(odd == 1)
    def _():
        f_all.wait_send()

    @pl.when(is_front)
    def _():
        x_all.wait_send()

    @pl.when(is_back & (odd == 0))
    def _():
        r_all.wait_send()


def solution(mesh):
    tiles = mesh.shape["tile"]

    def shards(layers, offsets, subap_valid, defocus, weights):
        n, cols = layers.shape[1], layers.shape[2]
        blocks = cols // n
        slices = defocus.shape[0]
        pairs = blocks // 2
        fr, fi = base_tables(n)
        right = jnp.asarray(np.block([[fr.T, fi.T], [-fi.T, fr.T]])).astype(jnp.bfloat16)
        vmem = pl.BlockSpec(memory_space=pltpu.VMEM)
        hbm = pl.BlockSpec(memory_space=pl.ANY)
        dma = pltpu.SemaphoreType.DMA
        half, full = jnp.bfloat16, jnp.float32
        return pl.pallas_call(
            functools.partial(kernel, tiles, n, blocks, slices),
            out_shape=pltpu.VMEM((1, 1, n, cols), half),
            in_specs=[hbm] * 7,
            out_specs=vmem,
            scratch_shapes=[
                pltpu.SMEM((4, 2, 4), jnp.int32),
                pltpu.SMEM((1, blocks), jnp.int32),
                pltpu.SMEM((slices,), full),
                pltpu.SMEM((slices,), full),
                pltpu.VMEM((blocks, n, n), half),
                pltpu.VMEM((blocks, n, n), half),
                pltpu.VMEM((2, blocks, n, n), half),
                pltpu.VMEM((2, REACH, blocks, n, n), half),
                pltpu.VMEM((pairs, 4 * n, 2 * n), half),
                pltpu.VMEM((2, 2, blocks, n, n), half),
                pltpu.VMEM(((REACH + 1) * n, 4 * n), half),
                pltpu.VMEM((4, 3 * n, 2 * n), half),
                pltpu.VMEM((2, 2 * n, (REACH + 1) * n), half),
                pltpu.VMEM((2, 6 * n, 2 * n), half),
                pltpu.VMEM((blocks, n, n), half),
                pltpu.VMEM((blocks, n, n), half),
                pltpu.VMEM((pairs, n, 2 * n), full),
                pltpu.VMEM((blocks, n, n), half),
                pltpu.VMEM((blocks, n, n), half),
                pltpu.VMEM((pairs, n, 2 * n), full),
                pltpu.VMEM((2 * slices * n, 2 * n), half),
                pltpu.VMEM((pairs, slices, 8, 2 * n), full),
                pltpu.VMEM((pairs, slices, 8, 2 * n), full),
                pltpu.VMEM((2, n, n), full),
                pltpu.VMEM((2 * n, 2 * n), half),
                dma, dma((6,)),
                dma, dma((pairs,)), dma, dma, dma((pairs,)),
                dma, dma, dma, dma,
                dma, dma((blocks,)), dma, dma((blocks,)),
                pltpu.SemaphoreType.REGULAR,
            ],
            compiler_params=pltpu.CompilerParams(collective_id=0, has_side_effects=True),
        )(layers, jnp.transpose(offsets, (0, 2, 1)), subap_valid, defocus, weights, jnp.asarray(np.stack([fr, fi])), right)

    placed = (P("dir", "tile", None), P(), P("tile", None), P(), P())
    return jax.shard_map(
        shards, mesh=mesh, in_specs=placed, out_specs=P("dir", "tile", None, None), check_vma=False
    )
```

```python
import functools
import math

import jax
import jax.numpy as jnp
import numpy as np
from jax import lax
from jax.experimental import pallas as pl
from jax.experimental.pallas import tpu as pltpu
from jax.sharding import PartitionSpec as P

OVER = 2
QUANT = 4
REACH = 2
GROUP = 8
BATCH = 4
LEAD = 2
MESH = pl.DeviceIdType.MESH
SIN = (3.141582022082025, -5.167142794167084, 2.541899009948703, -0.5546361567315732)
COS = (0.999999953466345, -4.934792858633932, 4.058411913339297, -1.3318801559459539, 0.21969678799073292)


def base_tables(n):
    frequency = np.arange(n, dtype=np.float64) - n // 2
    position = np.arange(n, dtype=np.float64) - (n - 1) / 2.0
    angle = -2.0 * math.pi / (OVER * n) * frequency[:, None] * position[None, :]
    factor = 1.0 / math.sqrt(n)
    return (np.cos(angle) * factor).astype(np.float32), (np.sin(angle) * factor).astype(np.float32)


def cos_sin(angle):
    turns = angle * (1.0 / math.pi)
    whole = jnp.round(turns)
    rest = turns - whole
    sign = jnp.where((whole.astype(jnp.int32) & 1) == 0, 1.0, -1.0)
    square = rest * rest
    sin, cos = SIN[-1], COS[-1]
    for factor in SIN[-2::-1]:
        sin = factor + square * sin
    for factor in COS[-2::-1]:
        cos = factor + square * cos
    return cos * sign, sin * (rest * sign)


def taps(shape, shift, fraction, along, across):
    gap = lax.broadcasted_iota(jnp.int32, shape, along) - lax.broadcasted_iota(
        jnp.int32, shape, across
    ) - shift
    return jnp.where(gap == 0, 1.0 - fraction, jnp.where(gap == 1, fraction, 0.0)).astype(
        jnp.bfloat16
    )


def kernel(
    tiles, n, blocks, slices,
    x_ref, off_hbm, valid_hbm, defocus_hbm, weights_hbm, base_ref, right_ref,
    out_ref,
    off_ref, valid_ref, defocus_ref, weights_ref, own, twin, far, halo, mixed, moved, front_mix, front_slide, back_mix, back_slide,
    x_buf, x_in, tail, out_buf, in_buf, local, left, col_cos, col_sin, base_tab, right_tab, field_buf,
    load_sem, table_sem, z_send, z_recv, f_send, r_send, h_recv, y_send, y_recv, t_send, t_recv,
    x_send, x_recv, o_send, o_recv, ready, go,
):
    tile = lax.axis_index("tile")
    place = lax.axis_index("dir")
    core = lax.rem(place, 2)
    chip = lax.div(place, 2)
    partner = chip * 2 + (1 - core)
    front, back = chip * 2, chip * 2 + 1
    far_front, far_back = (1 - chip) * 2, (1 - chip) * 2 + 1
    odd = lax.rem(tile, 2)
    mate = tile + 1 - 2 * odd
    below = lax.rem(tile + tiles - 2, tiles)
    above = lax.rem(tile + 2, tiles)
    pairs = blocks // 2
    is_front, is_back = core == 0, core == 1

    barrier = pltpu.get_barrier_semaphore()

    def greet(device):
        pl.semaphore_signal(barrier, inc=1, device_id=device, device_id_type=MESH)

    first, last = tile < 2, tile >= tiles - 2

    @pl.when(is_back)
    def _():
        greet((above, back))

    @pl.when(jnp.logical_not(last))
    def _():
        greet((above, front))

    @pl.when(first & is_front)
    def _():
        greet((below, back))
        greet((below, front))

    @pl.when(is_front)
    def _():
        greet((tile, far_back))

    @pl.when(is_back)
    def _():
        @pl.when(odd == 0)
        def _():
            greet((mate, front))

    greet((mate, front + core))
    greet((tile, far_front + core))
    greet((tile, partner))

    for k in range(blocks):
        pltpu.make_async_copy(x_ref.at[0, :, pl.ds(k * n, n)], own.at[k], load_sem).start()
    tables = [
        pltpu.make_async_copy(source, target, table_sem.at[i])
        for i, (source, target) in enumerate(
            (
                (defocus_hbm, defocus_ref), (off_hbm, off_ref), (weights_hbm, weights_ref),
                (valid_hbm, valid_ref), (base_ref, base_tab), (right_ref, right_tab),
            )
        )
    ]
    for table in tables:
        table.start()

    def copy(source, target, send, recv, device):
        return pltpu.make_async_remote_copy(
            src_ref=source, dst_ref=target, send_sem=send, recv_sem=recv,
            device_id=device, device_id_type=MESH,
        )

    def pair_of(k):
        return pl.ds(2 * k, 2)

    def z_copy(k, layer=core):
        return copy(
            own.at[pair_of(k)], halo.at[layer, 1, pair_of(k)], z_send, z_recv.at[layer, k],
            (below, back),
        )

    def f_copy(k):
        return copy(
            own.at[pair_of(k)], halo.at[core, 0, pair_of(k)], f_send, h_recv.at[k], (mate, back)
        )

    def relay(k, layer):
        return copy(
            halo.at[layer, 1, pair_of(k)], halo.at[layer, 0, pair_of(k)], r_send, h_recv.at[k],
            (mate, back),
        )

    def h_both(k):
        part = halo.at[:, 0, pair_of(k)]
        return copy(part, part, r_send, h_recv.at[k], (mate, back))

    z_all = copy(own, halo.at[core, 1], z_send, z_recv.at[0, 0], (below, back))
    f_all = copy(own, halo.at[core, 0], f_send, h_recv.at[0], (mate, back))
    r_all = copy(halo.at[:, 1], halo.at[:, 0], r_send, h_recv.at[0], (mate, back))
    far_copy = copy(own, far.at[core], y_send, y_recv, (tile, far_front))
    far_both = copy(far, far, y_send, y_recv, (tile, far_front))

    twin_copy = copy(own, twin, t_send, t_recv, (tile, partner))

    def x_copy(j):
        return copy(x_buf.at[j], x_in.at[j], x_send, x_recv.at[j], (mate, front))

    def down_copy(j):
        return copy(out_buf.at[j], in_buf.at[j], o_send, o_recv.at[lax.div(j, 2)], (below, front))

    def pass_on(j):
        for b in range(2):
            k = 2 * j + b
            x_copy(k).wait_recv()
            out_buf[k] = (
                tail[j, :, b * n : (b + 1) * n] + x_in[k].astype(jnp.float32)
            ).astype(jnp.bfloat16)

            @pl.when(k > 0)
            def _():
                down_copy(k - 1).start()

    def across_copy(j):
        return copy(
            out_buf.at[j], in_buf.at[j], o_send, o_recv.at[lax.div(j, 2)], (tile, far_back)
        )

    def await_in(j):
        part = pair_of(j)
        copy(out_buf.at[part], in_buf.at[part], o_send, o_recv.at[j], (tile, far_back)).wait_recv()

    x_all = copy(x_buf, x_in, x_send, x_recv.at[0], (mate, front))
    out_all = copy(out_buf, in_buf, o_send, o_recv.at[0], (tile, far_back))

    held = first & is_front
    pl.semaphore_wait(
        barrier,
        5 + jnp.where(is_front, odd, 0) - jnp.where(held, 2, 0) + jnp.where(last, 1, 0),
    )

    @pl.when(last)
    def _():
        pl.semaphore_signal(
            ready.at[core], inc=1, device_id=(above, front), device_id_type=MESH
        )

    pltpu.make_async_copy(twin, own, load_sem).wait()
    @pl.when(jnp.logical_not(held))
    def _():
        for k in range(pairs):
            z_copy(k).start()

    @pl.when(odd == 1)
    def _():
        for k in range(pairs):
            f_copy(k).start()

    far_copy.start()
    twin_copy.start()
    for table in tables:
        table.wait()

    first_row = (tile * n).astype(jnp.float32)
    row_at = lax.broadcasted_iota(jnp.int32, (8, n), 1).astype(jnp.float32)
    p = (first_row + row_at - (tiles * n - 1) / 2.0) / n
    col_at = lax.broadcasted_iota(jnp.int32, (8, blocks * n), 1).astype(jnp.float32)
    q = (col_at - (blocks * n - 1) / 2.0) / n
    weight_sum = weights_ref[0]
    for a in range(1, slices):
        weight_sum = weight_sum + weights_ref[a]
    for a in range(slices):
        row_cos, row_sin = cos_sin(defocus_ref[a] * (p * p))
        share = jnp.sqrt(jnp.full((8, n), weights_ref[a], jnp.float32) / weight_sum)
        row_cos, row_sin = (row_cos * share)[0:1], (row_sin * share)[0:1]
        real = base_tab[0] * row_cos - base_tab[1] * row_sin
        imag = base_tab[0] * row_sin + base_tab[1] * row_cos
        left[2 * a * n : (2 * a + 1) * n, 0:n] = real.astype(jnp.bfloat16)
        left[2 * a * n : (2 * a + 1) * n, n : 2 * n] = (-imag).astype(jnp.bfloat16)
        left[(2 * a + 1) * n : (2 * a + 2) * n, 0:n] = imag.astype(jnp.bfloat16)
        left[(2 * a + 1) * n : (2 * a + 2) * n, n : 2 * n] = real.astype(jnp.bfloat16)
        c, s = cos_sin(defocus_ref[a] * (q * q))
        for j in range(pairs):
            col_cos[j, a] = c[:, j * 2 * n : (j + 1) * 2 * n]
            col_sin[j, a] = s[:, j * 2 * n : (j + 1) * 2 * n]

    @pl.when(held)
    def _():
        pl.semaphore_wait(ready.at[1], 1)
        for k in range(pairs):
            z_copy(k).start()

    def plan_of(direction, layer):
        row_steps, col_steps = off_ref[direction, 0, layer], off_ref[direction, 1, layer]
        fy = (row_steps & (QUANT - 1)).astype(jnp.float32) * (1.0 / QUANT)
        fx = (col_steps & (QUANT - 1)).astype(jnp.float32) * (1.0 / QUANT)
        down = lax.shift_right_logical(row_steps, 2)
        over = lax.shift_right_logical(col_steps, 2) & (n - 1)
        begin = lax.shift_right_logical(col_steps, n.bit_length() + 1)
        return down, fy, over, fx, begin

    @pl.when(is_front)
    def _():
        plans = [
            plan_of(place, layer)
            for layer in (front, back, far_front, far_back)
        ]
        for slot, (down, fy, over, fx, _) in enumerate(plans):
            front_slide[slot] = taps((3 * n, 2 * n), over, fx, 0, 1)
            for reach in range(REACH + 1):
                front_mix[reach * n : (reach + 1) * n, slot * n : (slot + 1) * n] = taps(
                    (n, n), down - reach * n, fy, 1, 0
                )

        def shift(slot, block_of):
            begin = plans[slot][4]

            def step(g, carry):
                rows = []
                for j in range(GROUP):
                    at = begin + 2 * (g * GROUP + j)
                    rows.append(
                        jnp.concatenate([block_of((at + b) & (blocks - 1)) for b in range(3)], 1)
                    )
                total = jnp.dot(
                    jnp.concatenate(rows, 0), front_slide[slot], preferred_element_type=jnp.float32
                ).astype(jnp.bfloat16)
                for j in range(GROUP):
                    mixed[g * GROUP + j, slot * n : (slot + 1) * n, :] = total[j * n : (j + 1) * n]
                return carry

            lax.fori_loop(0, pairs // GROUP, step, 0)

        shift(0, lambda b: own[b])
        twin_copy.wait_recv()
        shift(1, lambda b: twin[b])
        far_both.wait_recv()
        groups = pairs // GROUP

        def far_step(i, carry):
            side, g = lax.div(i, groups), lax.rem(i, groups)
            begin = jnp.where(side == 0, plans[2][4], plans[3][4])
            rows = []
            for j in range(GROUP):
                at = begin + 2 * (g * GROUP + j)
                rows.append(
                    jnp.concatenate([far[side, (at + b) & (blocks - 1)] for b in range(3)], 1)
                )
            total = jnp.dot(
                jnp.concatenate(rows, 0), front_slide[2 + side], preferred_element_type=jnp.float32
            ).astype(jnp.bfloat16)
            place_at = pl.ds(pl.multiple_of((2 + side) * n, n), n)
            for j in range(GROUP):
                mixed[g * GROUP + j, place_at, :] = total[j * n : (j + 1) * n]
            return carry

        lax.fori_loop(0, 2 * groups, far_step, 0)

        def give_step(j, carry):
            total = jnp.dot(front_mix[...], mixed[j], preferred_element_type=jnp.float32)
            local[j] = total[:n]
            tail[j] = total[2 * n :]
            for b in range(2):
                part = slice(b * n, (b + 1) * n)
                x_buf[2 * j + b] = total[n : 2 * n, part].astype(jnp.bfloat16)
                out_buf[2 * j + b] = total[2 * n :, part].astype(jnp.bfloat16)

            return carry

        @pl.when(first)
        def _():
            pl.semaphore_wait(ready.at[0], 1)

        for half in range(2):
            lax.fori_loop(half * pairs // 2, (half + 1) * pairs // 2, give_step, 0, unroll=2)
            ready_blocks = range(half * blocks // 2, (half + 1) * blocks // 2)

            @pl.when(odd == 0)
            def _():
                for k in ready_blocks:
                    down_copy(k).start()

            @pl.when((odd == 0) & jnp.logical_not(last))
            def _():
                if half == 0:
                    pl.semaphore_wait(go, 1)
                for k in ready_blocks:
                    x_copy(k).start()

            @pl.when(odd == 1)
            def _():
                for k in ready_blocks:
                    x_copy(k).start()

        @pl.when((odd == 0) & last)
        def _():
            pl.semaphore_wait(go, 1)
            for k in range(blocks):
                x_copy(k).start()

        @pl.when(odd == 1)
        def _():
            def step(j, carry):
                pass_on(j)
                return carry

            lax.fori_loop(0, pairs, step, 0)

    @pl.when(is_back)
    def _():
        plans = [
            [plan_of(direction, layer) for layer in (front, back)]
            for direction in (far_back, place)
        ]
        for index in range(2):
            for slot in range(2):
                down, fy, over, fx, _ = plans[index][slot]
                back_mix[slot, index * n : (index + 1) * n, :] = taps((n, 3 * n), down, fy, 1, 0)
                back_slide[index, slot * 3 * n : (slot + 1) * 3 * n, :] = taps(
                    (3 * n, 2 * n), over, fx, 0, 1
                )
        twin_copy.wait_recv()

        lead = jnp.where(last & (odd == 0), LEAD, 0)

        def take(k, layer):
            z_copy(k, layer).wait_recv()

            @pl.when(odd == 0)
            def _():
                relay(k, layer).start()

        def lead_step(k, carry):
            take(k, 1)
            return carry

        lax.fori_loop(0, lead, lead_step, 0)

        def rows_step(j, carry):
            take(j, 0)

            @pl.when(j + lead < pairs)
            def _():
                take(j + lead, 1)

            h_both(j).wait_recv()
            for layer in range(2):
                nearest = twin if layer == 0 else own
                window = jnp.concatenate(
                    [
                        jnp.concatenate(
                            [nearest[2 * j + b], halo[layer, 0, 2 * j + b], halo[layer, 1, 2 * j + b]], 0
                        )
                        for b in range(2)
                    ],
                    1,
                )
                total = jnp.dot(
                    back_mix[layer], window, preferred_element_type=jnp.float32
                ).astype(jnp.bfloat16)
                for index in range(2):
                    for b in range(2):
                        moved[layer, index, 2 * j + b] = total[
                            index * n : (index + 1) * n, b * n : (b + 1) * n
                        ]
            return carry

        lax.fori_loop(0, pairs, rows_step, 0)

        @pl.when(odd == 0)
        def _():
            pl.semaphore_signal(go, inc=1, device_id=(tile, partner), device_id_type=MESH)

        def cols(index, g):
            rows = []
            for j in range(BATCH):
                parts = []
                for layer in range(2):
                    begin = plans[index][layer][4] + 2 * (g * BATCH + j)
                    for b in range(3):
                        parts.append(moved[layer, index, (begin + b) & (blocks - 1)])
                rows.append(jnp.concatenate(parts, 1))
            return jnp.dot(
                jnp.concatenate(rows, 0), back_slide[index], preferred_element_type=jnp.float32
            )

        def give_step(g, carry):
            total = cols(0, g).astype(jnp.bfloat16)
            for j in range(BATCH):
                for b in range(2):
                    out_buf[2 * (g * BATCH + j) + b] = total[j * n : (j + 1) * n, b * n : (b + 1) * n]

            @pl.when(g > 0)
            def _():
                for k in range(2 * BATCH):
                    across_copy(2 * (g - 1) * BATCH + k).start()

            return carry

        lax.fori_loop(0, pairs // BATCH, give_step, 0)

        def keep_step(g, carry):
            total = cols(1, g)
            for j in range(BATCH):
                local[g * BATCH + j] = total[j * n : (j + 1) * n]

            @pl.when(g == 0)
            def _():
                for k in range(2 * BATCH):
                    across_copy(blocks - 2 * BATCH + k).start()

            return carry

        lax.fori_loop(0, pairs // BATCH, keep_step, 0)

    def field_of(j):
        arrived = jnp.concatenate([in_buf[2 * j + b].astype(jnp.float32) for b in range(2)], 1)
        c, s = cos_sin(local[j] + arrived)
        return jnp.concatenate([c, s], 0).astype(jnp.bfloat16)

    def spots(j, field):
        focal = jnp.dot(left[...], field, preferred_element_type=jnp.float32)
        fields = []
        for a in range(slices):
            real, imag = focal[2 * a * n : (2 * a + 1) * n], focal[(2 * a + 1) * n : (2 * a + 2) * n]
            c, s = col_cos[j, a][0:1], col_sin[j, a][0:1]
            new_real = (real * c - imag * s).astype(jnp.bfloat16)
            new_imag = (real * s + imag * c).astype(jnp.bfloat16)
            for b in range(2):
                fields.append(
                    jnp.concatenate([new_real[:, b * n : (b + 1) * n], new_imag[:, b * n : (b + 1) * n]], 1)
                )
        spot = jnp.dot(jnp.concatenate(fields, 0), right_tab[...], preferred_element_type=jnp.float32)
        power = spot * spot
        for b in range(2):
            total = 0.0
            for a in range(slices):
                piece = power[(2 * a + b) * n : (2 * a + b + 1) * n]
                total = total + (piece[:, :n] + piece[:, n:])
            lit = valid_ref[0, 2 * j + b].astype(jnp.float32)
            out_ref[0, 0, :, pl.ds(pl.multiple_of((2 * j + b) * n, n), n)] = (total * lit).astype(
                jnp.bfloat16
            )

    passing = is_front & (odd == 1)

    @pl.when(jnp.logical_not(passing))
    def _():
        def final_step(j, carry):
            @pl.when(is_front)
            def _():
                for b in range(2):
                    x_copy(2 * j + b).wait_recv()
                    part = slice(b * n, (b + 1) * n)
                    local[j, :, part] = local[j, :, part] + x_in[2 * j + b].astype(jnp.float32)

            await_in(j)
            spots(j, field_of(j))
            return carry

        lax.fori_loop(0, pairs, final_step, 0, unroll=2)

    @pl.when(passing)
    def _():
        down_copy(blocks - 1).start()
        await_in(0)
        field_buf[0] = field_of(0)

        def final_step(i, carry):
            j = 2 * i
            await_in(j + 1)
            field_buf[1] = field_of(j + 1)
            spots(j, field_buf[0])
            await_in(j + 2)
            field_buf[0] = field_of(j + 2)
            spots(j + 1, field_buf[1])
            return carry

        lax.fori_loop(0, pairs // 2 - 1, final_step, 0)
        await_in(pairs - 1)
        field_buf[1] = field_of(pairs - 1)
        spots(pairs - 2, field_buf[0])
        spots(pairs - 1, field_buf[1])

    z_all.wait_send()
    far_copy.wait_send()
    twin_copy.wait_send()
    out_all.wait_send()

    @pl.when(odd == 1)
    def _():
        f_all.wait_send()

    @pl.when(is_front)
    def _():
        x_all.wait_send()

    @pl.when(is_back & (odd == 0))
    def _():
        r_all.wait_send()


def solution(mesh):
    tiles = mesh.shape["tile"]

    def shards(layers, offsets, subap_valid, defocus, weights):
        n, cols = layers.shape[1], layers.shape[2]
        blocks = cols // n
        slices = defocus.shape[0]
        pairs = blocks // 2
        fr, fi = base_tables(n)
        right = jnp.asarray(np.block([[fr.T, fi.T], [-fi.T, fr.T]])).astype(jnp.bfloat16)
        vmem = pl.BlockSpec(memory_space=pltpu.VMEM)
        hbm = pl.BlockSpec(memory_space=pl.ANY)
        dma = pltpu.SemaphoreType.DMA
        half, full = jnp.bfloat16, jnp.float32
        return pl.pallas_call(
            functools.partial(kernel, tiles, n, blocks, slices),
            out_shape=pltpu.VMEM((1, 1, n, cols), half),
            in_specs=[hbm] * 7,
            out_specs=vmem,
            scratch_shapes=[
                pltpu.SMEM((4, 2, 4), jnp.int32),
                pltpu.SMEM((1, blocks), jnp.int32),
                pltpu.SMEM((slices,), full),
                pltpu.SMEM((slices,), full),
                pltpu.VMEM((blocks, n, n), half),
                pltpu.VMEM((blocks, n, n), half),
                pltpu.VMEM((2, blocks, n, n), half),
                pltpu.VMEM((2, REACH, blocks, n, n), half),
                pltpu.VMEM((pairs, 4 * n, 2 * n), half),
                pltpu.VMEM((2, 2, blocks, n, n), half),
                pltpu.VMEM(((REACH + 1) * n, 4 * n), half),
                pltpu.VMEM((4, 3 * n, 2 * n), half),
                pltpu.VMEM((2, 2 * n, (REACH + 1) * n), half),
                pltpu.VMEM((2, 6 * n, 2 * n), half),
                pltpu.VMEM((blocks, n, n), half),
                pltpu.VMEM((blocks, n, n), half),
                pltpu.VMEM((pairs, n, 2 * n), full),
                pltpu.VMEM((blocks, n, n), half),
                pltpu.VMEM((blocks, n, n), half),
                pltpu.VMEM((pairs, n, 2 * n), full),
                pltpu.VMEM((2 * slices * n, 2 * n), half),
                pltpu.VMEM((pairs, slices, 8, 2 * n), full),
                pltpu.VMEM((pairs, slices, 8, 2 * n), full),
                pltpu.VMEM((2, n, n), full),
                pltpu.VMEM((2 * n, 2 * n), half),
                pltpu.VMEM((2, 2 * n, 2 * n), half),
                dma, dma((6,)),
                dma, dma((2, pairs)), dma, dma, dma((pairs,)),
                dma, dma, dma, dma,
                dma, dma((blocks,)), dma, dma((pairs,)),
                pltpu.SemaphoreType.REGULAR((2,)),
                pltpu.SemaphoreType.REGULAR,
            ],
            compiler_params=pltpu.CompilerParams(collective_id=0, has_side_effects=True),
        )(layers, jnp.transpose(offsets, (0, 2, 1)), subap_valid, defocus, weights, jnp.asarray(np.stack([fr, fi])), right)

    placed = (P("dir", "tile", None), P(), P("tile", None), P(), P())
    return jax.shard_map(
        shards, mesh=mesh, in_specs=placed, out_specs=P("dir", "tile", None, None), check_vma=False
    )
```

```python
import functools
import math

import jax
import jax.numpy as jnp
import numpy as np
from jax import lax
from jax.experimental import pallas as pl
from jax.experimental.pallas import tpu as pltpu
from jax.sharding import PartitionSpec as P

OVER = 2
QUANT = 4
REACH = 2
GROUP = 8
BATCH = 4
LEAD = 2
PACE = 2
DETOUR = 1
MESH = pl.DeviceIdType.MESH
SIN = (3.141582022082025, -5.167142794167084, 2.541899009948703, -0.5546361567315732)
COS = (0.999999953466345, -4.934792858633932, 4.058411913339297, -1.3318801559459539, 0.21969678799073292)


def base_tables(n):
    frequency = np.arange(n, dtype=np.float64) - n // 2
    position = np.arange(n, dtype=np.float64) - (n - 1) / 2.0
    angle = -2.0 * math.pi / (OVER * n) * frequency[:, None] * position[None, :]
    factor = 1.0 / math.sqrt(n)
    return (np.cos(angle) * factor).astype(np.float32), (np.sin(angle) * factor).astype(np.float32)


def cos_sin(angle):
    turns = angle * (1.0 / math.pi)
    whole = jnp.round(turns)
    rest = turns - whole
    sign = jnp.where((whole.astype(jnp.int32) & 1) == 0, 1.0, -1.0)
    square = rest * rest
    sin, cos = SIN[-1], COS[-1]
    for factor in SIN[-2::-1]:
        sin = factor + square * sin
    for factor in COS[-2::-1]:
        cos = factor + square * cos
    return cos * sign, sin * (rest * sign)


def taps(shape, shift, fraction, along, across):
    gap = lax.broadcasted_iota(jnp.int32, shape, along) - lax.broadcasted_iota(
        jnp.int32, shape, across
    ) - shift
    return jnp.where(gap == 0, 1.0 - fraction, jnp.where(gap == 1, fraction, 0.0)).astype(
        jnp.bfloat16
    )


def kernel(
    tiles, n, blocks, slices,
    x_ref, off_hbm, valid_hbm, defocus_hbm, weights_hbm, base_ref, right_ref,
    out_ref,
    off_ref, valid_ref, defocus_ref, weights_ref, own, twin, far, halo, via, mixed, moved, front_mix, front_slide, back_mix, back_slide,
    x_buf, x_in, tail, out_buf, in_buf, local, left, col_cos, col_sin, base_tab, right_tab, field_buf,
    load_sem, table_sem, z_send, z_recv, f_send, r_send, h_recv, y_send, y_recv, t_send, t_recv,
    x_send, x_recv, o_send, o_recv, v_send, v_recv, ready,
):
    tile = lax.axis_index("tile")
    place = lax.axis_index("dir")
    core = lax.rem(place, 2)
    chip = lax.div(place, 2)
    partner = chip * 2 + (1 - core)
    front, back = chip * 2, chip * 2 + 1
    far_front, far_back = (1 - chip) * 2, (1 - chip) * 2 + 1
    odd = lax.rem(tile, 2)
    mate = tile + 1 - 2 * odd
    below = lax.rem(tile + tiles - 2, tiles)
    above = lax.rem(tile + 2, tiles)
    pairs = blocks // 2
    is_front, is_back = core == 0, core == 1

    barrier = pltpu.get_barrier_semaphore()

    def greet(device):
        pl.semaphore_signal(barrier, inc=1, device_id=device, device_id_type=MESH)

    first, last = tile < 2, tile >= tiles - 2

    @pl.when(is_back)
    def _():
        greet((above, back))

    @pl.when(jnp.logical_not(last))
    def _():
        greet((above, front))

    @pl.when(first & is_front)
    def _():
        greet((below, back))
        greet((below, front))

    @pl.when(is_front)
    def _():
        greet((tile, far_back))

    @pl.when(is_back)
    def _():
        greet((mate, front))

    greet((mate, front + core))
    greet((tile, far_front + core))
    greet((tile, partner))

    for k in range(blocks):
        pltpu.make_async_copy(x_ref.at[0, :, pl.ds(k * n, n)], own.at[k], load_sem).start()
    tables = [
        pltpu.make_async_copy(source, target, table_sem.at[i])
        for i, (source, target) in enumerate(
            (
                (defocus_hbm, defocus_ref), (off_hbm, off_ref), (weights_hbm, weights_ref),
                (valid_hbm, valid_ref), (base_ref, base_tab), (right_ref, right_tab),
            )
        )
    ]
    for table in tables:
        table.start()

    def copy(source, target, send, recv, device):
        return pltpu.make_async_remote_copy(
            src_ref=source, dst_ref=target, send_sem=send, recv_sem=recv,
            device_id=device, device_id_type=MESH,
        )

    def pair_of(k):
        return pl.ds(2 * k, 2)

    def z_copy(k, layer=core):
        return copy(
            own.at[pair_of(k)], halo.at[layer, 1, pair_of(k)], z_send, z_recv.at[layer, k],
            (below, back),
        )

    def f_copy(k):
        return copy(
            own.at[pair_of(k)], halo.at[core, 0, pair_of(k)], f_send, h_recv.at[k], (mate, back)
        )

    def relay(k, layer):
        return copy(
            halo.at[layer, 1, pair_of(k)], halo.at[layer, 0, pair_of(k)], r_send, h_recv.at[k],
            (mate, back),
        )

    def h_both(k):
        part = halo.at[:, 0, pair_of(k)]
        return copy(part, part, r_send, h_recv.at[k], (mate, back))

    straight = pairs - DETOUR
    rest = pl.ds(2 * straight, 2 * DETOUR)

    def detour(layer=core):
        return copy(own.at[rest], via.at[layer], v_send, v_recv, (mate, back))

    detour_both = copy(via, via, v_send, v_recv, (mate, back))

    def onward(k):
        part = pl.ds(2 * (k - straight), 2)
        return copy(
            via.at[:, part], halo.at[:, 0, pair_of(k)], r_send, h_recv.at[k], (below, back)
        )

    z_all = copy(own, halo.at[core, 1], z_send, z_recv.at[0, 0], (below, back))
    f_all = copy(own, halo.at[core, 0], f_send, h_recv.at[0], (mate, back))
    before = pl.ds(0, 2 * straight)
    r_all = copy(halo.at[:, 1, before], halo.at[:, 0, before], r_send, h_recv.at[0], (mate, back))
    onward_all = copy(via, via, r_send, h_recv.at[0], (below, back))
    far_copy = copy(own, far.at[core], y_send, y_recv, (tile, far_front))
    far_both = copy(far, far, y_send, y_recv, (tile, far_front))

    twin_copy = copy(own, twin, t_send, t_recv, (tile, partner))

    def x_copy(j):
        return copy(x_buf.at[j], x_in.at[j], x_send, x_recv.at[j], (mate, front))

    def down_copy(j):
        return copy(out_buf.at[j], in_buf.at[j], o_send, o_recv.at[lax.div(j, 2)], (below, front))

    def pass_on(j):
        for b in range(2):
            k = 2 * j + b
            x_copy(k).wait_recv()
            out_buf[k] = (
                tail[j, :, b * n : (b + 1) * n] + x_in[k].astype(jnp.float32)
            ).astype(jnp.bfloat16)

            @pl.when(k > 0)
            def _():
                down_copy(k - 1).start()

    def across_copy(j):
        return copy(
            out_buf.at[j], in_buf.at[j], o_send, o_recv.at[lax.div(j, 2)], (tile, far_back)
        )

    def await_in(j):
        part = pair_of(j)
        copy(out_buf.at[part], in_buf.at[part], o_send, o_recv.at[j], (tile, far_back)).wait_recv()

    x_all = copy(x_buf, x_in, x_send, x_recv.at[0], (mate, front))
    out_all = copy(out_buf, in_buf, o_send, o_recv.at[0], (tile, far_back))

    held = first & is_front
    pl.semaphore_wait(
        barrier,
        5 + jnp.where(is_front, 1, 0) - jnp.where(held, 2, 0) + jnp.where(last, 1, 0),
    )

    @pl.when(last)
    def _():
        pl.semaphore_signal(
            ready.at[core], inc=1, device_id=(above, front), device_id_type=MESH
        )

    pltpu.make_async_copy(twin, own, load_sem).wait()
    @pl.when(odd == 0)
    def _():
        detour().start()

    @pl.when(jnp.logical_not(held))
    def _():
        for k in range(pairs):
            z_copy(k).start()

    @pl.when(odd == 1)
    def _():
        for k in range(pairs):
            f_copy(k).start()

    far_copy.start()
    twin_copy.start()
    for table in tables:
        table.wait()

    first_row = (tile * n).astype(jnp.float32)
    row_at = lax.broadcasted_iota(jnp.int32, (8, n), 1).astype(jnp.float32)
    p = (first_row + row_at - (tiles * n - 1) / 2.0) / n
    col_at = lax.broadcasted_iota(jnp.int32, (8, blocks * n), 1).astype(jnp.float32)
    q = (col_at - (blocks * n - 1) / 2.0) / n
    weight_sum = weights_ref[0]
    for a in range(1, slices):
        weight_sum = weight_sum + weights_ref[a]
    for a in range(slices):
        row_cos, row_sin = cos_sin(defocus_ref[a] * (p * p))
        share = jnp.sqrt(jnp.full((8, n), weights_ref[a], jnp.float32) / weight_sum)
        row_cos, row_sin = (row_cos * share)[0:1], (row_sin * share)[0:1]
        real = base_tab[0] * row_cos - base_tab[1] * row_sin
        imag = base_tab[0] * row_sin + base_tab[1] * row_cos
        left[2 * a * n : (2 * a + 1) * n, 0:n] = real.astype(jnp.bfloat16)
        left[2 * a * n : (2 * a + 1) * n, n : 2 * n] = (-imag).astype(jnp.bfloat16)
        left[(2 * a + 1) * n : (2 * a + 2) * n, 0:n] = imag.astype(jnp.bfloat16)
        left[(2 * a + 1) * n : (2 * a + 2) * n, n : 2 * n] = real.astype(jnp.bfloat16)
        c, s = cos_sin(defocus_ref[a] * (q * q))
        for j in range(pairs):
            col_cos[j, a] = c[:, j * 2 * n : (j + 1) * 2 * n]
            col_sin[j, a] = s[:, j * 2 * n : (j + 1) * 2 * n]

    @pl.when(held)
    def _():
        pl.semaphore_wait(ready.at[1], 1)
        for k in range(pairs):
            z_copy(k).start()

    def plan_of(direction, layer):
        row_steps, col_steps = off_ref[direction, 0, layer], off_ref[direction, 1, layer]
        fy = (row_steps & (QUANT - 1)).astype(jnp.float32) * (1.0 / QUANT)
        fx = (col_steps & (QUANT - 1)).astype(jnp.float32) * (1.0 / QUANT)
        down = lax.shift_right_logical(row_steps, 2)
        over = lax.shift_right_logical(col_steps, 2) & (n - 1)
        begin = lax.shift_right_logical(col_steps, n.bit_length() + 1)
        return down, fy, over, fx, begin

    @pl.when(is_front)
    def _():
        plans = [
            plan_of(place, layer)
            for layer in (front, back, far_front, far_back)
        ]
        for slot, (down, fy, over, fx, _) in enumerate(plans):
            front_slide[slot] = taps((3 * n, 2 * n), over, fx, 0, 1)
            for reach in range(REACH + 1):
                front_mix[reach * n : (reach + 1) * n, slot * n : (slot + 1) * n] = taps(
                    (n, n), down - reach * n, fy, 1, 0
                )

        def shift(slot, block_of):
            begin = plans[slot][4]

            def step(g, carry):
                rows = []
                for j in range(GROUP):
                    at = begin + 2 * (g * GROUP + j)
                    rows.append(
                        jnp.concatenate([block_of((at + b) & (blocks - 1)) for b in range(3)], 1)
                    )
                total = jnp.dot(
                    jnp.concatenate(rows, 0), front_slide[slot], preferred_element_type=jnp.float32
                ).astype(jnp.bfloat16)
                for j in range(GROUP):
                    mixed[g * GROUP + j, slot * n : (slot + 1) * n, :] = total[j * n : (j + 1) * n]
                return carry

            lax.fori_loop(0, pairs // GROUP, step, 0)

        shift(0, lambda b: own[b])
        twin_copy.wait_recv()
        shift(1, lambda b: twin[b])
        far_both.wait_recv()
        @pl.when(first)
        def _():
            pl.semaphore_wait(ready.at[0], 1)

        def send_pair(j):
            for b in range(2):
                x_copy(2 * j + b).start()

            @pl.when(odd == 0)
            def _():
                for b in range(2):
                    down_copy(2 * j + b).start()

        def give_step(g, carry):
            for side in range(2):
                begin = plans[2 + side][4] + 2 * PACE * g
                rows = []
                for j in range(PACE):
                    rows.append(
                        jnp.concatenate(
                            [far[side, (begin + 2 * j + b) & (blocks - 1)] for b in range(3)], 1
                        )
                    )
                total = jnp.dot(
                    jnp.concatenate(rows, 0), front_slide[2 + side], preferred_element_type=jnp.float32
                ).astype(jnp.bfloat16)
                for j in range(PACE):
                    mixed[g * PACE + j, (2 + side) * n : (3 + side) * n, :] = total[j * n : (j + 1) * n]
            for i in range(PACE):
                j = g * PACE + i
                total = jnp.dot(front_mix[...], mixed[j], preferred_element_type=jnp.float32)
                local[j] = total[:n]
                tail[j] = total[2 * n :]
                for b in range(2):
                    part = slice(b * n, (b + 1) * n)
                    x_buf[2 * j + b] = total[n : 2 * n, part].astype(jnp.bfloat16)
                    out_buf[2 * j + b] = total[2 * n :, part].astype(jnp.bfloat16)
            @pl.when(g > 0)
            def _():
                send_pair(g * PACE - 1)

            for j in range(PACE - 1):
                send_pair(g * PACE + j)
            return carry

        lax.fori_loop(0, pairs // PACE, give_step, 0)


        @pl.when(odd == 1)
        def _():
            pass_on(0)
            for b in range(2):
                x_copy(blocks - 2 + b).start()

            def step(j, carry):
                pass_on(j)
                return carry

            lax.fori_loop(1, pairs, step, 0)

    @pl.when(is_back)
    def _():
        plans = [
            [plan_of(direction, layer) for layer in (front, back)]
            for direction in (far_back, place)
        ]
        for index in range(2):
            for slot in range(2):
                down, fy, over, fx, _ = plans[index][slot]
                back_mix[slot, index * n : (index + 1) * n, :] = taps((n, 3 * n), down, fy, 1, 0)
                back_slide[index, slot * 3 * n : (slot + 1) * 3 * n, :] = taps(
                    (3 * n, 2 * n), over, fx, 0, 1
                )
        twin_copy.wait_recv()

        lead = jnp.where(last & (odd == 0), LEAD, 0)

        def take(k, layer):
            z_copy(k, layer).wait_recv()

            @pl.when((odd == 0) & (k < straight))
            def _():
                relay(k, layer).start()

        def lead_step(k, carry):
            take(k, 1)
            return carry

        lax.fori_loop(0, lead, lead_step, 0)

        @pl.when(odd == 1)
        def _():
            detour_both.wait_recv()
            for k in range(straight, pairs):
                onward(k).start()

        def rows_step(j, carry):
            take(j, 0)

            @pl.when(j + lead < pairs)
            def _():
                take(j + lead, 1)

            h_both(j).wait_recv()
            for layer in range(2):
                nearest = twin if layer == 0 else own
                window = jnp.concatenate(
                    [
                        jnp.concatenate(
                            [nearest[2 * j + b], halo[layer, 0, 2 * j + b], halo[layer, 1, 2 * j + b]], 0
                        )
                        for b in range(2)
                    ],
                    1,
                )
                total = jnp.dot(
                    back_mix[layer], window, preferred_element_type=jnp.float32
                ).astype(jnp.bfloat16)
                for index in range(2):
                    for b in range(2):
                        moved[layer, index, 2 * j + b] = total[
                            index * n : (index + 1) * n, b * n : (b + 1) * n
                        ]
            return carry

        lax.fori_loop(0, pairs, rows_step, 0)

        def cols(index, g):
            rows = []
            for j in range(BATCH):
                parts = []
                for layer in range(2):
                    begin = plans[index][layer][4] + 2 * (g * BATCH + j)
                    for b in range(3):
                        parts.append(moved[layer, index, (begin + b) & (blocks - 1)])
                rows.append(jnp.concatenate(parts, 1))
            return jnp.dot(
                jnp.concatenate(rows, 0), back_slide[index], preferred_element_type=jnp.float32
            )

        def give_step(g, carry):
            total = cols(0, g).astype(jnp.bfloat16)
            for j in range(BATCH):
                for b in range(2):
                    out_buf[2 * (g * BATCH + j) + b] = total[j * n : (j + 1) * n, b * n : (b + 1) * n]

            @pl.when(g > 0)
            def _():
                for k in range(2 * BATCH):
                    across_copy(2 * (g - 1) * BATCH + k).start()

            return carry

        lax.fori_loop(0, pairs // BATCH, give_step, 0)

        def keep_step(g, carry):
            total = cols(1, g)
            for j in range(BATCH):
                local[g * BATCH + j] = total[j * n : (j + 1) * n]

            @pl.when(g == 0)
            def _():
                for k in range(2 * BATCH):
                    across_copy(blocks - 2 * BATCH + k).start()

            return carry

        lax.fori_loop(0, pairs // BATCH, keep_step, 0)

    def field_of(j):
        arrived = jnp.concatenate([in_buf[2 * j + b].astype(jnp.float32) for b in range(2)], 1)
        c, s = cos_sin(local[j] + arrived)
        return jnp.concatenate([c, s], 0).astype(jnp.bfloat16)

    def spots(j, field):
        focal = jnp.dot(left[...], field, preferred_element_type=jnp.float32)
        fields = []
        for a in range(slices):
            real, imag = focal[2 * a * n : (2 * a + 1) * n], focal[(2 * a + 1) * n : (2 * a + 2) * n]
            c, s = col_cos[j, a][0:1], col_sin[j, a][0:1]
            new_real = (real * c - imag * s).astype(jnp.bfloat16)
            new_imag = (real * s + imag * c).astype(jnp.bfloat16)
            for b in range(2):
                fields.append(
                    jnp.concatenate([new_real[:, b * n : (b + 1) * n], new_imag[:, b * n : (b + 1) * n]], 1)
                )
        spot = jnp.dot(jnp.concatenate(fields, 0), right_tab[...], preferred_element_type=jnp.float32)
        power = spot * spot
        for b in range(2):
            total = 0.0
            for a in range(slices):
                piece = power[(2 * a + b) * n : (2 * a + b + 1) * n]
                total = total + (piece[:, :n] + piece[:, n:])
            lit = valid_ref[0, 2 * j + b].astype(jnp.float32)
            out_ref[0, 0, :, pl.ds(pl.multiple_of((2 * j + b) * n, n), n)] = (total * lit).astype(
                jnp.bfloat16
            )

    passing = is_front & (odd == 1)

    @pl.when(jnp.logical_not(passing))
    def _():
        def final_step(j, carry):
            @pl.when(is_front)
            def _():
                for b in range(2):
                    x_copy(2 * j + b).wait_recv()
                    part = slice(b * n, (b + 1) * n)
                    local[j, :, part] = local[j, :, part] + x_in[2 * j + b].astype(jnp.float32)

                @pl.when(j == 0)
                def _():
                    for b in range(2):
                        x_copy(blocks - 2 + b).start()
                        down_copy(blocks - 2 + b).start()

            await_in(j)
            spots(j, field_of(j))
            return carry

        lax.fori_loop(0, pairs, final_step, 0, unroll=2)

    @pl.when(passing)
    def _():
        down_copy(blocks - 1).start()
        await_in(0)
        field_buf[0] = field_of(0)

        def final_step(i, carry):
            j = 2 * i
            await_in(j + 1)
            field_buf[1] = field_of(j + 1)
            spots(j, field_buf[0])
            await_in(j + 2)
            field_buf[0] = field_of(j + 2)
            spots(j + 1, field_buf[1])
            return carry

        lax.fori_loop(0, pairs // 2 - 1, final_step, 0)
        await_in(pairs - 1)
        field_buf[1] = field_of(pairs - 1)
        spots(pairs - 2, field_buf[0])
        spots(pairs - 1, field_buf[1])

    z_all.wait_send()
    far_copy.wait_send()
    twin_copy.wait_send()
    out_all.wait_send()

    @pl.when(odd == 1)
    def _():
        f_all.wait_send()

    @pl.when(is_front)
    def _():
        x_all.wait_send()

    @pl.when(odd == 0)
    def _():
        detour().wait_send()

    @pl.when(is_back & (odd == 0))
    def _():
        r_all.wait_send()

    @pl.when(is_back & (odd == 1))
    def _():
        onward_all.wait_send()


def solution(mesh):
    tiles = mesh.shape["tile"]

    def shards(layers, offsets, subap_valid, defocus, weights):
        n, cols = layers.shape[1], layers.shape[2]
        blocks = cols // n
        slices = defocus.shape[0]
        pairs = blocks // 2
        fr, fi = base_tables(n)
        right = jnp.asarray(np.block([[fr.T, fi.T], [-fi.T, fr.T]])).astype(jnp.bfloat16)
        vmem = pl.BlockSpec(memory_space=pltpu.VMEM)
        hbm = pl.BlockSpec(memory_space=pl.ANY)
        dma = pltpu.SemaphoreType.DMA
        half, full = jnp.bfloat16, jnp.float32
        return pl.pallas_call(
            functools.partial(kernel, tiles, n, blocks, slices),
            out_shape=pltpu.VMEM((1, 1, n, cols), half),
            in_specs=[hbm] * 7,
            out_specs=vmem,
            scratch_shapes=[
                pltpu.SMEM((4, 2, 4), jnp.int32),
                pltpu.SMEM((1, blocks), jnp.int32),
                pltpu.SMEM((slices,), full),
                pltpu.SMEM((slices,), full),
                pltpu.VMEM((blocks, n, n), half),
                pltpu.VMEM((blocks, n, n), half),
                pltpu.VMEM((2, blocks, n, n), half),
                pltpu.VMEM((2, REACH, blocks, n, n), half),
                pltpu.VMEM((2, 2 * DETOUR, n, n), half),
                pltpu.VMEM((pairs, 4 * n, 2 * n), half),
                pltpu.VMEM((2, 2, blocks, n, n), half),
                pltpu.VMEM(((REACH + 1) * n, 4 * n), half),
                pltpu.VMEM((4, 3 * n, 2 * n), half),
                pltpu.VMEM((2, 2 * n, (REACH + 1) * n), half),
                pltpu.VMEM((2, 6 * n, 2 * n), half),
                pltpu.VMEM((blocks, n, n), half),
                pltpu.VMEM((blocks, n, n), half),
                pltpu.VMEM((pairs, n, 2 * n), full),
                pltpu.VMEM((blocks, n, n), half),
                pltpu.VMEM((blocks, n, n), half),
                pltpu.VMEM((pairs, n, 2 * n), full),
                pltpu.VMEM((2 * slices * n, 2 * n), half),
                pltpu.VMEM((pairs, slices, 8, 2 * n), full),
                pltpu.VMEM((pairs, slices, 8, 2 * n), full),
                pltpu.VMEM((2, n, n), full),
                pltpu.VMEM((2 * n, 2 * n), half),
                pltpu.VMEM((2, 2 * n, 2 * n), half),
                dma, dma((6,)),
                dma, dma((2, pairs)), dma, dma, dma((pairs,)),
                dma, dma, dma, dma,
                dma, dma((blocks,)), dma, dma((pairs,)), dma, dma,
                pltpu.SemaphoreType.REGULAR((2,)),
            ],
            compiler_params=pltpu.CompilerParams(collective_id=0, has_side_effects=True),
        )(layers, jnp.transpose(offsets, (0, 2, 1)), subap_valid, defocus, weights, jnp.asarray(np.stack([fr, fi])), right)

    placed = (P("dir", "tile", None), P(), P("tile", None), P(), P())
    return jax.shard_map(
        shards, mesh=mesh, in_specs=placed, out_specs=P("dir", "tile", None, None), check_vma=False
    )
```

```python
import functools
import math

import jax
import jax.numpy as jnp
import numpy as np
from jax import lax
from jax.experimental import pallas as pl
from jax.experimental.pallas import tpu as pltpu
from jax.sharding import PartitionSpec as P

OVER = 2
QUANT = 4
REACH = 2
GROUP = 8
BATCH = 4
LEAD = 3
PACE = 2
EARLY = 2
DETOUR = 2
MESH = pl.DeviceIdType.MESH
SIN = (3.141582022082025, -5.167142794167084, 2.541899009948703, -0.5546361567315732)
COS = (0.999999953466345, -4.934792858633932, 4.058411913339297, -1.3318801559459539, 0.21969678799073292)


def base_tables(n):
    frequency = np.arange(n, dtype=np.float64) - n // 2
    position = np.arange(n, dtype=np.float64) - (n - 1) / 2.0
    angle = -2.0 * math.pi / (OVER * n) * frequency[:, None] * position[None, :]
    factor = 1.0 / math.sqrt(n)
    return (np.cos(angle) * factor).astype(np.float32), (np.sin(angle) * factor).astype(np.float32)


def cos_sin(angle):
    turns = angle * (1.0 / math.pi)
    whole = jnp.round(turns)
    rest = turns - whole
    sign = jnp.where((whole.astype(jnp.int32) & 1) == 0, 1.0, -1.0)
    square = rest * rest
    sin, cos = SIN[-1], COS[-1]
    for factor in SIN[-2::-1]:
        sin = factor + square * sin
    for factor in COS[-2::-1]:
        cos = factor + square * cos
    return cos * sign, sin * (rest * sign)


def taps(shape, shift, fraction, along, across):
    gap = lax.broadcasted_iota(jnp.int32, shape, along) - lax.broadcasted_iota(
        jnp.int32, shape, across
    ) - shift
    return jnp.where(gap == 0, 1.0 - fraction, jnp.where(gap == 1, fraction, 0.0)).astype(
        jnp.bfloat16
    )


def kernel(
    tiles, n, blocks, slices,
    x_ref, off_hbm, valid_hbm, defocus_hbm, weights_hbm, base_ref, right_ref,
    out_ref,
    off_ref, valid_ref, defocus_ref, weights_ref, own, twin, far, halo, via, mixed, moved, front_mix, front_slide, back_mix, back_slide,
    x_buf, x_in, tail, out_buf, in_buf, local, left, col_cos, col_sin, base_tab, right_tab, field_buf,
    load_sem, table_sem, z_send, z_recv, f_send, r_send, h_recv, y_send, y_recv, t_send, t_recv,
    x_send, x_recv, o_send, o_recv, v_send, v_recv, ready,
):
    tile = lax.axis_index("tile")
    place = lax.axis_index("dir")
    core = lax.rem(place, 2)
    chip = lax.div(place, 2)
    partner = chip * 2 + (1 - core)
    front, back = chip * 2, chip * 2 + 1
    far_front, far_back = (1 - chip) * 2, (1 - chip) * 2 + 1
    odd = lax.rem(tile, 2)
    mate = tile + 1 - 2 * odd
    below = lax.rem(tile + tiles - 2, tiles)
    above = lax.rem(tile + 2, tiles)
    pairs = blocks // 2
    is_front, is_back = core == 0, core == 1

    first, last = tile < 2, tile >= tiles - 2
    ahead = jnp.where(first, pairs - EARLY, pairs)

    barrier = pltpu.get_barrier_semaphore()

    def greet(device):
        pl.semaphore_signal(barrier, inc=1, device_id=device, device_id_type=MESH)

    @pl.when(is_back)
    def _():
        greet((above, back))

    @pl.when(jnp.logical_not(last))
    def _():
        greet((above, front))

    @pl.when(first & is_front)
    def _():
        greet((below, back))
        greet((below, front))

    @pl.when(is_front)
    def _():
        greet((tile, far_back))

    @pl.when(is_back)
    def _():
        greet((mate, front))

    greet((mate, front + core))
    greet((tile, far_front + core))
    greet((tile, partner))

    for k in range(blocks):
        pltpu.make_async_copy(x_ref.at[0, :, pl.ds(k * n, n)], own.at[k], load_sem).start()
    tables = [
        pltpu.make_async_copy(source, target, table_sem.at[i])
        for i, (source, target) in enumerate(
            (
                (defocus_hbm, defocus_ref), (off_hbm, off_ref), (weights_hbm, weights_ref),
                (valid_hbm, valid_ref), (base_ref, base_tab), (right_ref, right_tab),
            )
        )
    ]
    for table in tables:
        table.start()

    def copy(source, target, send, recv, device):
        return pltpu.make_async_remote_copy(
            src_ref=source, dst_ref=target, send_sem=send, recv_sem=recv,
            device_id=device, device_id_type=MESH,
        )

    def pair_of(k):
        return pl.ds(2 * k, 2)

    def z_copy(k, layer=core):
        return copy(
            own.at[pair_of(k)], halo.at[layer, 1, pair_of(k)], z_send, z_recv.at[layer, k],
            (below, back),
        )

    def f_copy(k):
        return copy(
            own.at[pair_of(k)], halo.at[core, 0, pair_of(k)], f_send, h_recv.at[k], (mate, back)
        )

    def relay(k, layer):
        return copy(
            halo.at[layer, 1, pair_of(k)], halo.at[layer, 0, pair_of(k)], r_send, h_recv.at[k],
            (mate, back),
        )

    def h_both(k):
        part = halo.at[:, 0, pair_of(k)]
        return copy(part, part, r_send, h_recv.at[k], (mate, back))

    straight = pairs - DETOUR
    rest = pl.ds(2 * straight, 2 * DETOUR)

    def detour(layer=core):
        return copy(own.at[rest], via.at[layer], v_send, v_recv, (mate, back))

    detour_both = copy(via, via, v_send, v_recv, (mate, back))

    def onward(k):
        part = pl.ds(2 * (k - straight), 2)
        return copy(
            via.at[:, part], halo.at[:, 0, pair_of(k)], r_send, h_recv.at[k], (below, back)
        )

    z_all = copy(own, halo.at[core, 1], z_send, z_recv.at[0, 0], (below, back))
    f_all = copy(own, halo.at[core, 0], f_send, h_recv.at[0], (mate, back))
    before = pl.ds(0, 2 * straight)
    r_all = copy(halo.at[:, 1, before], halo.at[:, 0, before], r_send, h_recv.at[0], (mate, back))
    onward_all = copy(via, via, r_send, h_recv.at[0], (below, back))
    far_copy = copy(own, far.at[core], y_send, y_recv, (tile, far_front))
    far_both = copy(far, far, y_send, y_recv, (tile, far_front))

    twin_copy = copy(own, twin, t_send, t_recv, (tile, partner))

    def x_copy(j):
        return copy(x_buf.at[j], x_in.at[j], x_send, x_recv.at[j], (mate, front))

    def down_copy(j):
        return copy(out_buf.at[j], in_buf.at[j], o_send, o_recv.at[lax.div(j, 2)], (below, front))

    def pass_on(j):
        for b in range(2):
            k = 2 * j + b
            x_copy(k).wait_recv()
            out_buf[k] = (
                tail[j, :, b * n : (b + 1) * n] + x_in[k].astype(jnp.float32)
            ).astype(jnp.bfloat16)

            @pl.when(k > 0)
            def _():
                down_copy(k - 1).start()

    def across_copy(j):
        return copy(
            out_buf.at[j], in_buf.at[j], o_send, o_recv.at[lax.div(j, 2)], (tile, far_back)
        )

    def await_in(j):
        part = pair_of(j)
        copy(out_buf.at[part], in_buf.at[part], o_send, o_recv.at[j], (tile, far_back)).wait_recv()

    x_all = copy(x_buf, x_in, x_send, x_recv.at[0], (mate, front))
    out_all = copy(out_buf, in_buf, o_send, o_recv.at[0], (tile, far_back))

    held = first & is_front
    pl.semaphore_wait(
        barrier,
        5 + jnp.where(is_front, 1, 0) - jnp.where(held, 2, 0) + jnp.where(last, 1, 0),
    )

    @pl.when(last)
    def _():
        pl.semaphore_signal(
            ready.at[core], inc=1, device_id=(above, front), device_id_type=MESH
        )

    pltpu.make_async_copy(twin, own, load_sem).wait()
    @pl.when(odd == 0)
    def _():
        detour().start()

    @pl.when(jnp.logical_not(held))
    def _():
        for k in range(pairs):
            z_copy(k).start()

    @pl.when(odd == 1)
    def _():
        for k in range(pairs):
            f_copy(k).start()

    far_copy.start()
    twin_copy.start()
    for table in tables:
        table.wait()

    first_row = (tile * n).astype(jnp.float32)
    row_at = lax.broadcasted_iota(jnp.int32, (8, n), 1).astype(jnp.float32)
    p = (first_row + row_at - (tiles * n - 1) / 2.0) / n
    col_at = lax.broadcasted_iota(jnp.int32, (8, blocks * n), 1).astype(jnp.float32)
    q = (col_at - (blocks * n - 1) / 2.0) / n
    weight_sum = weights_ref[0]
    for a in range(1, slices):
        weight_sum = weight_sum + weights_ref[a]
    for a in range(slices):
        row_cos, row_sin = cos_sin(defocus_ref[a] * (p * p))
        share = jnp.sqrt(jnp.full((8, n), weights_ref[a], jnp.float32) / weight_sum)
        row_cos, row_sin = (row_cos * share)[0:1], (row_sin * share)[0:1]
        real = base_tab[0] * row_cos - base_tab[1] * row_sin
        imag = base_tab[0] * row_sin + base_tab[1] * row_cos
        left[2 * a * n : (2 * a + 1) * n, 0:n] = real.astype(jnp.bfloat16)
        left[2 * a * n : (2 * a + 1) * n, n : 2 * n] = (-imag).astype(jnp.bfloat16)
        left[(2 * a + 1) * n : (2 * a + 2) * n, 0:n] = imag.astype(jnp.bfloat16)
        left[(2 * a + 1) * n : (2 * a + 2) * n, n : 2 * n] = real.astype(jnp.bfloat16)
        c, s = cos_sin(defocus_ref[a] * (q * q))
        for j in range(pairs):
            col_cos[j, a] = c[:, j * 2 * n : (j + 1) * 2 * n]
            col_sin[j, a] = s[:, j * 2 * n : (j + 1) * 2 * n]

    @pl.when(held)
    def _():
        pl.semaphore_wait(ready.at[1], 1)
        for k in range(pairs):
            z_copy(k).start()

    def plan_of(direction, layer):
        row_steps, col_steps = off_ref[direction, 0, layer], off_ref[direction, 1, layer]
        fy = (row_steps & (QUANT - 1)).astype(jnp.float32) * (1.0 / QUANT)
        fx = (col_steps & (QUANT - 1)).astype(jnp.float32) * (1.0 / QUANT)
        down = lax.shift_right_logical(row_steps, 2)
        over = lax.shift_right_logical(col_steps, 2) & (n - 1)
        begin = lax.shift_right_logical(col_steps, n.bit_length() + 1)
        return down, fy, over, fx, begin

    @pl.when(is_front)
    def _():
        plans = [
            plan_of(place, layer)
            for layer in (front, back, far_front, far_back)
        ]
        for slot, (down, fy, over, fx, _) in enumerate(plans):
            front_slide[slot] = taps((3 * n, 2 * n), over, fx, 0, 1)
            for reach in range(REACH + 1):
                front_mix[reach * n : (reach + 1) * n, slot * n : (slot + 1) * n] = taps(
                    (n, n), down - reach * n, fy, 1, 0
                )

        def shift(slot, block_of):
            begin = plans[slot][4]

            def step(g, carry):
                rows = []
                for j in range(GROUP):
                    at = begin + 2 * (g * GROUP + j)
                    rows.append(
                        jnp.concatenate([block_of((at + b) & (blocks - 1)) for b in range(3)], 1)
                    )
                total = jnp.dot(
                    jnp.concatenate(rows, 0), front_slide[slot], preferred_element_type=jnp.float32
                ).astype(jnp.bfloat16)
                for j in range(GROUP):
                    mixed[g * GROUP + j, slot * n : (slot + 1) * n, :] = total[j * n : (j + 1) * n]
                return carry

            lax.fori_loop(0, pairs // GROUP, step, 0)

        shift(0, lambda b: own[b])
        twin_copy.wait_recv()
        shift(1, lambda b: twin[b])
        far_both.wait_recv()
        @pl.when(first)
        def _():
            pl.semaphore_wait(ready.at[0], 1)

        def send_pair(j):
            for b in range(2):
                x_copy(2 * j + b).start()

            @pl.when(odd == 0)
            def _():
                for b in range(2):
                    down_copy(2 * j + b).start()

        def give_step(g, carry):
            for side in range(2):
                begin = plans[2 + side][4] + 2 * PACE * g
                rows = []
                for j in range(PACE):
                    rows.append(
                        jnp.concatenate(
                            [far[side, (begin + 2 * j + b) & (blocks - 1)] for b in range(3)], 1
                        )
                    )
                total = jnp.dot(
                    jnp.concatenate(rows, 0), front_slide[2 + side], preferred_element_type=jnp.float32
                ).astype(jnp.bfloat16)
                for j in range(PACE):
                    mixed[g * PACE + j, (2 + side) * n : (3 + side) * n, :] = total[j * n : (j + 1) * n]
            for i in range(PACE):
                j = g * PACE + i
                total = jnp.dot(front_mix[...], mixed[j], preferred_element_type=jnp.float32)
                local[j] = total[:n]
                tail[j] = total[2 * n :]
                for b in range(2):
                    part = slice(b * n, (b + 1) * n)
                    x_buf[2 * j + b] = total[n : 2 * n, part].astype(jnp.bfloat16)
                    out_buf[2 * j + b] = total[2 * n :, part].astype(jnp.bfloat16)
            @pl.when(g > 0)
            def _():
                send_pair(g * PACE - 1)

            for j in range(PACE - 1):
                send_pair(g * PACE + j)
            return carry

        lax.fori_loop(0, pairs // PACE, give_step, 0)


        @pl.when(odd == 1)
        def _():
            pass_on(0)
            for b in range(2):
                x_copy(blocks - 2 + b).start()

            def step(j, carry):
                pass_on(j)
                return carry

            lax.fori_loop(1, ahead, step, 0)

    @pl.when(is_back)
    def _():
        plans = [
            [plan_of(direction, layer) for layer in (front, back)]
            for direction in (far_back, place)
        ]
        for index in range(2):
            for slot in range(2):
                down, fy, over, fx, _ = plans[index][slot]
                back_mix[slot, index * n : (index + 1) * n, :] = taps((n, 3 * n), down, fy, 1, 0)
                back_slide[index, slot * 3 * n : (slot + 1) * 3 * n, :] = taps(
                    (3 * n, 2 * n), over, fx, 0, 1
                )
        twin_copy.wait_recv()

        lead = jnp.where(last & (odd == 0), LEAD, 0)

        def take(k, layer):
            z_copy(k, layer).wait_recv()

            @pl.when((odd == 0) & (k < straight))
            def _():
                relay(k, layer).start()

        def lead_step(k, carry):
            take(k, 1)
            return carry

        lax.fori_loop(0, lead, lead_step, 0)

        @pl.when(odd == 1)
        def _():
            detour_both.wait_recv()
            for k in range(straight, pairs):
                onward(k).start()

        def rows_step(j, carry):
            take(j, 0)

            @pl.when(j + lead < pairs)
            def _():
                take(j + lead, 1)

            h_both(j).wait_recv()
            for layer in range(2):
                nearest = twin if layer == 0 else own
                window = jnp.concatenate(
                    [
                        jnp.concatenate(
                            [nearest[2 * j + b], halo[layer, 0, 2 * j + b], halo[layer, 1, 2 * j + b]], 0
                        )
                        for b in range(2)
                    ],
                    1,
                )
                total = jnp.dot(
                    back_mix[layer], window, preferred_element_type=jnp.float32
                ).astype(jnp.bfloat16)
                for index in range(2):
                    for b in range(2):
                        moved[layer, index, 2 * j + b] = total[
                            index * n : (index + 1) * n, b * n : (b + 1) * n
                        ]
            return carry

        lax.fori_loop(0, pairs, rows_step, 0)

        def cols(index, g, size):
            rows = []
            for j in range(size):
                parts = []
                for layer in range(2):
                    begin = plans[index][layer][4] + 2 * (g * size + j)
                    for b in range(3):
                        parts.append(moved[layer, index, (begin + b) & (blocks - 1)])
                rows.append(jnp.concatenate(parts, 1))
            return jnp.dot(
                jnp.concatenate(rows, 0), back_slide[index], preferred_element_type=jnp.float32
            )

        def send_pair(j):
            for b in range(2):
                across_copy(2 * j + b).start()

        def give_step(g, carry):
            total = cols(0, g, PACE).astype(jnp.bfloat16)
            for j in range(PACE):
                for b in range(2):
                    out_buf[2 * (g * PACE + j) + b] = total[j * n : (j + 1) * n, b * n : (b + 1) * n]

            @pl.when(g > 0)
            def _():
                send_pair(g * PACE - 1)

            for j in range(PACE - 1):
                send_pair(g * PACE + j)
            return carry

        lax.fori_loop(0, pairs // PACE, give_step, 0)

        def keep_step(g, carry):
            total = cols(1, g, BATCH)
            for j in range(BATCH):
                local[g * BATCH + j] = total[j * n : (j + 1) * n]

            @pl.when(g == 0)
            def _():
                send_pair(pairs - 1)

            return carry

        lax.fori_loop(0, pairs // BATCH, keep_step, 0)

    def field_of(j):
        arrived = jnp.concatenate([in_buf[2 * j + b].astype(jnp.float32) for b in range(2)], 1)
        c, s = cos_sin(local[j] + arrived)
        return jnp.concatenate([c, s], 0).astype(jnp.bfloat16)

    def spots(j, field):
        focal = jnp.dot(left[...], field, preferred_element_type=jnp.float32)
        fields = []
        for a in range(slices):
            real, imag = focal[2 * a * n : (2 * a + 1) * n], focal[(2 * a + 1) * n : (2 * a + 2) * n]
            c, s = col_cos[j, a][0:1], col_sin[j, a][0:1]
            new_real = (real * c - imag * s).astype(jnp.bfloat16)
            new_imag = (real * s + imag * c).astype(jnp.bfloat16)
            for b in range(2):
                fields.append(
                    jnp.concatenate([new_real[:, b * n : (b + 1) * n], new_imag[:, b * n : (b + 1) * n]], 1)
                )
        spot = jnp.dot(jnp.concatenate(fields, 0), right_tab[...], preferred_element_type=jnp.float32)
        power = spot * spot
        for b in range(2):
            total = 0.0
            for a in range(slices):
                piece = power[(2 * a + b) * n : (2 * a + b + 1) * n]
                total = total + (piece[:, :n] + piece[:, n:])
            lit = valid_ref[0, 2 * j + b].astype(jnp.float32)
            out_ref[0, 0, :, pl.ds(pl.multiple_of((2 * j + b) * n, n), n)] = (total * lit).astype(
                jnp.bfloat16
            )

    passing = is_front & (odd == 1)

    @pl.when(jnp.logical_not(passing))
    def _():
        def final_step(j, carry):
            @pl.when(is_front)
            def _():
                for b in range(2):
                    x_copy(2 * j + b).wait_recv()
                    part = slice(b * n, (b + 1) * n)
                    local[j, :, part] = local[j, :, part] + x_in[2 * j + b].astype(jnp.float32)

                @pl.when(j == 0)
                def _():
                    for b in range(2):
                        x_copy(blocks - 2 + b).start()
                        down_copy(blocks - 2 + b).start()

            await_in(j)
            spots(j, field_of(j))
            return carry

        lax.fori_loop(0, pairs, final_step, 0, unroll=2)

    @pl.when(passing)
    def _():
        @pl.when(jnp.logical_not(first))
        def _():
            down_copy(blocks - 1).start()

        await_in(0)
        field_buf[0] = field_of(0)

        def final_step(i, carry):
            j = 2 * i

            @pl.when(j + ahead < pairs)
            def _():
                pass_on(j + ahead)

            await_in(j + 1)
            field_buf[1] = field_of(j + 1)
            spots(j, field_buf[0])

            @pl.when(j + 1 + ahead < pairs)
            def _():
                pass_on(j + 1 + ahead)

            await_in(j + 2)

            @pl.when((j == 0) & first)
            def _():
                down_copy(blocks - 1).start()

            field_buf[0] = field_of(j + 2)
            spots(j + 1, field_buf[1])
            return carry

        lax.fori_loop(0, pairs // 2 - 1, final_step, 0)
        await_in(pairs - 1)
        field_buf[1] = field_of(pairs - 1)
        spots(pairs - 2, field_buf[0])
        spots(pairs - 1, field_buf[1])

    z_all.wait_send()
    far_copy.wait_send()
    twin_copy.wait_send()
    out_all.wait_send()

    @pl.when(odd == 1)
    def _():
        f_all.wait_send()

    @pl.when(is_front)
    def _():
        x_all.wait_send()

    @pl.when(odd == 0)
    def _():
        detour().wait_send()

    @pl.when(is_back & (odd == 0))
    def _():
        r_all.wait_send()

    @pl.when(is_back & (odd == 1))
    def _():
        onward_all.wait_send()


def solution(mesh):
    tiles = mesh.shape["tile"]

    def shards(layers, offsets, subap_valid, defocus, weights):
        n, cols = layers.shape[1], layers.shape[2]
        blocks = cols // n
        slices = defocus.shape[0]
        pairs = blocks // 2
        fr, fi = base_tables(n)
        right = jnp.asarray(np.block([[fr.T, fi.T], [-fi.T, fr.T]])).astype(jnp.bfloat16)
        vmem = pl.BlockSpec(memory_space=pltpu.VMEM)
        hbm = pl.BlockSpec(memory_space=pl.ANY)
        dma = pltpu.SemaphoreType.DMA
        half, full = jnp.bfloat16, jnp.float32
        return pl.pallas_call(
            functools.partial(kernel, tiles, n, blocks, slices),
            out_shape=pltpu.VMEM((1, 1, n, cols), half),
            in_specs=[hbm] * 7,
            out_specs=vmem,
            scratch_shapes=[
                pltpu.SMEM((4, 2, 4), jnp.int32),
                pltpu.SMEM((1, blocks), jnp.int32),
                pltpu.SMEM((slices,), full),
                pltpu.SMEM((slices,), full),
                pltpu.VMEM((blocks, n, n), half),
                pltpu.VMEM((blocks, n, n), half),
                pltpu.VMEM((2, blocks, n, n), half),
                pltpu.VMEM((2, REACH, blocks, n, n), half),
                pltpu.VMEM((2, 2 * DETOUR, n, n), half),
                pltpu.VMEM((pairs, 4 * n, 2 * n), half),
                pltpu.VMEM((2, 2, blocks, n, n), half),
                pltpu.VMEM(((REACH + 1) * n, 4 * n), half),
                pltpu.VMEM((4, 3 * n, 2 * n), half),
                pltpu.VMEM((2, 2 * n, (REACH + 1) * n), half),
                pltpu.VMEM((2, 6 * n, 2 * n), half),
                pltpu.VMEM((blocks, n, n), half),
                pltpu.VMEM((blocks, n, n), half),
                pltpu.VMEM((pairs, n, 2 * n), full),
                pltpu.VMEM((blocks, n, n), half),
                pltpu.VMEM((blocks, n, n), half),
                pltpu.VMEM((pairs, n, 2 * n), full),
                pltpu.VMEM((2 * slices * n, 2 * n), half),
                pltpu.VMEM((pairs, slices, 8, 2 * n), full),
                pltpu.VMEM((pairs, slices, 8, 2 * n), full),
                pltpu.VMEM((2, n, n), full),
                pltpu.VMEM((2 * n, 2 * n), half),
                pltpu.VMEM((2, 2 * n, 2 * n), half),
                dma, dma((6,)),
                dma, dma((2, pairs)), dma, dma, dma((pairs,)),
                dma, dma, dma, dma,
                dma, dma((blocks,)), dma, dma((pairs,)), dma, dma,
                pltpu.SemaphoreType.REGULAR((2,)),
            ],
            compiler_params=pltpu.CompilerParams(collective_id=0, has_side_effects=True),
        )(layers, jnp.transpose(offsets, (0, 2, 1)), subap_valid, defocus, weights, jnp.asarray(np.stack([fr, fi])), right)

    placed = (P("dir", "tile", None), P(), P("tile", None), P(), P())
    return jax.shard_map(
        shards, mesh=mesh, in_specs=placed, out_specs=P("dir", "tile", None, None), check_vma=False
    )
```

```python
import functools
import math

import jax
import jax.numpy as jnp
import numpy as np
from jax import lax
from jax.experimental import pallas as pl
from jax.experimental.pallas import tpu as pltpu
from jax.sharding import PartitionSpec as P

OVER = 2
QUANT = 4
REACH = 2
GROUP = 8
BATCH = 4
LEAD = 3
PACE = 2
STRIDE = 2
EARLY = 2
DETOUR = 2
MESH = pl.DeviceIdType.MESH
SIN = (3.141582022082025, -5.167142794167084, 2.541899009948703, -0.5546361567315732)
COS = (0.999999953466345, -4.934792858633932, 4.058411913339297, -1.3318801559459539, 0.21969678799073292)


def base_tables(n):
    frequency = np.arange(n, dtype=np.float64) - n // 2
    position = np.arange(n, dtype=np.float64) - (n - 1) / 2.0
    angle = -2.0 * math.pi / (OVER * n) * frequency[:, None] * position[None, :]
    factor = 1.0 / math.sqrt(n)
    return (np.cos(angle) * factor).astype(np.float32), (np.sin(angle) * factor).astype(np.float32)


def cos_sin(angle):
    turns = angle * (1.0 / math.pi)
    whole = jnp.round(turns)
    rest = turns - whole
    sign = jnp.where((whole.astype(jnp.int32) & 1) == 0, 1.0, -1.0)
    square = rest * rest
    sin, cos = SIN[-1], COS[-1]
    for factor in SIN[-2::-1]:
        sin = factor + square * sin
    for factor in COS[-2::-1]:
        cos = factor + square * cos
    return cos * sign, sin * (rest * sign)


def taps(shape, shift, fraction, along, across):
    gap = lax.broadcasted_iota(jnp.int32, shape, along) - lax.broadcasted_iota(
        jnp.int32, shape, across
    ) - shift
    return jnp.where(gap == 0, 1.0 - fraction, jnp.where(gap == 1, fraction, 0.0)).astype(
        jnp.bfloat16
    )


def kernel(
    tiles, n, blocks, slices,
    x_ref, off_hbm, valid_hbm, defocus_hbm, weights_hbm, base_ref, right_ref,
    out_ref,
    off_ref, valid_ref, defocus_ref, weights_ref, own, twin, far, halo, via, mixed, moved, front_mix, front_slide, back_mix, back_slide,
    x_buf, x_in, tail, out_buf, in_buf, local, left, col_cos, col_sin, base_tab, right_tab, field_buf,
    load_sem, table_sem, z_send, z_recv, f_send, r_send, h_recv, y_send, y_recv, t_send, t_recv,
    x_send, x_recv, o_send, o_recv, v_send, v_recv, ready,
):
    tile = lax.axis_index("tile")
    place = lax.axis_index("dir")
    core = lax.rem(place, 2)
    chip = lax.div(place, 2)
    partner = chip * 2 + (1 - core)
    front, back = chip * 2, chip * 2 + 1
    far_front, far_back = (1 - chip) * 2, (1 - chip) * 2 + 1
    odd = lax.rem(tile, 2)
    mate = tile + 1 - 2 * odd
    below = lax.rem(tile + tiles - 2, tiles)
    above = lax.rem(tile + 2, tiles)
    pairs = blocks // 2
    is_front, is_back = core == 0, core == 1

    first, last = tile < 2, tile >= tiles - 2
    ahead = jnp.where(first, pairs - EARLY, pairs)

    barrier = pltpu.get_barrier_semaphore()

    def greet(device):
        pl.semaphore_signal(barrier, inc=1, device_id=device, device_id_type=MESH)

    @pl.when(is_back)
    def _():
        greet((above, back))

    @pl.when(jnp.logical_not(last))
    def _():
        greet((above, front))

    @pl.when(first & is_front)
    def _():
        greet((below, back))
        greet((below, front))

    @pl.when(is_front)
    def _():
        greet((tile, far_back))

    @pl.when(is_back)
    def _():
        greet((mate, front))

    greet((mate, front + core))
    greet((tile, far_front + core))
    greet((tile, partner))

    for k in range(blocks):
        pltpu.make_async_copy(x_ref.at[0, :, pl.ds(k * n, n)], own.at[k], load_sem).start()
    tables = [
        pltpu.make_async_copy(source, target, table_sem.at[i])
        for i, (source, target) in enumerate(
            (
                (defocus_hbm, defocus_ref), (off_hbm, off_ref), (weights_hbm, weights_ref),
                (valid_hbm, valid_ref), (base_ref, base_tab), (right_ref, right_tab),
            )
        )
    ]
    for table in tables:
        table.start()

    def copy(source, target, send, recv, device):
        return pltpu.make_async_remote_copy(
            src_ref=source, dst_ref=target, send_sem=send, recv_sem=recv,
            device_id=device, device_id_type=MESH,
        )

    def pair_of(k):
        return pl.ds(2 * k, 2)

    def z_copy(k, layer=core):
        return copy(
            own.at[pair_of(k)], halo.at[layer, 1, pair_of(k)], z_send, z_recv.at[layer, k],
            (below, back),
        )

    def f_copy(k):
        return copy(
            own.at[pair_of(k)], halo.at[core, 0, pair_of(k)], f_send, h_recv.at[k], (mate, back)
        )

    def relay(k, layer):
        return copy(
            halo.at[layer, 1, pair_of(k)], halo.at[layer, 0, pair_of(k)], r_send, h_recv.at[k],
            (mate, back),
        )

    def h_both(k):
        part = halo.at[:, 0, pair_of(k)]
        return copy(part, part, r_send, h_recv.at[k], (mate, back))

    straight = pairs - DETOUR
    rest = pl.ds(2 * straight, 2 * DETOUR)

    def detour(layer=core):
        return copy(own.at[rest], via.at[layer], v_send, v_recv, (mate, back))

    detour_both = copy(via, via, v_send, v_recv, (mate, back))

    def onward(k):
        part = pl.ds(2 * (k - straight), 2)
        return copy(
            via.at[:, part], halo.at[:, 0, pair_of(k)], r_send, h_recv.at[k], (below, back)
        )

    z_all = copy(own, halo.at[core, 1], z_send, z_recv.at[0, 0], (below, back))
    f_all = copy(own, halo.at[core, 0], f_send, h_recv.at[0], (mate, back))
    before = pl.ds(0, 2 * straight)
    r_all = copy(halo.at[:, 1, before], halo.at[:, 0, before], r_send, h_recv.at[0], (mate, back))
    onward_all = copy(via, via, r_send, h_recv.at[0], (below, back))
    far_copy = copy(own, far.at[core], y_send, y_recv, (tile, far_front))
    far_both = copy(far, far, y_send, y_recv, (tile, far_front))

    twin_copy = copy(own, twin, t_send, t_recv, (tile, partner))

    def x_copy(j):
        return copy(x_buf.at[j], x_in.at[j], x_send, x_recv.at[lax.div(j, 2)], (mate, front))

    def await_x(j):
        part = pair_of(j)
        copy(x_buf.at[part], x_in.at[part], x_send, x_recv.at[j], (mate, front)).wait_recv()

    def down_copy(j):
        return copy(out_buf.at[j], in_buf.at[j], o_send, o_recv.at[lax.div(j, 2)], (below, front))

    def pass_on(j):
        await_x(j)
        for b in range(2):
            k = 2 * j + b
            out_buf[k] = (
                tail[j, :, b * n : (b + 1) * n] + x_in[k].astype(jnp.float32)
            ).astype(jnp.bfloat16)

            @pl.when(k > 0)
            def _():
                down_copy(k - 1).start()

    def across_copy(j):
        return copy(
            out_buf.at[j], in_buf.at[j], o_send, o_recv.at[lax.div(j, 2)], (tile, far_back)
        )

    def await_in(j):
        part = pair_of(j)
        copy(out_buf.at[part], in_buf.at[part], o_send, o_recv.at[j], (tile, far_back)).wait_recv()

    x_all = copy(x_buf, x_in, x_send, x_recv.at[0], (mate, front))
    out_all = copy(out_buf, in_buf, o_send, o_recv.at[0], (tile, far_back))

    held = first & is_front
    pl.semaphore_wait(
        barrier,
        5 + jnp.where(is_front, 1, 0) - jnp.where(held, 2, 0) + jnp.where(last, 1, 0),
    )

    @pl.when(last)
    def _():
        pl.semaphore_signal(
            ready.at[core], inc=1, device_id=(above, front), device_id_type=MESH
        )

    pltpu.make_async_copy(twin, own, load_sem).wait()
    far_copy.start()
    @pl.when(odd == 0)
    def _():
        detour().start()

    @pl.when(jnp.logical_not(held))
    def _():
        for k in range(pairs):
            z_copy(k).start()

    @pl.when(odd == 1)
    def _():
        for k in range(pairs):
            f_copy(k).start()

    twin_copy.start()
    for table in tables:
        table.wait()

    first_row = (tile * n).astype(jnp.float32)
    row_at = lax.broadcasted_iota(jnp.int32, (8, n), 1).astype(jnp.float32)
    p = (first_row + row_at - (tiles * n - 1) / 2.0) / n
    col_at = lax.broadcasted_iota(jnp.int32, (8, blocks * n), 1).astype(jnp.float32)
    q = (col_at - (blocks * n - 1) / 2.0) / n
    weight_sum = weights_ref[0]
    for a in range(1, slices):
        weight_sum = weight_sum + weights_ref[a]
    for a in range(slices):
        row_cos, row_sin = cos_sin(defocus_ref[a] * (p * p))
        share = jnp.sqrt(jnp.full((8, n), weights_ref[a], jnp.float32) / weight_sum)
        row_cos, row_sin = (row_cos * share)[0:1], (row_sin * share)[0:1]
        real = base_tab[0] * row_cos - base_tab[1] * row_sin
        imag = base_tab[0] * row_sin + base_tab[1] * row_cos
        left[2 * a * n : (2 * a + 1) * n, 0:n] = real.astype(jnp.bfloat16)
        left[2 * a * n : (2 * a + 1) * n, n : 2 * n] = (-imag).astype(jnp.bfloat16)
        left[(2 * a + 1) * n : (2 * a + 2) * n, 0:n] = imag.astype(jnp.bfloat16)
        left[(2 * a + 1) * n : (2 * a + 2) * n, n : 2 * n] = real.astype(jnp.bfloat16)
        c, s = cos_sin(defocus_ref[a] * (q * q))
        for j in range(pairs):
            col_cos[j, a] = c[:, j * 2 * n : (j + 1) * 2 * n]
            col_sin[j, a] = s[:, j * 2 * n : (j + 1) * 2 * n]

    @pl.when(held)
    def _():
        pl.semaphore_wait(ready.at[1], 1)
        for k in range(pairs):
            z_copy(k).start()

    def plan_of(direction, layer):
        row_steps, col_steps = off_ref[direction, 0, layer], off_ref[direction, 1, layer]
        fy = (row_steps & (QUANT - 1)).astype(jnp.float32) * (1.0 / QUANT)
        fx = (col_steps & (QUANT - 1)).astype(jnp.float32) * (1.0 / QUANT)
        down = lax.shift_right_logical(row_steps, 2)
        over = lax.shift_right_logical(col_steps, 2) & (n - 1)
        begin = lax.shift_right_logical(col_steps, n.bit_length() + 1)
        return down, fy, over, fx, begin

    @pl.when(is_front)
    def _():
        plans = [
            plan_of(place, layer)
            for layer in (front, back, far_front, far_back)
        ]
        for slot, (down, fy, over, fx, _) in enumerate(plans):
            front_slide[slot] = taps((3 * n, 2 * n), over, fx, 0, 1)
            for reach in range(REACH + 1):
                front_mix[reach * n : (reach + 1) * n, slot * n : (slot + 1) * n] = taps(
                    (n, n), down - reach * n, fy, 1, 0
                )

        def shift(slot, block_of):
            begin = plans[slot][4]

            def step(g, carry):
                rows = []
                for j in range(GROUP):
                    at = begin + 2 * (g * GROUP + j)
                    rows.append(
                        jnp.concatenate([block_of((at + b) & (blocks - 1)) for b in range(3)], 1)
                    )
                total = jnp.dot(
                    jnp.concatenate(rows, 0), front_slide[slot], preferred_element_type=jnp.float32
                ).astype(jnp.bfloat16)
                for j in range(GROUP):
                    mixed[g * GROUP + j, slot * n : (slot + 1) * n, :] = total[j * n : (j + 1) * n]
                return carry

            lax.fori_loop(0, pairs // GROUP, step, 0)

        shift(0, lambda b: own[b])
        twin_copy.wait_recv()
        shift(1, lambda b: twin[b])
        far_both.wait_recv()
        @pl.when(first)
        def _():
            pl.semaphore_wait(ready.at[0], 1)

        def send_pair(j):
            for b in range(2):
                x_copy(2 * j + b).start()

            @pl.when(odd == 0)
            def _():
                for b in range(2):
                    down_copy(2 * j + b).start()

        def give_step(g, carry):
            for side in range(2):
                begin = plans[2 + side][4] + 2 * PACE * g
                rows = []
                for j in range(PACE):
                    rows.append(
                        jnp.concatenate(
                            [far[side, (begin + 2 * j + b) & (blocks - 1)] for b in range(3)], 1
                        )
                    )
                total = jnp.dot(
                    jnp.concatenate(rows, 0), front_slide[2 + side], preferred_element_type=jnp.float32
                ).astype(jnp.bfloat16)
                for j in range(PACE):
                    mixed[g * PACE + j, (2 + side) * n : (3 + side) * n, :] = total[j * n : (j + 1) * n]
            for i in range(PACE):
                j = g * PACE + i
                total = jnp.dot(front_mix[...], mixed[j], preferred_element_type=jnp.float32)
                local[j] = total[:n]
                tail[j] = total[2 * n :]
                for b in range(2):
                    part = slice(b * n, (b + 1) * n)
                    x_buf[2 * j + b] = total[n : 2 * n, part].astype(jnp.bfloat16)
                    out_buf[2 * j + b] = total[2 * n :, part].astype(jnp.bfloat16)
            @pl.when(g > 0)
            def _():
                send_pair(g * PACE - 1)

            for j in range(PACE - 1):
                send_pair(g * PACE + j)
            return carry

        lax.fori_loop(0, pairs // PACE, give_step, 0)


        @pl.when(odd == 1)
        def _():
            pass_on(0)
            for b in range(2):
                x_copy(blocks - 2 + b).start()

            def step(j, carry):
                pass_on(j)
                return carry

            lax.fori_loop(1, ahead, step, 0)

    @pl.when(is_back)
    def _():
        plans = [
            [plan_of(direction, layer) for layer in (front, back)]
            for direction in (far_back, place)
        ]
        for index in range(2):
            for slot in range(2):
                down, fy, over, fx, _ = plans[index][slot]
                back_mix[slot, index * n : (index + 1) * n, :] = taps((n, 3 * n), down, fy, 1, 0)
                back_slide[index, slot * 3 * n : (slot + 1) * 3 * n, :] = taps(
                    (3 * n, 2 * n), over, fx, 0, 1
                )
        twin_copy.wait_recv()

        lead = jnp.where(last & (odd == 0), LEAD, 0)

        def take(k, layer):
            z_copy(k, layer).wait_recv()

            @pl.when((odd == 0) & (k < straight))
            def _():
                relay(k, layer).start()

        def lead_step(k, carry):
            take(k, 1)
            return carry

        lax.fori_loop(0, lead, lead_step, 0)

        @pl.when(odd == 1)
        def _():
            detour_both.wait_recv()
            for k in range(straight, pairs):
                onward(k).start()

        def rows_step(j, carry):
            take(j, 0)

            @pl.when(j + lead < pairs)
            def _():
                take(j + lead, 1)

            h_both(j).wait_recv()
            for layer in range(2):
                nearest = twin if layer == 0 else own
                window = jnp.concatenate(
                    [
                        jnp.concatenate(
                            [nearest[2 * j + b], halo[layer, 0, 2 * j + b], halo[layer, 1, 2 * j + b]], 0
                        )
                        for b in range(2)
                    ],
                    1,
                )
                total = jnp.dot(
                    back_mix[layer], window, preferred_element_type=jnp.float32
                ).astype(jnp.bfloat16)
                for index in range(2):
                    for b in range(2):
                        moved[layer, index, 2 * j + b] = total[
                            index * n : (index + 1) * n, b * n : (b + 1) * n
                        ]
            return carry

        lax.fori_loop(0, pairs, rows_step, 0)

        def cols(index, g, size):
            rows = []
            for j in range(size):
                parts = []
                for layer in range(2):
                    begin = plans[index][layer][4] + 2 * (g * size + j)
                    for b in range(3):
                        parts.append(moved[layer, index, (begin + b) & (blocks - 1)])
                rows.append(jnp.concatenate(parts, 1))
            return jnp.dot(
                jnp.concatenate(rows, 0), back_slide[index], preferred_element_type=jnp.float32
            )

        def send_pair(j):
            for b in range(2):
                across_copy(2 * j + b).start()

        def give_step(g, carry):
            total = cols(0, g, STRIDE).astype(jnp.bfloat16)
            for j in range(STRIDE):
                for b in range(2):
                    out_buf[2 * (g * STRIDE + j) + b] = total[j * n : (j + 1) * n, b * n : (b + 1) * n]

            @pl.when(g > 0)
            def _():
                send_pair(g * STRIDE - 1)

            for j in range(STRIDE - 1):
                send_pair(g * STRIDE + j)
            return carry

        lax.fori_loop(0, pairs // STRIDE, give_step, 0)

        def keep_step(g, carry):
            total = cols(1, g, BATCH)
            for j in range(BATCH):
                local[g * BATCH + j] = total[j * n : (j + 1) * n]

            @pl.when(g == 0)
            def _():
                send_pair(pairs - 1)

            return carry

        lax.fori_loop(0, pairs // BATCH, keep_step, 0)

    def field_of(j):
        arrived = jnp.concatenate([in_buf[2 * j + b].astype(jnp.float32) for b in range(2)], 1)
        c, s = cos_sin(local[j] + arrived)
        return jnp.concatenate([c, s], 0).astype(jnp.bfloat16)

    def spots(j, field):
        focal = jnp.dot(left[...], field, preferred_element_type=jnp.float32)
        fields = []
        for a in range(slices):
            real, imag = focal[2 * a * n : (2 * a + 1) * n], focal[(2 * a + 1) * n : (2 * a + 2) * n]
            c, s = col_cos[j, a][0:1], col_sin[j, a][0:1]
            new_real = (real * c - imag * s).astype(jnp.bfloat16)
            new_imag = (real * s + imag * c).astype(jnp.bfloat16)
            for b in range(2):
                fields.append(
                    jnp.concatenate([new_real[:, b * n : (b + 1) * n], new_imag[:, b * n : (b + 1) * n]], 1)
                )
        spot = jnp.dot(jnp.concatenate(fields, 0), right_tab[...], preferred_element_type=jnp.float32)
        power = spot * spot
        for b in range(2):
            total = 0.0
            for a in range(slices):
                piece = power[(2 * a + b) * n : (2 * a + b + 1) * n]
                total = total + (piece[:, :n] + piece[:, n:])
            lit = valid_ref[0, 2 * j + b].astype(jnp.float32)
            out_ref[0, 0, :, pl.ds(pl.multiple_of((2 * j + b) * n, n), n)] = (total * lit).astype(
                jnp.bfloat16
            )

    passing = is_front & (odd == 1)

    @pl.when(jnp.logical_not(passing))
    def _():
        def final_step(j, carry):
            @pl.when(is_front)
            def _():
                await_x(j)
                for b in range(2):
                    part = slice(b * n, (b + 1) * n)
                    local[j, :, part] = local[j, :, part] + x_in[2 * j + b].astype(jnp.float32)

                @pl.when(j == 0)
                def _():
                    for b in range(2):
                        x_copy(blocks - 2 + b).start()
                        down_copy(blocks - 2 + b).start()

            await_in(j)
            spots(j, field_of(j))
            return carry

        lax.fori_loop(0, pairs, final_step, 0, unroll=2)

    @pl.when(passing)
    def _():
        @pl.when(jnp.logical_not(first))
        def _():
            down_copy(blocks - 1).start()

        await_in(0)
        field_buf[0] = field_of(0)

        def final_step(i, carry):
            j = 2 * i

            @pl.when(j + ahead < pairs)
            def _():
                pass_on(j + ahead)

            await_in(j + 1)
            field_buf[1] = field_of(j + 1)
            spots(j, field_buf[0])

            @pl.when(j + 1 + ahead < pairs)
            def _():
                pass_on(j + 1 + ahead)

            await_in(j + 2)

            @pl.when((j == 0) & first)
            def _():
                down_copy(blocks - 1).start()

            field_buf[0] = field_of(j + 2)
            spots(j + 1, field_buf[1])
            return carry

        lax.fori_loop(0, pairs // 2 - 1, final_step, 0)
        await_in(pairs - 1)
        field_buf[1] = field_of(pairs - 1)
        spots(pairs - 2, field_buf[0])
        spots(pairs - 1, field_buf[1])

    z_all.wait_send()
    far_copy.wait_send()
    twin_copy.wait_send()
    out_all.wait_send()

    @pl.when(odd == 1)
    def _():
        f_all.wait_send()

    @pl.when(is_front)
    def _():
        x_all.wait_send()

    @pl.when(odd == 0)
    def _():
        detour().wait_send()

    @pl.when(is_back & (odd == 0))
    def _():
        r_all.wait_send()

    @pl.when(is_back & (odd == 1))
    def _():
        onward_all.wait_send()


def solution(mesh):
    tiles = mesh.shape["tile"]

    def shards(layers, offsets, subap_valid, defocus, weights):
        n, cols = layers.shape[1], layers.shape[2]
        blocks = cols // n
        slices = defocus.shape[0]
        pairs = blocks // 2
        fr, fi = base_tables(n)
        right = jnp.asarray(np.block([[fr.T, fi.T], [-fi.T, fr.T]])).astype(jnp.bfloat16)
        vmem = pl.BlockSpec(memory_space=pltpu.VMEM)
        hbm = pl.BlockSpec(memory_space=pl.ANY)
        dma = pltpu.SemaphoreType.DMA
        half, full = jnp.bfloat16, jnp.float32
        return pl.pallas_call(
            functools.partial(kernel, tiles, n, blocks, slices),
            out_shape=pltpu.VMEM((1, 1, n, cols), half),
            in_specs=[hbm] * 7,
            out_specs=vmem,
            scratch_shapes=[
                pltpu.SMEM((4, 2, 4), jnp.int32),
                pltpu.SMEM((1, blocks), jnp.int32),
                pltpu.SMEM((slices,), full),
                pltpu.SMEM((slices,), full),
                pltpu.VMEM((blocks, n, n), half),
                pltpu.VMEM((blocks, n, n), half),
                pltpu.VMEM((2, blocks, n, n), half),
                pltpu.VMEM((2, REACH, blocks, n, n), half),
                pltpu.VMEM((2, 2 * DETOUR, n, n), half),
                pltpu.VMEM((pairs, 4 * n, 2 * n), half),
                pltpu.VMEM((2, 2, blocks, n, n), half),
                pltpu.VMEM(((REACH + 1) * n, 4 * n), half),
                pltpu.VMEM((4, 3 * n, 2 * n), half),
                pltpu.VMEM((2, 2 * n, (REACH + 1) * n), half),
                pltpu.VMEM((2, 6 * n, 2 * n), half),
                pltpu.VMEM((blocks, n, n), half),
                pltpu.VMEM((blocks, n, n), half),
                pltpu.VMEM((pairs, n, 2 * n), full),
                pltpu.VMEM((blocks, n, n), half),
                pltpu.VMEM((blocks, n, n), half),
                pltpu.VMEM((pairs, n, 2 * n), full),
                pltpu.VMEM((2 * slices * n, 2 * n), half),
                pltpu.VMEM((pairs, slices, 8, 2 * n), full),
                pltpu.VMEM((pairs, slices, 8, 2 * n), full),
                pltpu.VMEM((2, n, n), full),
                pltpu.VMEM((2 * n, 2 * n), half),
                pltpu.VMEM((2, 2 * n, 2 * n), half),
                dma, dma((6,)),
                dma, dma((2, pairs)), dma, dma, dma((pairs,)),
                dma, dma, dma, dma,
                dma, dma((pairs,)), dma, dma((pairs,)), dma, dma,
                pltpu.SemaphoreType.REGULAR((2,)),
            ],
            compiler_params=pltpu.CompilerParams(collective_id=0, has_side_effects=True),
        )(layers, jnp.transpose(offsets, (0, 2, 1)), subap_valid, defocus, weights, jnp.asarray(np.stack([fr, fi])), right)

    placed = (P("dir", "tile", None), P(), P("tile", None), P(), P())
    return jax.shard_map(
        shards, mesh=mesh, in_specs=placed, out_specs=P("dir", "tile", None, None), check_vma=False
    )
```

```python
import functools
import math

import jax
import jax.numpy as jnp
import numpy as np
from jax import lax
from jax.experimental import pallas as pl
from jax.experimental.pallas import tpu as pltpu
from jax.sharding import PartitionSpec as P

OVER = 2
QUANT = 4
REACH = 2
GROUP = 8
BATCH = 8
LEAD = 3
PACE = 2
EARLY = 2
DETOUR = 2
MESH = pl.DeviceIdType.MESH
SIN = (3.141582022082025, -5.167142794167084, 2.541899009948703, -0.5546361567315732)
COS = (0.999999953466345, -4.934792858633932, 4.058411913339297, -1.3318801559459539, 0.21969678799073292)


def base_tables(n):
    frequency = np.arange(n, dtype=np.float64) - n // 2
    position = np.arange(n, dtype=np.float64) - (n - 1) / 2.0
    angle = -2.0 * math.pi / (OVER * n) * frequency[:, None] * position[None, :]
    factor = 1.0 / math.sqrt(n)
    return (np.cos(angle) * factor).astype(np.float32), (np.sin(angle) * factor).astype(np.float32)


def cos_sin(angle):
    turns = angle * (1.0 / math.pi)
    whole = jnp.round(turns)
    rest = turns - whole
    sign = jnp.where((whole.astype(jnp.int32) & 1) == 0, 1.0, -1.0)
    square = rest * rest
    sin, cos = SIN[-1], COS[-1]
    for factor in SIN[-2::-1]:
        sin = factor + square * sin
    for factor in COS[-2::-1]:
        cos = factor + square * cos
    return cos * sign, sin * (rest * sign)


def taps(shape, shift, fraction, along, across):
    gap = lax.broadcasted_iota(jnp.int32, shape, along) - lax.broadcasted_iota(
        jnp.int32, shape, across
    ) - shift
    return jnp.where(gap == 0, 1.0 - fraction, jnp.where(gap == 1, fraction, 0.0)).astype(
        jnp.bfloat16
    )


def kernel(
    tiles, n, blocks, slices,
    x_ref, off_hbm, valid_hbm, defocus_hbm, weights_hbm, base_ref, right_ref,
    out_ref,
    off_ref, valid_ref, defocus_ref, weights_ref, own, twin, far, halo, via, mixed, moved, front_mix, front_slide, back_mix, back_slide,
    x_buf, x_in, tail, out_buf, in_buf, local, left, col_cos, col_sin, base_tab, right_tab, field_buf,
    load_sem, table_sem, z_send, z_recv, f_send, r_send, h_recv, y_send, y_recv, t_send, t_recv,
    x_send, x_recv, o_send, o_recv, v_send, v_recv, ready,
):
    tile = lax.axis_index("tile")
    place = lax.axis_index("dir")
    core = lax.rem(place, 2)
    chip = lax.div(place, 2)
    partner = chip * 2 + (1 - core)
    front, back = chip * 2, chip * 2 + 1
    far_front, far_back = (1 - chip) * 2, (1 - chip) * 2 + 1
    odd = lax.rem(tile, 2)
    mate = tile + 1 - 2 * odd
    below = lax.rem(tile + tiles - 2, tiles)
    above = lax.rem(tile + 2, tiles)
    pairs = blocks // 2
    is_front, is_back = core == 0, core == 1

    first, last = tile < 2, tile >= tiles - 2
    ahead = jnp.where(first, pairs - EARLY, pairs)

    barrier = pltpu.get_barrier_semaphore()

    def greet(device):
        pl.semaphore_signal(barrier, inc=1, device_id=device, device_id_type=MESH)

    @pl.when(is_back)
    def _():
        greet((above, back))

    @pl.when(jnp.logical_not(last))
    def _():
        greet((above, front))

    @pl.when(first & is_front)
    def _():
        greet((below, back))
        greet((below, front))

    @pl.when(is_front)
    def _():
        greet((tile, far_back))

    @pl.when(is_back)
    def _():
        greet((mate, front))

    greet((mate, front + core))
    greet((tile, far_front + core))
    greet((tile, partner))

    for k in range(blocks):
        pltpu.make_async_copy(x_ref.at[0, :, pl.ds(k * n, n)], own.at[k], load_sem).start()
    tables = [
        pltpu.make_async_copy(source, target, table_sem.at[i])
        for i, (source, target) in enumerate(
            (
                (defocus_hbm, defocus_ref), (off_hbm, off_ref), (weights_hbm, weights_ref),
                (valid_hbm, valid_ref), (base_ref, base_tab), (right_ref, right_tab),
            )
        )
    ]
    for table in tables:
        table.start()

    def copy(source, target, send, recv, device):
        return pltpu.make_async_remote_copy(
            src_ref=source, dst_ref=target, send_sem=send, recv_sem=recv,
            device_id=device, device_id_type=MESH,
        )

    def pair_of(k):
        return pl.ds(2 * k, 2)

    def z_copy(k, layer=core):
        return copy(
            own.at[pair_of(k)], halo.at[layer, 1, pair_of(k)], z_send, z_recv.at[layer, k],
            (below, back),
        )

    def f_copy(k):
        return copy(
            own.at[pair_of(k)], halo.at[core, 0, pair_of(k)], f_send, h_recv.at[k], (mate, back)
        )

    def relay(k, layer):
        return copy(
            halo.at[layer, 1, pair_of(k)], halo.at[layer, 0, pair_of(k)], r_send, h_recv.at[k],
            (mate, back),
        )

    def h_both(k):
        part = halo.at[:, 0, pair_of(k)]
        return copy(part, part, r_send, h_recv.at[k], (mate, back))

    straight = pairs - DETOUR
    rest = pl.ds(2 * straight, 2 * DETOUR)

    def detour(layer=core):
        return copy(own.at[rest], via.at[layer], v_send, v_recv, (mate, back))

    detour_both = copy(via, via, v_send, v_recv, (mate, back))

    def onward(k):
        part = pl.ds(2 * (k - straight), 2)
        return copy(
            via.at[:, part], halo.at[:, 0, pair_of(k)], r_send, h_recv.at[k], (below, back)
        )

    z_all = copy(own, halo.at[core, 1], z_send, z_recv.at[0, 0], (below, back))
    f_all = copy(own, halo.at[core, 0], f_send, h_recv.at[0], (mate, back))
    before = pl.ds(0, 2 * straight)
    r_all = copy(halo.at[:, 1, before], halo.at[:, 0, before], r_send, h_recv.at[0], (mate, back))
    onward_all = copy(via, via, r_send, h_recv.at[0], (below, back))
    far_copy = copy(own, far.at[core], y_send, y_recv, (tile, far_front))
    far_both = copy(far, far, y_send, y_recv, (tile, far_front))

    twin_copy = copy(own, twin, t_send, t_recv, (tile, partner))

    def x_copy(j):
        return copy(x_buf.at[j], x_in.at[j], x_send, x_recv.at[j], (mate, front))

    def down_copy(j):
        return copy(out_buf.at[j], in_buf.at[j], o_send, o_recv.at[lax.div(j, 2)], (below, front))

    def pass_on(j):
        for b in range(2):
            k = 2 * j + b
            x_copy(k).wait_recv()
            out_buf[k] = (
                tail[j, :, b * n : (b + 1) * n] + x_in[k].astype(jnp.float32)
            ).astype(jnp.bfloat16)

            @pl.when(k > 0)
            def _():
                down_copy(k - 1).start()

    def across_copy(j):
        return copy(
            out_buf.at[j], in_buf.at[j], o_send, o_recv.at[lax.div(j, 2)], (tile, far_back)
        )

    def await_in(j):
        part = pair_of(j)
        copy(out_buf.at[part], in_buf.at[part], o_send, o_recv.at[j], (tile, far_back)).wait_recv()

    x_all = copy(x_buf, x_in, x_send, x_recv.at[0], (mate, front))
    out_all = copy(out_buf, in_buf, o_send, o_recv.at[0], (tile, far_back))

    held = first & is_front
    pl.semaphore_wait(
        barrier,
        5 + jnp.where(is_front, 1, 0) - jnp.where(held, 2, 0) + jnp.where(last, 1, 0),
    )

    @pl.when(last)
    def _():
        pl.semaphore_signal(
            ready.at[core], inc=1, device_id=(above, front), device_id_type=MESH
        )

    pltpu.make_async_copy(twin, own, load_sem).wait()
    @pl.when(odd == 0)
    def _():
        detour().start()

    @pl.when(jnp.logical_not(held))
    def _():
        for k in range(pairs):
            z_copy(k).start()

    @pl.when(odd == 1)
    def _():
        for k in range(pairs):
            f_copy(k).start()

    far_copy.start()
    twin_copy.start()
    for table in tables:
        table.wait()

    first_row = (tile * n).astype(jnp.float32)
    row_at = lax.broadcasted_iota(jnp.int32, (8, n), 1).astype(jnp.float32)
    p = (first_row + row_at - (tiles * n - 1) / 2.0) / n
    col_at = lax.broadcasted_iota(jnp.int32, (8, blocks * n), 1).astype(jnp.float32)
    q = (col_at - (blocks * n - 1) / 2.0) / n
    weight_sum = weights_ref[0]
    for a in range(1, slices):
        weight_sum = weight_sum + weights_ref[a]
    for a in range(slices):
        row_cos, row_sin = cos_sin(defocus_ref[a] * (p * p))
        share = jnp.sqrt(jnp.full((8, n), weights_ref[a], jnp.float32) / weight_sum)
        row_cos, row_sin = (row_cos * share)[0:1], (row_sin * share)[0:1]
        real = base_tab[0] * row_cos - base_tab[1] * row_sin
        imag = base_tab[0] * row_sin + base_tab[1] * row_cos
        left[2 * a * n : (2 * a + 1) * n, 0:n] = real.astype(jnp.bfloat16)
        left[2 * a * n : (2 * a + 1) * n, n : 2 * n] = (-imag).astype(jnp.bfloat16)
        left[(2 * a + 1) * n : (2 * a + 2) * n, 0:n] = imag.astype(jnp.bfloat16)
        left[(2 * a + 1) * n : (2 * a + 2) * n, n : 2 * n] = real.astype(jnp.bfloat16)
        c, s = cos_sin(defocus_ref[a] * (q * q))
        for j in range(pairs):
            col_cos[j, a] = c[:, j * 2 * n : (j + 1) * 2 * n]
            col_sin[j, a] = s[:, j * 2 * n : (j + 1) * 2 * n]

    @pl.when(held)
    def _():
        pl.semaphore_wait(ready.at[1], 1)
        for k in range(pairs):
            z_copy(k).start()

    def plan_of(direction, layer):
        row_steps, col_steps = off_ref[direction, 0, layer], off_ref[direction, 1, layer]
        fy = (row_steps & (QUANT - 1)).astype(jnp.float32) * (1.0 / QUANT)
        fx = (col_steps & (QUANT - 1)).astype(jnp.float32) * (1.0 / QUANT)
        down = lax.shift_right_logical(row_steps, 2)
        over = lax.shift_right_logical(col_steps, 2) & (n - 1)
        begin = lax.shift_right_logical(col_steps, n.bit_length() + 1)
        return down, fy, over, fx, begin

    @pl.when(is_front)
    def _():
        plans = [
            plan_of(place, layer)
            for layer in (front, back, far_front, far_back)
        ]
        for slot, (down, fy, over, fx, _) in enumerate(plans):
            front_slide[slot] = taps((3 * n, 2 * n), over, fx, 0, 1)
            for reach in range(REACH + 1):
                front_mix[reach * n : (reach + 1) * n, slot * n : (slot + 1) * n] = taps(
                    (n, n), down - reach * n, fy, 1, 0
                )

        def shift(slot, block_of):
            begin = plans[slot][4]

            def step(g, carry):
                rows = []
                for j in range(GROUP):
                    at = begin + 2 * (g * GROUP + j)
                    rows.append(
                        jnp.concatenate([block_of((at + b) & (blocks - 1)) for b in range(3)], 1)
                    )
                total = jnp.dot(
                    jnp.concatenate(rows, 0), front_slide[slot], preferred_element_type=jnp.float32
                ).astype(jnp.bfloat16)
                for j in range(GROUP):
                    mixed[g * GROUP + j, slot * n : (slot + 1) * n, :] = total[j * n : (j + 1) * n]
                return carry

            lax.fori_loop(0, pairs // GROUP, step, 0)

        shift(0, lambda b: own[b])
        twin_copy.wait_recv()
        shift(1, lambda b: twin[b])
        far_both.wait_recv()
        @pl.when(first)
        def _():
            pl.semaphore_wait(ready.at[0], 1)

        def send_pair(j):
            for b in range(2):
                x_copy(2 * j + b).start()

            @pl.when(odd == 0)
            def _():
                for b in range(2):
                    down_copy(2 * j + b).start()

        def give_step(g, carry):
            for side in range(2):
                begin = plans[2 + side][4] + 2 * PACE * g
                rows = []
                for j in range(PACE):
                    rows.append(
                        jnp.concatenate(
                            [far[side, (begin + 2 * j + b) & (blocks - 1)] for b in range(3)], 1
                        )
                    )
                total = jnp.dot(
                    jnp.concatenate(rows, 0), front_slide[2 + side], preferred_element_type=jnp.float32
                ).astype(jnp.bfloat16)
                for j in range(PACE):
                    mixed[g * PACE + j, (2 + side) * n : (3 + side) * n, :] = total[j * n : (j + 1) * n]
            for i in range(PACE):
                j = g * PACE + i
                total = jnp.dot(front_mix[...], mixed[j], preferred_element_type=jnp.float32)
                local[j] = total[:n]
                tail[j] = total[2 * n :]
                for b in range(2):
                    part = slice(b * n, (b + 1) * n)
                    x_buf[2 * j + b] = total[n : 2 * n, part].astype(jnp.bfloat16)
                    out_buf[2 * j + b] = total[2 * n :, part].astype(jnp.bfloat16)
            @pl.when(g > 0)
            def _():
                send_pair(g * PACE - 1)

            for j in range(PACE - 1):
                send_pair(g * PACE + j)
            return carry

        lax.fori_loop(0, pairs // PACE, give_step, 0)


        @pl.when(odd == 1)
        def _():
            pass_on(0)
            for b in range(2):
                x_copy(blocks - 2 + b).start()

            def step(j, carry):
                pass_on(j)
                return carry

            lax.fori_loop(1, ahead, step, 0)

    @pl.when(is_back)
    def _():
        plans = [
            [plan_of(direction, layer) for layer in (front, back)]
            for direction in (far_back, place)
        ]
        for index in range(2):
            for slot in range(2):
                down, fy, over, fx, _ = plans[index][slot]
                back_mix[slot, index * n : (index + 1) * n, :] = taps((n, 3 * n), down, fy, 1, 0)
                back_slide[index, slot * 3 * n : (slot + 1) * 3 * n, :] = taps(
                    (3 * n, 2 * n), over, fx, 0, 1
                )
        twin_copy.wait_recv()

        lead = jnp.where(last & (odd == 0), LEAD, 0)

        def take(k, layer):
            z_copy(k, layer).wait_recv()

            @pl.when((odd == 0) & (k < straight))
            def _():
                relay(k, layer).start()

        def lead_step(k, carry):
            take(k, 1)
            return carry

        lax.fori_loop(0, lead, lead_step, 0)

        @pl.when(odd == 1)
        def _():
            detour_both.wait_recv()
            for k in range(straight, pairs):
                onward(k).start()

        def rows_step(j, carry):
            take(j, 0)

            @pl.when(j + lead < pairs)
            def _():
                take(j + lead, 1)

            h_both(j).wait_recv()
            for layer in range(2):
                nearest = twin if layer == 0 else own
                window = jnp.concatenate(
                    [
                        jnp.concatenate(
                            [nearest[2 * j + b], halo[layer, 0, 2 * j + b], halo[layer, 1, 2 * j + b]], 0
                        )
                        for b in range(2)
                    ],
                    1,
                )
                total = jnp.dot(
                    back_mix[layer], window, preferred_element_type=jnp.float32
                ).astype(jnp.bfloat16)
                for index in range(2):
                    for b in range(2):
                        moved[layer, index, 2 * j + b] = total[
                            index * n : (index + 1) * n, b * n : (b + 1) * n
                        ]
            return carry

        lax.fori_loop(0, pairs, rows_step, 0)

        def cols(index, g, size):
            rows = []
            for j in range(size):
                parts = []
                for layer in range(2):
                    begin = plans[index][layer][4] + 2 * (g * size + j)
                    for b in range(3):
                        parts.append(moved[layer, index, (begin + b) & (blocks - 1)])
                rows.append(jnp.concatenate(parts, 1))
            return jnp.dot(
                jnp.concatenate(rows, 0), back_slide[index], preferred_element_type=jnp.float32
            )

        def send_pair(j):
            for b in range(2):
                across_copy(2 * j + b).start()

        def give_step(g, carry):
            total = cols(0, g, PACE).astype(jnp.bfloat16)
            for j in range(PACE):
                for b in range(2):
                    out_buf[2 * (g * PACE + j) + b] = total[j * n : (j + 1) * n, b * n : (b + 1) * n]

            @pl.when(g > 0)
            def _():
                send_pair(g * PACE - 1)

            for j in range(PACE - 1):
                send_pair(g * PACE + j)
            return carry

        lax.fori_loop(0, pairs // PACE, give_step, 0)

        def keep_step(g, carry):
            total = cols(1, g, BATCH)
            for j in range(BATCH):
                local[g * BATCH + j] = total[j * n : (j + 1) * n]

            @pl.when(g == 0)
            def _():
                send_pair(pairs - 1)

            return carry

        lax.fori_loop(0, pairs // BATCH, keep_step, 0)

    def field_of(j):
        arrived = jnp.concatenate([in_buf[2 * j + b].astype(jnp.float32) for b in range(2)], 1)
        c, s = cos_sin(local[j] + arrived)
        return jnp.concatenate([c, s], 0).astype(jnp.bfloat16)

    def spots(j, field):
        focal = jnp.dot(left[...], field, preferred_element_type=jnp.float32)
        fields = []
        for a in range(slices):
            real, imag = focal[2 * a * n : (2 * a + 1) * n], focal[(2 * a + 1) * n : (2 * a + 2) * n]
            c, s = col_cos[j, a][0:1], col_sin[j, a][0:1]
            new_real = (real * c - imag * s).astype(jnp.bfloat16)
            new_imag = (real * s + imag * c).astype(jnp.bfloat16)
            for b in range(2):
                fields.append(
                    jnp.concatenate([new_real[:, b * n : (b + 1) * n], new_imag[:, b * n : (b + 1) * n]], 1)
                )
        spot = jnp.dot(jnp.concatenate(fields, 0), right_tab[...], preferred_element_type=jnp.float32)
        power = spot * spot
        for b in range(2):
            total = 0.0
            for a in range(slices):
                piece = power[(2 * a + b) * n : (2 * a + b + 1) * n]
                total = total + (piece[:, :n] + piece[:, n:])
            lit = valid_ref[0, 2 * j + b].astype(jnp.float32)
            out_ref[0, 0, :, pl.ds(pl.multiple_of((2 * j + b) * n, n), n)] = (total * lit).astype(
                jnp.bfloat16
            )

    passing = is_front & (odd == 1)

    @pl.when(jnp.logical_not(passing))
    def _():
        def final_step(j, carry):
            @pl.when(is_front)
            def _():
                for b in range(2):
                    x_copy(2 * j + b).wait_recv()
                    part = slice(b * n, (b + 1) * n)
                    local[j, :, part] = local[j, :, part] + x_in[2 * j + b].astype(jnp.float32)

                @pl.when(j == 0)
                def _():
                    for b in range(2):
                        x_copy(blocks - 2 + b).start()
                        down_copy(blocks - 2 + b).start()

            await_in(j)
            spots(j, field_of(j))
            return carry

        lax.fori_loop(0, pairs, final_step, 0, unroll=2)

    @pl.when(passing)
    def _():
        @pl.when(jnp.logical_not(first))
        def _():
            down_copy(blocks - 1).start()

        await_in(0)
        field_buf[0] = field_of(0)

        def final_step(i, carry):
            j = 2 * i

            @pl.when(j + ahead < pairs)
            def _():
                pass_on(j + ahead)

            await_in(j + 1)
            field_buf[1] = field_of(j + 1)
            spots(j, field_buf[0])

            @pl.when(j + 1 + ahead < pairs)
            def _():
                pass_on(j + 1 + ahead)

            await_in(j + 2)

            @pl.when((j == 0) & first)
            def _():
                down_copy(blocks - 1).start()

            field_buf[0] = field_of(j + 2)
            spots(j + 1, field_buf[1])
            return carry

        lax.fori_loop(0, pairs // 2 - 1, final_step, 0)
        await_in(pairs - 1)
        field_buf[1] = field_of(pairs - 1)
        spots(pairs - 2, field_buf[0])
        spots(pairs - 1, field_buf[1])

    z_all.wait_send()
    far_copy.wait_send()
    twin_copy.wait_send()
    out_all.wait_send()

    @pl.when(odd == 1)
    def _():
        f_all.wait_send()

    @pl.when(is_front)
    def _():
        x_all.wait_send()

    @pl.when(odd == 0)
    def _():
        detour().wait_send()

    @pl.when(is_back & (odd == 0))
    def _():
        r_all.wait_send()

    @pl.when(is_back & (odd == 1))
    def _():
        onward_all.wait_send()


def solution(mesh):
    tiles = mesh.shape["tile"]

    def shards(layers, offsets, subap_valid, defocus, weights):
        n, cols = layers.shape[1], layers.shape[2]
        blocks = cols // n
        slices = defocus.shape[0]
        pairs = blocks // 2
        fr, fi = base_tables(n)
        right = jnp.asarray(np.block([[fr.T, fi.T], [-fi.T, fr.T]])).astype(jnp.bfloat16)
        vmem = pl.BlockSpec(memory_space=pltpu.VMEM)
        hbm = pl.BlockSpec(memory_space=pl.ANY)
        dma = pltpu.SemaphoreType.DMA
        half, full = jnp.bfloat16, jnp.float32
        return pl.pallas_call(
            functools.partial(kernel, tiles, n, blocks, slices),
            out_shape=pltpu.VMEM((1, 1, n, cols), half),
            in_specs=[hbm] * 7,
            out_specs=vmem,
            scratch_shapes=[
                pltpu.SMEM((4, 2, 4), jnp.int32),
                pltpu.SMEM((1, blocks), jnp.int32),
                pltpu.SMEM((slices,), full),
                pltpu.SMEM((slices,), full),
                pltpu.VMEM((blocks, n, n), half),
                pltpu.VMEM((blocks, n, n), half),
                pltpu.VMEM((2, blocks, n, n), half),
                pltpu.VMEM((2, REACH, blocks, n, n), half),
                pltpu.VMEM((2, 2 * DETOUR, n, n), half),
                pltpu.VMEM((pairs, 4 * n, 2 * n), half),
                pltpu.VMEM((2, 2, blocks, n, n), half),
                pltpu.VMEM(((REACH + 1) * n, 4 * n), half),
                pltpu.VMEM((4, 3 * n, 2 * n), half),
                pltpu.VMEM((2, 2 * n, (REACH + 1) * n), half),
                pltpu.VMEM((2, 6 * n, 2 * n), half),
                pltpu.VMEM((blocks, n, n), half),
                pltpu.VMEM((blocks, n, n), half),
                pltpu.VMEM((pairs, n, 2 * n), full),
                pltpu.VMEM((blocks, n, n), half),
                pltpu.VMEM((blocks, n, n), half),
                pltpu.VMEM((pairs, n, 2 * n), full),
                pltpu.VMEM((2 * slices * n, 2 * n), half),
                pltpu.VMEM((pairs, slices, 8, 2 * n), full),
                pltpu.VMEM((pairs, slices, 8, 2 * n), full),
                pltpu.VMEM((2, n, n), full),
                pltpu.VMEM((2 * n, 2 * n), half),
                pltpu.VMEM((2, 2 * n, 2 * n), half),
                dma, dma((6,)),
                dma, dma((2, pairs)), dma, dma, dma((pairs,)),
                dma, dma, dma, dma,
                dma, dma((blocks,)), dma, dma((pairs,)), dma, dma,
                pltpu.SemaphoreType.REGULAR((2,)),
            ],
            compiler_params=pltpu.CompilerParams(collective_id=0, has_side_effects=True),
        )(layers, jnp.transpose(offsets, (0, 2, 1)), subap_valid, defocus, weights, jnp.asarray(np.stack([fr, fi])), right)

    placed = (P("dir", "tile", None), P(), P("tile", None), P(), P())
    return jax.shard_map(
        shards, mesh=mesh, in_specs=placed, out_specs=P("dir", "tile", None, None), check_vma=False
    )
```

```python
import functools
import math

import jax
import jax.numpy as jnp
import numpy as np
from jax import lax
from jax.experimental import pallas as pl
from jax.experimental.pallas import tpu as pltpu
from jax.sharding import PartitionSpec as P

OVER = 2
QUANT = 4
REACH = 2
GROUP = 8
BATCH = 8
LEAD = 3
PACE = 2
STRIDE = 2
EARLY = 2
DETOUR = 2
MESH = pl.DeviceIdType.MESH
SIN = (3.141582022082025, -5.167142794167084, 2.541899009948703, -0.5546361567315732)
COS = (0.999999953466345, -4.934792858633932, 4.058411913339297, -1.3318801559459539, 0.21969678799073292)


def base_tables(n):
    frequency = np.arange(n, dtype=np.float64) - n // 2
    position = np.arange(n, dtype=np.float64) - (n - 1) / 2.0
    angle = -2.0 * math.pi / (OVER * n) * frequency[:, None] * position[None, :]
    factor = 1.0 / math.sqrt(n)
    return (np.cos(angle) * factor).astype(np.float32), (np.sin(angle) * factor).astype(np.float32)


def cos_sin(angle):
    turns = angle * (1.0 / math.pi)
    whole = jnp.round(turns)
    rest = turns - whole
    sign = jnp.where((whole.astype(jnp.int32) & 1) == 0, 1.0, -1.0)
    square = rest * rest
    sin, cos = SIN[-1], COS[-1]
    for factor in SIN[-2::-1]:
        sin = factor + square * sin
    for factor in COS[-2::-1]:
        cos = factor + square * cos
    return cos * sign, sin * (rest * sign)


def taps(shape, shift, fraction, along, across):
    gap = lax.broadcasted_iota(jnp.int32, shape, along) - lax.broadcasted_iota(
        jnp.int32, shape, across
    ) - shift
    return jnp.where(gap == 0, 1.0 - fraction, jnp.where(gap == 1, fraction, 0.0)).astype(
        jnp.bfloat16
    )


def kernel(
    tiles, n, blocks, slices,
    x_ref, off_hbm, valid_hbm, defocus_hbm, weights_hbm, base_ref, right_ref,
    out_ref,
    off_ref, valid_ref, defocus_ref, weights_ref, own, twin, far, halo, via, mixed, moved, front_mix, front_slide, back_mix, back_slide,
    x_buf, x_in, tail, out_buf, in_buf, local, left, col_cos, col_sin, base_tab, right_tab, field_buf,
    load_sem, table_sem, z_send, z_recv, f_send, r_send, h_recv, y_send, y_recv, t_send, t_recv,
    x_send, x_recv, o_send, o_recv, v_send, v_recv, ready,
):
    tile = lax.axis_index("tile")
    place = lax.axis_index("dir")
    core = lax.rem(place, 2)
    chip = lax.div(place, 2)
    partner = chip * 2 + (1 - core)
    front, back = chip * 2, chip * 2 + 1
    far_front, far_back = (1 - chip) * 2, (1 - chip) * 2 + 1
    odd = lax.rem(tile, 2)
    mate = tile + 1 - 2 * odd
    below = lax.rem(tile + tiles - 2, tiles)
    above = lax.rem(tile + 2, tiles)
    pairs = blocks // 2
    is_front, is_back = core == 0, core == 1

    first, last = tile < 2, tile >= tiles - 2
    ahead = jnp.where(first, pairs - EARLY, pairs)

    barrier = pltpu.get_barrier_semaphore()

    def greet(device):
        pl.semaphore_signal(barrier, inc=1, device_id=device, device_id_type=MESH)

    @pl.when(is_back)
    def _():
        greet((above, back))

    @pl.when(jnp.logical_not(last))
    def _():
        greet((above, front))

    @pl.when(first & is_front)
    def _():
        greet((below, back))
        greet((below, front))

    @pl.when(is_front)
    def _():
        greet((tile, far_back))

    @pl.when(is_back)
    def _():
        greet((mate, front))

    greet((mate, front + core))
    greet((tile, far_front + core))
    greet((tile, partner))

    for k in range(blocks):
        pltpu.make_async_copy(x_ref.at[0, :, pl.ds(k * n, n)], own.at[k], load_sem).start()
    tables = [
        pltpu.make_async_copy(source, target, table_sem.at[i])
        for i, (source, target) in enumerate(
            (
                (defocus_hbm, defocus_ref), (off_hbm, off_ref), (weights_hbm, weights_ref),
                (valid_hbm, valid_ref), (base_ref, base_tab), (right_ref, right_tab),
            )
        )
    ]
    for table in tables:
        table.start()

    def copy(source, target, send, recv, device):
        return pltpu.make_async_remote_copy(
            src_ref=source, dst_ref=target, send_sem=send, recv_sem=recv,
            device_id=device, device_id_type=MESH,
        )

    def pair_of(k):
        return pl.ds(2 * k, 2)

    def z_copy(k, layer=core):
        return copy(
            own.at[pair_of(k)], halo.at[layer, 1, pair_of(k)], z_send, z_recv.at[layer, k],
            (below, back),
        )

    def f_copy(k):
        return copy(
            own.at[pair_of(k)], halo.at[core, 0, pair_of(k)], f_send, h_recv.at[k], (mate, back)
        )

    def relay(k, layer):
        return copy(
            halo.at[layer, 1, pair_of(k)], halo.at[layer, 0, pair_of(k)], r_send, h_recv.at[k],
            (mate, back),
        )

    def h_both(k):
        part = halo.at[:, 0, pair_of(k)]
        return copy(part, part, r_send, h_recv.at[k], (mate, back))

    straight = pairs - DETOUR
    rest = pl.ds(2 * straight, 2 * DETOUR)

    def detour(layer=core):
        return copy(own.at[rest], via.at[layer], v_send, v_recv, (mate, back))

    detour_both = copy(via, via, v_send, v_recv, (mate, back))

    def onward(k):
        part = pl.ds(2 * (k - straight), 2)
        return copy(
            via.at[:, part], halo.at[:, 0, pair_of(k)], r_send, h_recv.at[k], (below, back)
        )

    z_all = copy(own, halo.at[core, 1], z_send, z_recv.at[0, 0], (below, back))
    f_all = copy(own, halo.at[core, 0], f_send, h_recv.at[0], (mate, back))
    before = pl.ds(0, 2 * straight)
    r_all = copy(halo.at[:, 1, before], halo.at[:, 0, before], r_send, h_recv.at[0], (mate, back))
    onward_all = copy(via, via, r_send, h_recv.at[0], (below, back))
    far_copy = copy(own, far.at[core], y_send, y_recv, (tile, far_front))
    far_both = copy(far, far, y_send, y_recv, (tile, far_front))

    twin_copy = copy(own, twin, t_send, t_recv, (tile, partner))

    def x_copy(j):
        return copy(x_buf.at[j], x_in.at[j], x_send, x_recv.at[lax.div(j, 2)], (mate, front))

    def await_x(j):
        part = pair_of(j)
        copy(x_buf.at[part], x_in.at[part], x_send, x_recv.at[j], (mate, front)).wait_recv()

    def down_copy(j):
        return copy(out_buf.at[j], in_buf.at[j], o_send, o_recv.at[lax.div(j, 2)], (below, front))

    def pass_on(j):
        await_x(j)
        for b in range(2):
            k = 2 * j + b
            out_buf[k] = (
                tail[j, :, b * n : (b + 1) * n] + x_in[k].astype(jnp.float32)
            ).astype(jnp.bfloat16)

            @pl.when(k > 0)
            def _():
                down_copy(k - 1).start()

    def across_copy(j):
        return copy(
            out_buf.at[j], in_buf.at[j], o_send, o_recv.at[lax.div(j, 2)], (tile, far_back)
        )

    def await_in(j):
        part = pair_of(j)
        copy(out_buf.at[part], in_buf.at[part], o_send, o_recv.at[j], (tile, far_back)).wait_recv()

    x_all = copy(x_buf, x_in, x_send, x_recv.at[0], (mate, front))
    out_all = copy(out_buf, in_buf, o_send, o_recv.at[0], (tile, far_back))

    held = first & is_front
    pl.semaphore_wait(
        barrier,
        5 + jnp.where(is_front, 1, 0) - jnp.where(held, 2, 0) + jnp.where(last, 1, 0),
    )

    @pl.when(last)
    def _():
        pl.semaphore_signal(
            ready.at[core], inc=1, device_id=(above, front), device_id_type=MESH
        )

    pltpu.make_async_copy(twin, own, load_sem).wait()
    far_copy.start()
    @pl.when(odd == 0)
    def _():
        detour().start()

    @pl.when(jnp.logical_not(held))
    def _():
        for k in range(pairs):
            z_copy(k).start()

    @pl.when(odd == 1)
    def _():
        for k in range(pairs):
            f_copy(k).start()

    twin_copy.start()
    for table in tables:
        table.wait()

    first_row = (tile * n).astype(jnp.float32)
    row_at = lax.broadcasted_iota(jnp.int32, (8, n), 1).astype(jnp.float32)
    p = (first_row + row_at - (tiles * n - 1) / 2.0) / n
    col_at = lax.broadcasted_iota(jnp.int32, (8, blocks * n), 1).astype(jnp.float32)
    q = (col_at - (blocks * n - 1) / 2.0) / n
    weight_sum = weights_ref[0]
    for a in range(1, slices):
        weight_sum = weight_sum + weights_ref[a]
    for a in range(slices):
        row_cos, row_sin = cos_sin(defocus_ref[a] * (p * p))
        share = jnp.sqrt(jnp.full((8, n), weights_ref[a], jnp.float32) / weight_sum)
        row_cos, row_sin = (row_cos * share)[0:1], (row_sin * share)[0:1]
        real = base_tab[0] * row_cos - base_tab[1] * row_sin
        imag = base_tab[0] * row_sin + base_tab[1] * row_cos
        left[2 * a * n : (2 * a + 1) * n, 0:n] = real.astype(jnp.bfloat16)
        left[2 * a * n : (2 * a + 1) * n, n : 2 * n] = (-imag).astype(jnp.bfloat16)
        left[(2 * a + 1) * n : (2 * a + 2) * n, 0:n] = imag.astype(jnp.bfloat16)
        left[(2 * a + 1) * n : (2 * a + 2) * n, n : 2 * n] = real.astype(jnp.bfloat16)
        c, s = cos_sin(defocus_ref[a] * (q * q))
        for j in range(pairs):
            col_cos[j, a] = c[:, j * 2 * n : (j + 1) * 2 * n]
            col_sin[j, a] = s[:, j * 2 * n : (j + 1) * 2 * n]

    @pl.when(held)
    def _():
        pl.semaphore_wait(ready.at[1], 1)
        for k in range(pairs):
            z_copy(k).start()

    def plan_of(direction, layer):
        row_steps, col_steps = off_ref[direction, 0, layer], off_ref[direction, 1, layer]
        fy = (row_steps & (QUANT - 1)).astype(jnp.float32) * (1.0 / QUANT)
        fx = (col_steps & (QUANT - 1)).astype(jnp.float32) * (1.0 / QUANT)
        down = lax.shift_right_logical(row_steps, 2)
        over = lax.shift_right_logical(col_steps, 2) & (n - 1)
        begin = lax.shift_right_logical(col_steps, n.bit_length() + 1)
        return down, fy, over, fx, begin

    @pl.when(is_front)
    def _():
        plans = [
            plan_of(place, layer)
            for layer in (front, back, far_front, far_back)
        ]
        for slot, (down, fy, over, fx, _) in enumerate(plans):
            front_slide[slot] = taps((3 * n, 2 * n), over, fx, 0, 1)
            for reach in range(REACH + 1):
                front_mix[reach * n : (reach + 1) * n, slot * n : (slot + 1) * n] = taps(
                    (n, n), down - reach * n, fy, 1, 0
                )

        def shift(slot, block_of):
            begin = plans[slot][4]

            def step(g, carry):
                rows = []
                for j in range(GROUP):
                    at = begin + 2 * (g * GROUP + j)
                    rows.append(
                        jnp.concatenate([block_of((at + b) & (blocks - 1)) for b in range(3)], 1)
                    )
                total = jnp.dot(
                    jnp.concatenate(rows, 0), front_slide[slot], preferred_element_type=jnp.float32
                ).astype(jnp.bfloat16)
                for j in range(GROUP):
                    mixed[g * GROUP + j, slot * n : (slot + 1) * n, :] = total[j * n : (j + 1) * n]
                return carry

            lax.fori_loop(0, pairs // GROUP, step, 0)

        shift(0, lambda b: own[b])
        twin_copy.wait_recv()
        shift(1, lambda b: twin[b])
        far_both.wait_recv()
        @pl.when(first)
        def _():
            pl.semaphore_wait(ready.at[0], 1)

        def send_pair(j):
            for b in range(2):
                x_copy(2 * j + b).start()

            @pl.when(odd == 0)
            def _():
                for b in range(2):
                    down_copy(2 * j + b).start()

        def give_step(g, carry):
            for side in range(2):
                begin = plans[2 + side][4] + 2 * PACE * g
                rows = []
                for j in range(PACE):
                    rows.append(
                        jnp.concatenate(
                            [far[side, (begin + 2 * j + b) & (blocks - 1)] for b in range(3)], 1
                        )
                    )
                total = jnp.dot(
                    jnp.concatenate(rows, 0), front_slide[2 + side], preferred_element_type=jnp.float32
                ).astype(jnp.bfloat16)
                for j in range(PACE):
                    mixed[g * PACE + j, (2 + side) * n : (3 + side) * n, :] = total[j * n : (j + 1) * n]
            for i in range(PACE):
                j = g * PACE + i
                total = jnp.dot(front_mix[...], mixed[j], preferred_element_type=jnp.float32)
                local[j] = total[:n]
                tail[j] = total[2 * n :]
                for b in range(2):
                    part = slice(b * n, (b + 1) * n)
                    x_buf[2 * j + b] = total[n : 2 * n, part].astype(jnp.bfloat16)
                    out_buf[2 * j + b] = total[2 * n :, part].astype(jnp.bfloat16)
            @pl.when(g > 0)
            def _():
                send_pair(g * PACE - 1)

            for j in range(PACE - 1):
                send_pair(g * PACE + j)
            return carry

        lax.fori_loop(0, pairs // PACE, give_step, 0)


        @pl.when(odd == 1)
        def _():
            pass_on(0)
            for b in range(2):
                x_copy(blocks - 2 + b).start()

            def step(j, carry):
                pass_on(j)
                return carry

            lax.fori_loop(1, ahead, step, 0)

    @pl.when(is_back)
    def _():
        plans = [
            [plan_of(direction, layer) for layer in (front, back)]
            for direction in (far_back, place)
        ]
        for index in range(2):
            for slot in range(2):
                down, fy, over, fx, _ = plans[index][slot]
                back_mix[slot, index * n : (index + 1) * n, :] = taps((n, 3 * n), down, fy, 1, 0)
                back_slide[index, slot * 3 * n : (slot + 1) * 3 * n, :] = taps(
                    (3 * n, 2 * n), over, fx, 0, 1
                )
        twin_copy.wait_recv()

        lead = jnp.where(last & (odd == 0), LEAD, 0)

        def take(k, layer):
            z_copy(k, layer).wait_recv()

            @pl.when((odd == 0) & (k < straight))
            def _():
                relay(k, layer).start()

        def lead_step(k, carry):
            take(k, 1)
            return carry

        lax.fori_loop(0, lead, lead_step, 0)

        @pl.when(odd == 1)
        def _():
            detour_both.wait_recv()
            for k in range(straight, pairs):
                onward(k).start()

        def rows_step(j, carry):
            take(j, 0)

            @pl.when(j + lead < pairs)
            def _():
                take(j + lead, 1)

            h_both(j).wait_recv()
            for layer in range(2):
                nearest = twin if layer == 0 else own
                window = jnp.concatenate(
                    [
                        jnp.concatenate(
                            [nearest[2 * j + b], halo[layer, 0, 2 * j + b], halo[layer, 1, 2 * j + b]], 0
                        )
                        for b in range(2)
                    ],
                    1,
                )
                total = jnp.dot(
                    back_mix[layer], window, preferred_element_type=jnp.float32
                ).astype(jnp.bfloat16)
                for index in range(2):
                    for b in range(2):
                        moved[layer, index, 2 * j + b] = total[
                            index * n : (index + 1) * n, b * n : (b + 1) * n
                        ]
            return carry

        lax.fori_loop(0, pairs, rows_step, 0)

        def cols(index, g, size):
            rows = []
            for j in range(size):
                parts = []
                for layer in range(2):
                    begin = plans[index][layer][4] + 2 * (g * size + j)
                    for b in range(3):
                        parts.append(moved[layer, index, (begin + b) & (blocks - 1)])
                rows.append(jnp.concatenate(parts, 1))
            return jnp.dot(
                jnp.concatenate(rows, 0), back_slide[index], preferred_element_type=jnp.float32
            )

        def send_pair(j):
            for b in range(2):
                across_copy(2 * j + b).start()

        def give_step(g, carry):
            total = cols(0, g, STRIDE).astype(jnp.bfloat16)
            for j in range(STRIDE):
                for b in range(2):
                    out_buf[2 * (g * STRIDE + j) + b] = total[j * n : (j + 1) * n, b * n : (b + 1) * n]

            @pl.when(g > 0)
            def _():
                send_pair(g * STRIDE - 1)

            for j in range(STRIDE - 1):
                send_pair(g * STRIDE + j)
            return carry

        lax.fori_loop(0, pairs // STRIDE, give_step, 0)

        def keep_step(g, carry):
            total = cols(1, g, BATCH)
            for j in range(BATCH):
                local[g * BATCH + j] = total[j * n : (j + 1) * n]

            @pl.when(g == 0)
            def _():
                send_pair(pairs - 1)

            return carry

        lax.fori_loop(0, pairs // BATCH, keep_step, 0)

    def field_of(j):
        arrived = jnp.concatenate([in_buf[2 * j + b].astype(jnp.float32) for b in range(2)], 1)
        c, s = cos_sin(local[j] + arrived)
        return jnp.concatenate([c, s], 0).astype(jnp.bfloat16)

    def spots(j, field):
        focal = jnp.dot(left[...], field, preferred_element_type=jnp.float32)
        fields = []
        for a in range(slices):
            real, imag = focal[2 * a * n : (2 * a + 1) * n], focal[(2 * a + 1) * n : (2 * a + 2) * n]
            c, s = col_cos[j, a][0:1], col_sin[j, a][0:1]
            new_real = (real * c - imag * s).astype(jnp.bfloat16)
            new_imag = (real * s + imag * c).astype(jnp.bfloat16)
            for b in range(2):
                fields.append(
                    jnp.concatenate([new_real[:, b * n : (b + 1) * n], new_imag[:, b * n : (b + 1) * n]], 1)
                )
        spot = jnp.dot(jnp.concatenate(fields, 0), right_tab[...], preferred_element_type=jnp.float32)
        power = spot * spot
        for b in range(2):
            total = 0.0
            for a in range(slices):
                piece = power[(2 * a + b) * n : (2 * a + b + 1) * n]
                total = total + (piece[:, :n] + piece[:, n:])
            lit = valid_ref[0, 2 * j + b].astype(jnp.float32)
            out_ref[0, 0, :, pl.ds(pl.multiple_of((2 * j + b) * n, n), n)] = (total * lit).astype(
                jnp.bfloat16
            )

    passing = is_front & (odd == 1)

    @pl.when(jnp.logical_not(passing))
    def _():
        def final_step(j, carry):
            @pl.when(is_front)
            def _():
                await_x(j)
                for b in range(2):
                    part = slice(b * n, (b + 1) * n)
                    local[j, :, part] = local[j, :, part] + x_in[2 * j + b].astype(jnp.float32)

                @pl.when(j == 0)
                def _():
                    for b in range(2):
                        x_copy(blocks - 2 + b).start()
                        down_copy(blocks - 2 + b).start()

            await_in(j)
            spots(j, field_of(j))
            return carry

        lax.fori_loop(0, pairs, final_step, 0, unroll=2)

    @pl.when(passing)
    def _():
        @pl.when(jnp.logical_not(first))
        def _():
            down_copy(blocks - 1).start()

        await_in(0)
        field_buf[0] = field_of(0)

        def final_step(i, carry):
            j = 2 * i

            @pl.when(j + ahead < pairs)
            def _():
                pass_on(j + ahead)

            await_in(j + 1)
            field_buf[1] = field_of(j + 1)
            spots(j, field_buf[0])

            @pl.when(j + 1 + ahead < pairs)
            def _():
                pass_on(j + 1 + ahead)

            await_in(j + 2)

            @pl.when((j == 0) & first)
            def _():
                down_copy(blocks - 1).start()

            field_buf[0] = field_of(j + 2)
            spots(j + 1, field_buf[1])
            return carry

        lax.fori_loop(0, pairs // 2 - 1, final_step, 0)
        await_in(pairs - 1)
        field_buf[1] = field_of(pairs - 1)
        spots(pairs - 2, field_buf[0])
        spots(pairs - 1, field_buf[1])

    z_all.wait_send()
    far_copy.wait_send()
    twin_copy.wait_send()
    out_all.wait_send()

    @pl.when(odd == 1)
    def _():
        f_all.wait_send()

    @pl.when(is_front)
    def _():
        x_all.wait_send()

    @pl.when(odd == 0)
    def _():
        detour().wait_send()

    @pl.when(is_back & (odd == 0))
    def _():
        r_all.wait_send()

    @pl.when(is_back & (odd == 1))
    def _():
        onward_all.wait_send()


def solution(mesh):
    tiles = mesh.shape["tile"]

    def shards(layers, offsets, subap_valid, defocus, weights):
        n, cols = layers.shape[1], layers.shape[2]
        blocks = cols // n
        slices = defocus.shape[0]
        pairs = blocks // 2
        fr, fi = base_tables(n)
        right = jnp.asarray(np.block([[fr.T, fi.T], [-fi.T, fr.T]])).astype(jnp.bfloat16)
        vmem = pl.BlockSpec(memory_space=pltpu.VMEM)
        hbm = pl.BlockSpec(memory_space=pl.ANY)
        dma = pltpu.SemaphoreType.DMA
        half, full = jnp.bfloat16, jnp.float32
        return pl.pallas_call(
            functools.partial(kernel, tiles, n, blocks, slices),
            out_shape=pltpu.VMEM((1, 1, n, cols), half),
            in_specs=[hbm] * 7,
            out_specs=vmem,
            scratch_shapes=[
                pltpu.SMEM((4, 2, 4), jnp.int32),
                pltpu.SMEM((1, blocks), jnp.int32),
                pltpu.SMEM((slices,), full),
                pltpu.SMEM((slices,), full),
                pltpu.VMEM((blocks, n, n), half),
                pltpu.VMEM((blocks, n, n), half),
                pltpu.VMEM((2, blocks, n, n), half),
                pltpu.VMEM((2, REACH, blocks, n, n), half),
                pltpu.VMEM((2, 2 * DETOUR, n, n), half),
                pltpu.VMEM((pairs, 4 * n, 2 * n), half),
                pltpu.VMEM((2, 2, blocks, n, n), half),
                pltpu.VMEM(((REACH + 1) * n, 4 * n), half),
                pltpu.VMEM((4, 3 * n, 2 * n), half),
                pltpu.VMEM((2, 2 * n, (REACH + 1) * n), half),
                pltpu.VMEM((2, 6 * n, 2 * n), half),
                pltpu.VMEM((blocks, n, n), half),
                pltpu.VMEM((blocks, n, n), half),
                pltpu.VMEM((pairs, n, 2 * n), full),
                pltpu.VMEM((blocks, n, n), half),
                pltpu.VMEM((blocks, n, n), half),
                pltpu.VMEM((pairs, n, 2 * n), full),
                pltpu.VMEM((2 * slices * n, 2 * n), half),
                pltpu.VMEM((pairs, slices, 8, 2 * n), full),
                pltpu.VMEM((pairs, slices, 8, 2 * n), full),
                pltpu.VMEM((2, n, n), full),
                pltpu.VMEM((2 * n, 2 * n), half),
                pltpu.VMEM((2, 2 * n, 2 * n), half),
                dma, dma((6,)),
                dma, dma((2, pairs)), dma, dma, dma((pairs,)),
                dma, dma, dma, dma,
                dma, dma((pairs,)), dma, dma((pairs,)), dma, dma,
                pltpu.SemaphoreType.REGULAR((2,)),
            ],
            compiler_params=pltpu.CompilerParams(collective_id=0, has_side_effects=True),
        )(layers, jnp.transpose(offsets, (0, 2, 1)), subap_valid, defocus, weights, jnp.asarray(np.stack([fr, fi])), right)

    placed = (P("dir", "tile", None), P(), P("tile", None), P(), P())
    return jax.shard_map(
        shards, mesh=mesh, in_specs=placed, out_specs=P("dir", "tile", None, None), check_vma=False
    )
```
